512 devices in a mesh: gx: 128 (over z, y, core), gy: 4 (over x).
Axes of the slice: x: 4, y: 8, z: 8, core: 2. Of those that a mesh axis runs over, the one named last changes fastest.
Arguments:
- anomalies: float32 [80, 256, 32, 128], P(None, 'gx', 'gy'), may hold values from -6 to 6
- state_mean: float32 [256, 32, 128], P('gx', 'gy'), may hold values from -6 to 6
- obs_value: float32 [16, 256], P(None, 'gy'), may hold values from -8 to 8
- obs_cell: int32 [16, 256], replicated, may hold values from 0 to 2047
- owner: int32 [16], replicated, may hold values from 0 to 127, as said below
- order: int32 [16], replicated, may hold values from 0 to 15, each once
- root_inv: float32 [16, 256, 256], P(None, 'gy'), as said below
- gain_inv: float32 [16, 256, 256], P(None, 'gy'), as said below
Outputs:
- post_anomalies: float32 [80, 256, 32, 128], P(None, 'gx', 'gy')
- post_mean: float32 [256, 32, 128], P('gx', 'gy')
The draws below stay inside these ranges and needn't reach their ends.
Inputs may be any that keep to these rules, and one draw needn't show every extreme that they name: `owner`: some batch lies at slab 128 - 2, some at slab 1 and some at slab 128 // 2; the others favour low slabs. `order`: each batch number once. `root_inv`: symmetric. `gain_inv`: symmetric.
All inputs are finite; a program needn't handle non-finite values.
Results may differ from the reference program's by a relative error of at most 0.0001.
Values sent between devices are 32-bit elements; how exact they have to be, the bound alone decides.
A program may use at most 64 MiB of HBM per device.

```python
import math
import jax
import jax.numpy as jnp
from jax import lax

MEMBERS = 80
OBS = 256
BATCHES = 16
LON_DEV = 2
LAT_DEV = 8
LEVELS = 128
REACH = 3
NLON = 256
NLAT = 32
CELLS = 2048
N_GX = 128
N_GY = 4


def inverse_table(key, floor_value, top_value):
    key_diag, key_off = jax.random.split(key, 2)
    diagonal = jnp.exp(jax.random.uniform(key_diag, (BATCHES, OBS), jnp.float32, math.log(floor_value), math.log(top_value)))
    spread = 0.6 * math.sqrt(floor_value * top_value) / math.sqrt(OBS)
    offdiag_noise = jax.random.normal(key_off, (BATCHES, OBS, OBS), jnp.float32) * spread
    inverse = 0.5 * (offdiag_noise + jnp.swapaxes(offdiag_noise, 1, 2)) + diagonal[:, :, None] * jnp.eye(OBS, dtype=jnp.float32)
    return inverse


def draw_root_inv(key, part):
    return inverse_table(jax.random.fold_in(key, 11), 0.15, 0.5)


def draw_gain_inv(key, part):
    return inverse_table(jax.random.fold_in(key, 23), 0.3, 0.9)


def draw_owner(key, part):
    key_first, key_second, key_perm = jax.random.split(jax.random.fold_in(key, 37), 3)
    first_draw = jax.random.randint(key_first, (BATCHES,), 0, N_GX, dtype=jnp.int32)
    second_draw = jax.random.randint(key_second, (BATCHES,), 0, N_GX, dtype=jnp.int32)
    slabs = jnp.minimum(first_draw, second_draw)
    anchors = jnp.array([N_GX - 2, 1, N_GX // 2], dtype=jnp.int32)
    slabs = slabs.at[:3].set(anchors)
    shuffle = jax.random.permutation(key_perm, BATCHES)
    return slabs[shuffle].astype(jnp.int32)


def place_ends(drawn, own_key, least, high):
    index_at = [jax.random.randint(jax.random.fold_in(own_key, axis), (), 0, length) for axis, length in enumerate(drawn.shape)]
    longest = drawn.shape.index(max(drawn.shape))
    neighbour = index_at[:longest] + [(index_at[longest] + 1) % drawn.shape[longest]] + index_at[longest + 1:]
    return drawn.at[tuple(index_at)].set(least).at[tuple(neighbour)].set(high)


def block_levels(own_key, shape, cuts, low, largest):
    loudness = 1.0
    for dim, parts in cuts:
        draws = jax.random.uniform(jax.random.fold_in(jax.random.fold_in(own_key, 6), dim), (parts,), jnp.float32, low / len(cuts), largest / len(cuts))
        loudness = loudness * jnp.repeat(jnp.exp(draws), shape[dim] // parts).reshape((-1,) + (1,) * (len(shape) - 1 - dim))
    return loudness


def noise(key, dims, deviation, most, shards=(), kind=jnp.bfloat16):
    level = block_levels(key, dims, shards, -0.22, 0.18) if shards else 1.0
    drawn = jax.random.normal(key, dims, jnp.float32) * deviation * level
    return jnp.minimum(jnp.maximum(drawn, -most), most).astype(kind)


def setup_inputs(seed: int = 0) -> dict:
    arg_keys = jax.random.split(jax.random.key(seed), 9)
    anomalies = noise(arg_keys[0], (MEMBERS, NLON, NLAT, LEVELS), 1.0, 6.0, ((1, 128), (2, 4)), jnp.float32)
    state_mean = noise(arg_keys[1], (NLON, NLAT, LEVELS), 1.0, 6.0, ((0, 128), (1, 4)), jnp.float32)
    obs_value = noise(arg_keys[2], (BATCHES, OBS), 1.5, 8.0, ((1, 4),), jnp.float32)
    obs_cell = place_ends(jax.random.randint(arg_keys[3], (BATCHES, OBS), 0, CELLS), jax.random.fold_in(arg_keys[3], 1), 0, CELLS - 1).astype(jnp.int32)
    owner = draw_owner(jax.random.fold_in(arg_keys[8], 71), 0)
    order = jax.random.permutation(arg_keys[5], BATCHES).astype(jnp.int32)
    root_inv = draw_root_inv(jax.random.fold_in(arg_keys[8], 71), 0)
    gain_inv = draw_gain_inv(jax.random.fold_in(arg_keys[8], 71), 0)
    return {"anomalies": anomalies, "state_mean": state_mean, "obs_value": obs_value, "obs_cell": obs_cell, "owner": owner, "order": order, "root_inv": root_inv, "gain_inv": gain_inv}


def product(left_side, right_side):
    return jnp.dot(left_side, right_side, precision=lax.Precision.HIGHEST, preferred_element_type=jnp.float32)


def reference(anomalies, state_mean, obs_value, obs_cell, owner, order, root_inv, gain_inv):
    lon_total = LON_DEV * N_GX
    lat_total = LAT_DEV * N_GY
    quarter = OBS // N_GY
    window_width = (2 * REACH + 1) * LON_DEV
    reach_cells = REACH * LON_DEV
    taper_span = REACH * LON_DEV + 1.0
    obs_band = jnp.arange(OBS, dtype=jnp.int32) // quarter
    lat_index = jnp.arange(lat_total, dtype=jnp.int32)
    offsets = jnp.arange(window_width, dtype=jnp.int32)

    def assimilate(batch_turn, carried):
        state_field, mean_field = carried
        batch_id = order[batch_turn]
        root_slab = owner[batch_id]
        cells_of = obs_cell[batch_id]
        obs_lon = root_slab * LON_DEV + cells_of // (LAT_DEV * LEVELS)
        obs_lat = obs_band * LAT_DEV + (cells_of // LEVELS) % LAT_DEV
        obs_lev = cells_of % LEVELS
        prior_all = state_field[:, obs_lon, obs_lat, obs_lev]
        innovation = obs_value[batch_id] - mean_field[obs_lon, obs_lat, obs_lev]
        weighted = product(prior_all, root_inv[batch_id].T)
        gain_vec = product(gain_inv[batch_id], innovation)
        window_lon = (root_slab * LON_DEV - reach_cells + offsets) % lon_total
        window = state_field[:, window_lon].reshape(MEMBERS, -1)
        mean_window = mean_field[window_lon].reshape(-1)
        cell_lon = jnp.broadcast_to(window_lon[:, None, None], (window_width, lat_total, LEVELS)).reshape(-1)
        cell_lat = jnp.broadcast_to(lat_index[None, :, None], (window_width, lat_total, LEVELS)).reshape(-1)
        lon_gap = jnp.abs(obs_lon[:, None] - cell_lon[None, :])
        cycle_gap = jnp.minimum(lon_gap, lon_total - lon_gap)
        lat_gap = jnp.abs(obs_lat[:, None] - cell_lat[None, :])
        taper_rows = jnp.maximum(0.0, 1.0 - cycle_gap.astype(jnp.float32) / taper_span) * (1.0 - lat_gap.astype(jnp.float32) / lat_total)
        covariance = product(prior_all.T, window) / (MEMBERS - 1.0)
        gained = taper_rows * covariance
        stacked = jnp.concatenate([weighted, gain_vec[None, :]], axis=0)
        increment = product(stacked, gained)
        new_window = (window - increment[:MEMBERS]).reshape(MEMBERS, window_width, lat_total, LEVELS)
        new_mean = (mean_window + increment[MEMBERS]).reshape(window_width, lat_total, LEVELS)
        state_field = state_field.at[:, window_lon].set(new_window)
        mean_field = mean_field.at[window_lon].set(new_mean)
        return state_field, mean_field

    post_anomalies, post_mean = lax.fori_loop(0, BATCHES, assimilate, (anomalies, state_mean))
    return post_anomalies, post_mean
```

```python
import functools

import jax
import jax.numpy as jnp
from jax import lax
from jax.experimental import pallas as pl
from jax.experimental.pallas import tpu as pltpu
from jax.sharding import PartitionSpec as P

MEMBERS = 80
OBS = 256
BATCHES = 16
REACH = 3
SLABS = 128
BANDS = 4
NLON = 256
NLAT = 32
QUARTER = 64
CELLS = 2048
GROUPS = 16
ROWS = 96
HALF = 48
PAIRS = 8
RING = 8
MESH = pl.DeviceIdType.MESH
F32 = jnp.float32
BF16 = jnp.bfloat16


def dist(a, b):
    gap = jnp.abs(a - b)
    return jnp.minimum(gap, SLABS - gap)


def split(value):
    high = value.astype(BF16)
    return high, (value - high.astype(F32)).astype(BF16)


def dot(left, right):
    return jnp.dot(left, right, preferred_element_type=F32)


def dot3(left_high, left_low, right_high, right_low):
    return dot(left_high, right_high) + (dot(left_high, right_low) + dot(left_low, right_high))


def load_state(anom_ref, mean_ref, state):
    tail = lax.broadcasted_iota(jnp.int32, (16, 128), 0)
    for c in range(GROUPS):
        lanes = pl.ds(c * 128, 128)
        state[0:MEMBERS, lanes] = anom_ref[pl.ds(c, MEMBERS, stride=GROUPS), :]
        state[MEMBERS:ROWS, lanes] = jnp.where(tail == 0, -mean_ref[pl.ds(c, 1), :], 0.0)


def prep_kernel(
    order_s, owner_s, anom_ref, mean_ref, cell_ref, value_ref, root_ref, gain_ref,
    packet_ref, rows_ref, table_s,
    state, held, need_s, in_sem, out_sem,
):
    column = lax.axis_index("gx")
    band = lax.axis_index("gy")
    chip_low = column - lax.rem(column, 2)

    for t in reversed(range(BATCHES)):
        slab = owner_s[order_s[t]]
        near = jnp.minimum(dist(slab, chip_low), dist(slab, chip_low + 1)) <= REACH
        need = jnp.where(near, 1, 0)

        def later(s, need, slab=slab):
            linked = dist(owner_s[order_s[s]], slab) <= REACH
            return jnp.where(linked, need | need_s[s], need)

        need_s[t] = lax.fori_loop(t + 1, BATCHES, later, need)

    def listing(t, count):
        @pl.when(need_s[t] == 1)
        def _():
            table_s[1 + count] = order_s[t]

        return count + need_s[t]

    count = lax.fori_loop(0, BATCHES, listing, 0)
    table_s[0] = count

    def fetch(i, which, source):
        return pltpu.make_async_copy(source, held.at[i, which], in_sem.at[i, which])

    def start_fetch(i, carry):
        batch = table_s[1 + i]
        fetch(i, 0, root_ref.at[batch]).start()
        fetch(i, 1, gain_ref.at[batch]).start()
        return carry

    lax.fori_loop(0, count, start_fetch, 0)

    lane = lax.broadcasted_iota(jnp.int32, (8, 128), 1)
    low = 2 * lax.rem(lane, SLABS // 2)
    slabs = [owner_s[order_s[t]] for t in range(BATCHES)]
    needs = [None] * BATCHES
    total = jnp.zeros((8, 128), jnp.int32)
    for t in reversed(range(BATCHES)):
        near = jnp.minimum(dist(slabs[t], low), dist(slabs[t], low + 1)) <= REACH
        need = jnp.where(near, 1, 0)
        for s in range(t + 1, BATCHES):
            linked = jnp.where(dist(slabs[s], slabs[t]) <= REACH, 1, 0)
            need = need | (needs[s] * linked)
        needs[t] = need
        total = total + need
    table_s[BATCHES + 1] = jnp.max(total)

    packet_ref[...] = jnp.zeros_like(packet_ref)
    load_state(anom_ref, mean_ref, state)

    def pick(batch, carry):
        @pl.when(owner_s[batch] == column)
        def _():
            half = batch // PAIRS
            pair = lax.rem(batch, PAIRS)
            cells = jnp.broadcast_to(cell_ref[pl.ds(batch, 1), :], (8, OBS))
            shift = lax.rem(half * QUARTER - band * QUARTER + OBS, OBS)
            mine = pltpu.roll(cells, shift, 1)[0:1, 0:128]
            spot = lax.broadcasted_iota(jnp.int32, (1, 128), 1)
            valid = (spot // QUARTER) == half
            mine = jnp.where(valid, mine, -1)
            picked = jnp.zeros((ROWS, 128), F32)
            step = 512
            for at in range(0, CELLS, step):
                ids = lax.broadcasted_iota(jnp.int32, (step, 128), 0) + at
                hot = jnp.where(ids == mine, 1.0, 0.0).astype(BF16)
                block = state[:, pl.ds(at, step)]
                high = block.astype(BF16)
                rest = block - high.astype(F32)
                mid = rest.astype(BF16)
                last = (rest - mid.astype(F32)).astype(BF16)
                picked = picked + (dot(high, hot) + (dot(mid, hot) + dot(last, hot)))
            row = lax.broadcasted_iota(jnp.int32, (ROWS, 128), 0)
            seen = jnp.where(valid, value_ref[pl.ds(batch, 1), :], 0.0)
            picked = picked + jnp.where(row == MEMBERS, seen, 0.0)
            packet_ref[pair] = packet_ref[pair] + picked

        return carry

    lax.fori_loop(0, BATCHES, pick, 0)

    def put(i):
        return pltpu.make_async_copy(held.at[i], rows_ref.at[i], out_sem.at[i])

    def pass_on(i, carry):
        fetch(i, 0, root_ref.at[0]).wait()
        fetch(i, 1, gain_ref.at[0]).wait()
        put(i).start()
        return carry

    def finish(i, carry):
        put(i).wait()
        return carry

    lax.fori_loop(0, count, pass_on, 0)
    lax.fori_loop(0, count, finish, 0)


def comm_kernel(
    listed, packet_ref, rows_ref, spread_ref, full_ref,
    mixed, rx_core, rx_y, plane, rx_z,
    core_s, core_r, y_s, y_r, z_s, z_r, back_s, back_r, x_s, x_r, pair_s, pair_r,
    mat_s, mat_r, twin_s, twin_r,
):
    column = lax.axis_index("gx")
    band = lax.axis_index("gy")
    core = lax.rem(column, 2)
    y = lax.rem(column // 2, RING)
    z = column // (2 * RING)
    partner = (z * RING + y) * 2 + 1 - core

    def at_y(step):
        return (z * RING + lax.rem(y + step, RING)) * 2 + core

    def at_z(step):
        return (lax.rem(z + step, RING) * RING + y) * 2 + core

    def at_x(step):
        return lax.rem(band + step, BANDS)

    def copy(src, dst, send, recv, gx, gy):
        return pltpu.make_async_remote_copy(
            src_ref=src, dst_ref=dst, send_sem=send, recv_sem=recv,
            device_id=(gx, gy), device_id_type=MESH,
        )

    barrier = pltpu.get_barrier_semaphore()
    peers = [(partner, band)]
    peers += [(at_y(d), band) for d in range(1, RING)]
    peers += [(at_z(d), band) for d in range(1, RING)]
    peers += [(column, at_x(d)) for d in range(1, BANDS)]
    for peer in peers:
        pl.semaphore_signal(barrier, inc=1, device_id=peer, device_id_type=MESH)
    pl.semaphore_wait(barrier, len(peers))

    mine = pl.ds(pl.multiple_of(core * HALF, 8), HALF)
    other = pl.ds(pl.multiple_of((1 - core) * HALF, 8), HALF)
    sends = []

    def go(descriptor):
        descriptor.start()
        sends.append(descriptor)

    swap = copy(packet_ref.at[:, other, :], rx_core, core_s, core_r, partner, band)
    go(swap)

    def my_rows(of):
        return pl.ds(pl.multiple_of(of * QUARTER, 8), QUARTER)

    source = rows_ref.at[pl.ds(0, listed), core]
    for d in range(1, BANDS):
        go(copy(source, full_ref.at[:, core, my_rows(band), :], mat_s.at[d - 1], mat_r.at[d - 1], column, at_x(d)))

    swap.wait_recv()
    mixed[...] = packet_ref[:, mine, :] + rx_core[...]

    for d in (4, 3, 5, 2, 6, 1, 7):
        go(copy(mixed.at[lax.rem(y + d, RING)], rx_y.at[d - 1], y_s.at[d - 1], y_r.at[d - 1], at_y(d), band))
    part = mixed[y]
    for d in (1, 7, 2, 6, 3, 5, 4):
        copy(mixed.at[0], rx_y.at[d - 1], y_s.at[d - 1], y_r.at[d - 1], at_y(RING - d), band).wait_recv()
        part = part + rx_y[d - 1]
    plane[...] = part

    for d in (4, 3, 5, 2, 6, 1, 7):
        go(copy(plane, rx_z.at[d - 1], z_s.at[d - 1], z_r.at[d - 1], at_z(d), band))
    for d in (1, 7, 2, 6, 3, 5, 4):
        copy(plane, rx_z.at[d - 1], z_s.at[d - 1], z_r.at[d - 1], at_z(RING - d), band).wait_recv()
        part = part + rx_z[d - 1]
    spread_ref[band, y, mine, :] = part

    def slot(x, home):
        return spread_ref.at[x, home, mine, :]

    own = slot(band, y)
    for d in (4, 3, 5, 2, 6, 1, 7):
        go(copy(own, own, back_s.at[d - 1], back_r.at[d - 1], at_y(d), band))

    homes = [(0, y)] + [(d, lax.rem(y + RING - d, RING)) for d in (1, 7, 2, 6, 3, 5, 4)]
    for d, home in homes:
        here = slot(band, home)
        if d:
            copy(here, here, back_s.at[d - 1], back_r.at[d - 1], at_y(RING - d), band).wait_recv()
        for e in (2, 1, 3):
            go(copy(here, here, x_s.at[e - 1, d], x_r.at[e - 1, d], column, at_x(e)))
        go(copy(here, here, pair_s.at[0, d], pair_r.at[0, d], partner, band))
    for d, home in homes:
        for e in (1, 3, 2):
            here = slot(at_x(BANDS - e), home)
            copy(here, here, x_s.at[e - 1, d], x_r.at[e - 1, d], column, at_x(BANDS - e)).wait_recv()
            go(copy(here, here, pair_s.at[e, d], pair_r.at[e, d], partner, band))

    for d in (1, 3, 2):
        came = full_ref.at[:, core, my_rows(at_x(BANDS - d)), :]
        copy(came, came, mat_s.at[d - 1], mat_r.at[d - 1], column, at_x(BANDS - d)).wait_recv()
        go(copy(came, came, twin_s.at[d - 1], twin_r.at[d - 1], partner, band))

    for d, home in homes:
        for e in range(BANDS):
            there = spread_ref.at[at_x(BANDS - e), home, other, :]
            copy(there, there, pair_s.at[e, d], pair_r.at[e, d], partner, band).wait_recv()
    for d in (1, 3, 2):
        came = full_ref.at[:, 1 - core, my_rows(at_x(BANDS - d)), :]
        copy(came, came, twin_s.at[d - 1], twin_r.at[d - 1], partner, band).wait_recv()
    for descriptor in sends:
        descriptor.wait_send()


def solve_kernel(
    owner_s, table_s, anom_ref, mean_ref, cell_ref, spread_ref, rows_ref, full_ref,
    out_anom_ref, out_mean_ref,
    state, prior, mats, left_high, left_low, middle, mat_sem,
):
    column = lax.axis_index("gx")
    band = lax.axis_index("gy")
    count = table_s[0]

    def fetch(i, x, from_own):
        rows = pl.ds(x * QUARTER, QUARTER)
        source = rows_ref.at[i] if from_own else full_ref.at[i, :, rows, :]
        return pltpu.make_async_copy(source, mats.at[i, :, rows, :], mat_sem.at[i, x])

    def start(i, carry):
        for x in range(BANDS):
            @pl.when(band == x)
            def _():
                fetch(i, x, True).start()

            @pl.when(band != x)
            def _():
                fetch(i, x, False).start()

        return carry

    lax.fori_loop(0, count, start, 0)
    load_state(anom_ref, mean_ref, state)

    lane = lax.broadcasted_iota(jnp.int32, (ROWS, 128), 1)

    def assemble(i, carry):
        batch = table_s[1 + i]
        half = batch // PAIRS
        pair = lax.rem(batch, PAIRS)
        for x in (0, 2):
            first = pltpu.roll(spread_ref[x, pair], half * QUARTER, 1)
            second = pltpu.roll(spread_ref[x + 1, pair], (1 - half) * QUARTER, 1)
            prior[i, :, pl.ds(x * QUARTER, 128)] = jnp.where(lane < QUARTER, first, second)
        return carry

    lax.fori_loop(0, count, assemble, 0)

    spot = lax.broadcasted_iota(jnp.int32, (1, OBS), 1)
    scale = 1.0 / (7.0 * 32.0 * 79.0)

    def places(batch):
        cells = cell_ref[pl.ds(batch, 1), :]
        lon = owner_s[batch] * 2 + cells // 1024
        lat = (spot // QUARTER) * 8 + lax.rem(cells // 128, 8)
        return lon, lat

    def taper(lon_gap, lat_gap):
        lon_gap = jnp.minimum(lon_gap, NLON - lon_gap)
        return (
            jnp.maximum(7 - lon_gap, 0).astype(F32) * (NLAT - lat_gap).astype(F32) * scale
        )

    row = lax.broadcasted_iota(jnp.int32, (ROWS, OBS), 0)

    def assimilate(i, carry):
        batch = table_s[1 + i]
        slab = owner_s[batch]
        for x in range(BANDS):
            fetch(i, x, False).wait()
        z = prior[i]
        z_high, z_low = split(z)
        root_high, root_low = split(mats[i, 0])
        gain_high, gain_low = split(mats[i, 1])
        weighted = dot3(z_high, z_low, root_high, root_low)
        gained = dot3(z_high[MEMBERS:ROWS], z_low[MEMBERS:ROWS], gain_high, gain_low)
        weights = jnp.concatenate([weighted[0:MEMBERS], gained], axis=0)
        turned = jnp.transpose(jnp.where(row < MEMBERS, z, 0.0))
        turned_high, turned_low = split(turned)
        lon, lat = places(batch)
        both = jnp.concatenate(
            [jnp.broadcast_to(lon, (8, OBS)), jnp.broadcast_to(lat, (8, OBS))], axis=0
        ).astype(F32)
        upright = jnp.transpose(both).astype(jnp.int32)
        lon_col = upright[:, 0:1]
        lat_col = upright[:, 8:9]

        weights_high, weights_low = split(weights)

        def later(j, carry):
            other = table_s[1 + j]

            @pl.when(dist(owner_s[other], slab) <= REACH)
            def _():
                held = prior[j]
                held_high, held_low = split(held)
                covariance = dot3(turned_high, turned_low, held_high, held_low)
                lon_j, lat_j = places(other)
                gain = covariance * taper(jnp.abs(lon_col - lon_j), jnp.abs(lat_col - lat_j))
                gain_h, gain_l = split(gain)
                prior[j] = held - dot3(weights_high, weights_low, gain_h, gain_l)

            return carry

        lax.fori_loop(i + 1, count, later, 0)

        @pl.when(dist(slab, column) <= REACH)
        def _():
            for c in range(GROUPS):
                cell_lon = column * 2 + c // 8
                cell_lat = band * 8 + c % 8
                factor = taper(jnp.abs(lon - cell_lon), jnp.abs(lat - cell_lat))
                high, low = split(weights * factor)
                left_high[pl.ds(c * ROWS, ROWS), :] = high
                left_low[pl.ds(c * ROWS, ROWS), :] = low
            middle[...] = dot3(left_high[...], left_low[...], turned_high, turned_low)
            for c in range(GROUPS):
                lanes = pl.ds(c * 128, 128)
                block = state[:, lanes]
                m_high, m_low = split(middle[pl.ds(c * ROWS, ROWS), :])
                b_high, b_low = split(block)
                state[:, lanes] = block - dot3(m_high, m_low, b_high, b_low)

        return carry

    lax.fori_loop(0, count, assimilate, 0)

    for c in range(GROUPS):
        lanes = pl.ds(c * 128, 128)
        out_anom_ref[pl.ds(c, MEMBERS, stride=GROUPS), :] = state[0:MEMBERS, lanes]
        out_mean_ref[pl.ds(c, 1), :] = -state[pl.ds(MEMBERS, 1), lanes]


VMEM = pl.BlockSpec(memory_space=pltpu.VMEM)
SMEM = pl.BlockSpec(memory_space=pltpu.SMEM)
HBM = pl.BlockSpec(memory_space=pl.ANY)
DMA = pltpu.SemaphoreType.DMA


def exchange(listed, collective_id, packet, rows):
    return pl.pallas_call(
        functools.partial(comm_kernel, listed),
        name="exchange",
        out_shape=(
            jax.ShapeDtypeStruct((BANDS, PAIRS, ROWS, 128), F32),
            jax.ShapeDtypeStruct((listed, 2, OBS, OBS), F32),
        ),
        in_specs=[VMEM, HBM],
        out_specs=(VMEM, HBM),
        scratch_shapes=[
            pltpu.VMEM((PAIRS, HALF, 128), F32),
            pltpu.VMEM((PAIRS, HALF, 128), F32),
            pltpu.VMEM((RING - 1, HALF, 128), F32),
            pltpu.VMEM((HALF, 128), F32),
            pltpu.VMEM((RING - 1, HALF, 128), F32),
            DMA, DMA,
            DMA((RING - 1,)), DMA((RING - 1,)),
            DMA((RING - 1,)), DMA((RING - 1,)),
            DMA((RING - 1,)), DMA((RING - 1,)),
            DMA((BANDS - 1, PAIRS)), DMA((BANDS - 1, PAIRS)),
            DMA((BANDS, PAIRS)), DMA((BANDS, PAIRS)),
            DMA((BANDS - 1,)), DMA((BANDS - 1,)),
            DMA((BANDS - 1,)), DMA((BANDS - 1,)),
        ],
        compiler_params=pltpu.CompilerParams(collective_id=collective_id, has_side_effects=True),
    )(packet, rows)


def local(anomalies, state_mean, obs_value, obs_cell, owner, order, root_inv, gain_inv):
    flat = anomalies.reshape(MEMBERS * GROUPS, 128)
    mean = state_mean.reshape(GROUPS, 128)
    values = jnp.concatenate([obs_value, obs_value], axis=1)
    packet, rows, table = pl.pallas_call(
        prep_kernel,
        name="prep",
        out_shape=(
            jax.ShapeDtypeStruct((PAIRS, ROWS, 128), F32),
            jax.ShapeDtypeStruct((BATCHES, 2, QUARTER, OBS), F32),
            jax.ShapeDtypeStruct((32,), jnp.int32),
        ),
        in_specs=[SMEM, SMEM, VMEM, VMEM, VMEM, VMEM, HBM, HBM],
        out_specs=(VMEM, HBM, SMEM),
        scratch_shapes=[
            pltpu.VMEM((ROWS, CELLS), F32),
            pltpu.VMEM((BATCHES, 2, QUARTER, OBS), F32),
            pltpu.SMEM((BATCHES,), jnp.int32),
            DMA((BATCHES, 2)),
            DMA((BATCHES,)),
        ],
    )(order, owner, flat, mean, obs_cell, values, root_inv, gain_inv)
    spread, full = exchange(BATCHES, 1, packet, rows)
    out_flat, out_mean = pl.pallas_call(
        solve_kernel,
        name="solve",
        out_shape=(
            jax.ShapeDtypeStruct((MEMBERS * GROUPS, 128), F32),
            jax.ShapeDtypeStruct((GROUPS, 128), F32),
        ),
        in_specs=[SMEM, SMEM, VMEM, VMEM, VMEM, VMEM, HBM, HBM],
        out_specs=(VMEM, VMEM),
        scratch_shapes=[
            pltpu.VMEM((ROWS, CELLS), F32),
            pltpu.VMEM((BATCHES, ROWS, OBS), F32),
            pltpu.VMEM((BATCHES, 2, OBS, OBS), F32),
            pltpu.VMEM((GROUPS * ROWS, OBS), BF16),
            pltpu.VMEM((GROUPS * ROWS, OBS), BF16),
            pltpu.VMEM((GROUPS * ROWS, ROWS), F32),
            DMA((BATCHES, BANDS)),
        ],
    )(owner, table, flat, mean, obs_cell, spread, rows, full)
    return out_flat.reshape(anomalies.shape), out_mean.reshape(state_mean.shape)


def solution(mesh):
    return jax.shard_map(
        local,
        mesh=mesh,
        in_specs=(
            P(None, "gx", "gy", None),
            P("gx", "gy", None),
            P(None, "gy"),
            P(),
            P(),
            P(),
            P(None, "gy", None),
            P(None, "gy", None),
        ),
        out_specs=(P(None, "gx", "gy", None), P("gx", "gy", None)),
        check_vma=False,
    )
```

```python
import functools

import jax
import jax.numpy as jnp
from jax import lax
from jax.experimental import pallas as pl
from jax.experimental.pallas import tpu as pltpu
from jax.sharding import PartitionSpec as P

MEMBERS = 80
OBS = 256
BATCHES = 16
REACH = 3
SLABS = 128
BANDS = 4
NLON = 256
NLAT = 32
QUARTER = 64
CELLS = 2048
GROUPS = 16
ROWS = 96
HALF = 48
PAIRS = 8
RING = 8
MESH = pl.DeviceIdType.MESH
F32 = jnp.float32
BF16 = jnp.bfloat16


def dist(a, b):
    gap = jnp.abs(a - b)
    return jnp.minimum(gap, SLABS - gap)


def split(value):
    high = value.astype(BF16)
    return high, (value - high.astype(F32)).astype(BF16)


def dot(left, right):
    return jnp.dot(left, right, preferred_element_type=F32)


def dot3(left_high, left_low, right_high, right_low):
    return dot(left_high, right_high) + (dot(left_high, right_low) + dot(left_low, right_high))


def load_state(anom_ref, mean_ref, state):
    tail = lax.broadcasted_iota(jnp.int32, (16, 128), 0)
    for c in range(GROUPS):
        lanes = pl.ds(c * 128, 128)
        state[0:MEMBERS, lanes] = anom_ref[pl.ds(c, MEMBERS, stride=GROUPS), :]
        state[MEMBERS:ROWS, lanes] = jnp.where(tail == 0, -mean_ref[pl.ds(c, 1), :], 0.0)


def prep_kernel(
    order_s, owner_s, anom_ref, mean_ref, cell_ref, value_ref, root_ref, gain_ref,
    packet_ref, rows_ref, choice_ref, table_s,
    state, held, values, need_s, in_sem, out_sem,
):
    column = lax.axis_index("gx")
    band = lax.axis_index("gy")
    chip_low = column - lax.rem(column, 2)

    for t in reversed(range(BATCHES)):
        slab = owner_s[order_s[t]]
        near = jnp.minimum(dist(slab, chip_low), dist(slab, chip_low + 1)) <= REACH
        need = jnp.where(near, 1, 0)

        def later(s, need, slab=slab):
            linked = dist(owner_s[order_s[s]], slab) <= REACH
            return jnp.where(linked, need | need_s[s], need)

        need_s[t] = lax.fori_loop(t + 1, BATCHES, later, need)

    for i in range(BATCHES):
        table_s[1 + i] = -1

    def listing(t, count):
        @pl.when(need_s[t] == 1)
        def _():
            table_s[1 + count] = order_s[t]

        return count + need_s[t]

    count = lax.fori_loop(0, BATCHES, listing, 0)
    table_s[0] = count

    def fetch(i, which, source):
        return pltpu.make_async_copy(source, held.at[i, which], in_sem.at[i, which])

    def start_fetch(i, carry):
        batch = table_s[1 + i]
        fetch(i, 0, root_ref.at[batch]).start()
        fetch(i, 1, gain_ref.at[batch]).start()
        return carry

    lax.fori_loop(0, count, start_fetch, 0)

    at = lax.broadcasted_iota(jnp.int32, (2 * PAIRS, 128), 0)
    left = lax.broadcasted_iota(jnp.int32, (2 * PAIRS, 128), 1) < QUARTER
    slot = at // 2 + jnp.where(left == (lax.rem(at, 2) == 0), 0, PAIRS)
    for q in range(PAIRS):
        wanted = jnp.where(left, table_s[1 + 2 * q], table_s[2 + 2 * q])
        choice_ref[q] = jnp.where(wanted == slot, 1.0, 0.0)

    lane = lax.broadcasted_iota(jnp.int32, (8, 128), 1)
    low = 2 * lax.rem(lane, SLABS // 2)
    slabs = [owner_s[order_s[t]] for t in range(BATCHES)]
    needs = [None] * BATCHES
    total = jnp.zeros((8, 128), jnp.int32)
    far = jnp.zeros((8, 128), jnp.int32)
    own_plane = low // (2 * RING)
    for t in reversed(range(BATCHES)):
        near = jnp.minimum(dist(slabs[t], low), dist(slabs[t], low + 1)) <= REACH
        need = jnp.where(near, 1, 0)
        for s in range(t + 1, BATCHES):
            linked = jnp.where(dist(slabs[s], slabs[t]) <= REACH, 1, 0)
            need = need | (needs[s] * linked)
        needs[t] = need
        total = total + need
        apart = jnp.abs(own_plane - slabs[t] // (2 * RING))
        apart = jnp.minimum(apart, RING - apart)
        far = far | jnp.where(apart > 1, need, 0)
    table_s[BATCHES + 1] = jnp.max(total + far * (2 * BATCHES))
    values[:, 0:QUARTER] = value_ref[...]
    values[:, QUARTER:128] = value_ref[...]

    packet_ref[...] = jnp.zeros_like(packet_ref)
    load_state(anom_ref, mean_ref, state)

    def pick(batch, carry):
        @pl.when(owner_s[batch] == column)
        def _():
            half = batch // PAIRS
            pair = lax.rem(batch, PAIRS)
            cells = jnp.broadcast_to(cell_ref[pl.ds(batch, 1), :], (8, OBS))
            shift = lax.rem(half * QUARTER - band * QUARTER + OBS, OBS)
            mine = pltpu.roll(cells, shift, 1)[0:1, 0:128]
            spot = lax.broadcasted_iota(jnp.int32, (1, 128), 1)
            valid = (spot // QUARTER) == half
            mine = jnp.where(valid, mine, -1)
            picked = jnp.zeros((ROWS, 128), F32)
            step = 512
            for at in range(0, CELLS, step):
                ids = lax.broadcasted_iota(jnp.int32, (step, 128), 0) + at
                hot = jnp.where(ids == mine, 1.0, 0.0).astype(BF16)
                block = state[:, pl.ds(at, step)]
                high = block.astype(BF16)
                rest = block - high.astype(F32)
                mid = rest.astype(BF16)
                last = (rest - mid.astype(F32)).astype(BF16)
                picked = picked + (dot(high, hot) + (dot(mid, hot) + dot(last, hot)))
            row = lax.broadcasted_iota(jnp.int32, (ROWS, 128), 0)
            seen = jnp.where(valid, values[pl.ds(batch, 1), :], 0.0)
            picked = picked + jnp.where(row == MEMBERS, seen, 0.0)
            packet_ref[pair] = packet_ref[pair] + picked

        return carry

    lax.fori_loop(0, BATCHES, pick, 0)

    def put(i):
        return pltpu.make_async_copy(held.at[i], rows_ref.at[i], out_sem.at[i])

    def pass_on(i, carry):
        fetch(i, 0, root_ref.at[0]).wait()
        fetch(i, 1, gain_ref.at[0]).wait()
        put(i).start()
        return carry

    def finish(i, carry):
        put(i).wait()
        return carry

    lax.fori_loop(0, count, pass_on, 0)
    lax.fori_loop(0, count, finish, 0)


def comm_kernel(
    listed, planes, packet_ref, choice_ref, rows_ref, spread_ref, full_ref,
    mixed, rx_core, rx_y, plane, rx_z, slots,
    core_s, core_r, y_s, y_r, z_s, z_r, back_s, back_r, x_s, x_r, pair_s, pair_r,
    mat_s, mat_r, twin_s, twin_r,
):
    column = lax.axis_index("gx")
    band = lax.axis_index("gy")
    core = lax.rem(column, 2)
    y = lax.rem(column // 2, RING)
    z = column // (2 * RING)
    partner = (z * RING + y) * 2 + 1 - core

    def at_y(step):
        return (z * RING + lax.rem(y + step, RING)) * 2 + core

    def at_z(step):
        return (lax.rem(z + step, RING) * RING + y) * 2 + core

    def at_x(step):
        return lax.rem(band + step, BANDS)

    def copy(src, dst, send, recv, gx, gy):
        return pltpu.make_async_remote_copy(
            src_ref=src, dst_ref=dst, send_sem=send, recv_sem=recv,
            device_id=(gx, gy), device_id_type=MESH,
        )

    barrier = pltpu.get_barrier_semaphore()
    peers = [(partner, band)]
    peers += [(at_y(d), band) for d in range(1, RING)]
    peers += [(at_z(d), band) for d in planes]
    peers += [(column, at_x(d)) for d in range(1, BANDS)]
    for peer in peers:
        pl.semaphore_signal(barrier, inc=1, device_id=peer, device_id_type=MESH)
    pl.semaphore_wait(barrier, len(peers))

    mine = pl.ds(pl.multiple_of(core * HALF, 8), HALF)
    other = pl.ds(pl.multiple_of((1 - core) * HALF, 8), HALF)
    sends = []

    def go(descriptor):
        descriptor.start()
        sends.append(descriptor)

    swap = copy(packet_ref.at[:, other, :], rx_core, core_s, core_r, partner, band)
    go(swap)

    def my_rows(of):
        return pl.ds(pl.multiple_of(of * QUARTER, 8), QUARTER)

    source = rows_ref.at[pl.ds(0, listed), core]
    for d in range(1, BANDS):
        go(copy(source, full_ref.at[:, core, my_rows(band), :], mat_s.at[d - 1], mat_r.at[d - 1], column, at_x(d)))

    swap.wait_recv()
    mixed[...] = packet_ref[:, mine, :] + rx_core[...]

    for d in (4, 3, 5, 2, 6, 1, 7):
        go(copy(mixed.at[lax.rem(y + d, RING)], rx_y.at[d - 1], y_s.at[d - 1], y_r.at[d - 1], at_y(d), band))
    part = mixed[y]
    for d in (1, 7, 2, 6, 3, 5, 4):
        copy(mixed.at[0], rx_y.at[d - 1], y_s.at[d - 1], y_r.at[d - 1], at_y(RING - d), band).wait_recv()
        part = part + rx_y[d - 1]
    plane[...] = part

    for d in planes:
        go(copy(plane, rx_z.at[d - 1], z_s.at[d - 1], z_r.at[d - 1], at_z(d), band))
    for d in reversed(planes):
        copy(plane, rx_z.at[d - 1], z_s.at[d - 1], z_r.at[d - 1], at_z(RING - d), band).wait_recv()
        part = part + rx_z[d - 1]
    slots[y] = part
    own = slots.at[y]
    for d in (4, 3, 5, 2, 6, 1, 7):
        go(copy(own, own, back_s.at[d - 1], back_r.at[d - 1], at_y(d), band))
    for d in (1, 7, 2, 6, 3, 5, 4):
        here = slots.at[lax.rem(y + RING - d, RING)]
        copy(here, here, back_s.at[d - 1], back_r.at[d - 1], at_y(RING - d), band).wait_recv()

    chosen = [jnp.zeros((HALF, 128), F32)] * (listed // 2)
    for p in range(PAIRS):
        straight = slots[p]
        crossed = pltpu.roll(straight, QUARTER, 1)
        for q in range(listed // 2):
            chosen[q] = chosen[q] + (
                straight * choice_ref[q, 2 * p : 2 * p + 1, :]
                + crossed * choice_ref[q, 2 * p + 1 : 2 * p + 2, :]
            )
    for q in range(listed // 2):
        spread_ref[band, q, mine, :] = chosen[q]

    def part_of(x, rows):
        return spread_ref.at[x, :, rows, :]

    here = part_of(band, mine)
    for e in (2, 1, 3):
        go(copy(here, here, x_s.at[e - 1], x_r.at[e - 1], column, at_x(e)))
    go(copy(here, here, pair_s.at[0], pair_r.at[0], partner, band))
    for e in (1, 3, 2):
        here = part_of(at_x(BANDS - e), mine)
        copy(here, here, x_s.at[e - 1], x_r.at[e - 1], column, at_x(BANDS - e)).wait_recv()
        go(copy(here, here, pair_s.at[e], pair_r.at[e], partner, band))

    for d in (1, 3, 2):
        came = full_ref.at[:, core, my_rows(at_x(BANDS - d)), :]
        copy(came, came, mat_s.at[d - 1], mat_r.at[d - 1], column, at_x(BANDS - d)).wait_recv()
        go(copy(came, came, twin_s.at[d - 1], twin_r.at[d - 1], partner, band))

    for e in range(BANDS):
        there = part_of(at_x(BANDS - e), other)
        copy(there, there, pair_s.at[e], pair_r.at[e], partner, band).wait_recv()
    for d in (1, 3, 2):
        came = full_ref.at[:, 1 - core, my_rows(at_x(BANDS - d)), :]
        copy(came, came, twin_s.at[d - 1], twin_r.at[d - 1], partner, band).wait_recv()
    for descriptor in sends:
        descriptor.wait_send()


def solve_kernel(
    owner_s, table_s, anom_ref, mean_ref, cell_ref, spread_ref, rows_ref, full_ref,
    out_anom_ref, out_mean_ref,
    state, prior, mats, left_high, left_low, middle, mat_sem,
):
    column = lax.axis_index("gx")
    band = lax.axis_index("gy")
    count = table_s[0]

    def fetch(i, x, from_own):
        rows = pl.ds(x * QUARTER, QUARTER)
        source = rows_ref.at[i] if from_own else full_ref.at[i, :, rows, :]
        return pltpu.make_async_copy(source, mats.at[i, :, rows, :], mat_sem.at[i, x])

    def start(i, carry):
        for x in range(BANDS):
            @pl.when(band == x)
            def _():
                fetch(i, x, True).start()

            @pl.when(band != x)
            def _():
                fetch(i, x, False).start()

        return carry

    lax.fori_loop(0, count, start, 0)
    load_state(anom_ref, mean_ref, state)

    left = lax.broadcasted_iota(jnp.int32, (ROWS, 128), 1) < QUARTER
    for q in range(spread_ref.shape[1]):
        for x in (0, 2):
            first = spread_ref[x, q]
            second = spread_ref[x + 1, q]
            lanes = pl.ds(x * QUARTER, 128)
            prior[2 * q, :, lanes] = jnp.where(left, first, pltpu.roll(second, QUARTER, 1))
            prior[2 * q + 1, :, lanes] = jnp.where(left, pltpu.roll(first, QUARTER, 1), second)

    spot = lax.broadcasted_iota(jnp.int32, (1, OBS), 1)
    scale = 1.0 / (7.0 * 32.0 * 79.0)

    def places(batch):
        cells = cell_ref[pl.ds(batch, 1), :]
        lon = owner_s[batch] * 2 + cells // 1024
        lat = (spot // QUARTER) * 8 + lax.rem(cells // 128, 8)
        return lon, lat

    def taper(lon_gap, lat_gap):
        lon_gap = jnp.minimum(lon_gap, NLON - lon_gap)
        return (
            jnp.maximum(7 - lon_gap, 0).astype(F32) * (NLAT - lat_gap).astype(F32) * scale
        )

    row = lax.broadcasted_iota(jnp.int32, (ROWS, OBS), 0)

    def assimilate(i, carry):
        batch = table_s[1 + i]
        slab = owner_s[batch]
        for x in range(BANDS):
            fetch(i, x, False).wait()
        z = prior[i]
        z_high, z_low = split(z)
        root_high, root_low = split(mats[i, 0])
        gain_high, gain_low = split(mats[i, 1])
        weighted = dot3(z_high, z_low, root_high, root_low)
        gained = dot3(z_high[MEMBERS:ROWS], z_low[MEMBERS:ROWS], gain_high, gain_low)
        weights = jnp.concatenate([weighted[0:MEMBERS], gained], axis=0)
        turned = jnp.transpose(jnp.where(row < MEMBERS, z, 0.0))
        turned_high, turned_low = split(turned)
        lon, lat = places(batch)
        both = jnp.concatenate(
            [jnp.broadcast_to(lon, (8, OBS)), jnp.broadcast_to(lat, (8, OBS))], axis=0
        ).astype(F32)
        upright = jnp.transpose(both).astype(jnp.int32)
        lon_col = upright[:, 0:1]
        lat_col = upright[:, 8:9]

        weights_high, weights_low = split(weights)

        def later(j, carry):
            other = table_s[1 + j]

            @pl.when(dist(owner_s[other], slab) <= REACH)
            def _():
                held = prior[j]
                held_high, held_low = split(held)
                covariance = dot3(turned_high, turned_low, held_high, held_low)
                lon_j, lat_j = places(other)
                gain = covariance * taper(jnp.abs(lon_col - lon_j), jnp.abs(lat_col - lat_j))
                gain_h, gain_l = split(gain)
                prior[j] = held - dot3(weights_high, weights_low, gain_h, gain_l)

            return carry

        lax.fori_loop(i + 1, count, later, 0)

        @pl.when(dist(slab, column) <= REACH)
        def _():
            for c in range(GROUPS):
                cell_lon = column * 2 + c // 8
                cell_lat = band * 8 + c % 8
                factor = taper(jnp.abs(lon - cell_lon), jnp.abs(lat - cell_lat))
                high, low = split(weights * factor)
                left_high[pl.ds(c * ROWS, ROWS), :] = high
                left_low[pl.ds(c * ROWS, ROWS), :] = low
            middle[...] = dot3(left_high[...], left_low[...], turned_high, turned_low)
            for c in range(GROUPS):
                lanes = pl.ds(c * 128, 128)
                block = state[:, lanes]
                m_high, m_low = split(middle[pl.ds(c * ROWS, ROWS), :])
                b_high, b_low = split(block)
                state[:, lanes] = block - dot3(m_high, m_low, b_high, b_low)

        return carry

    lax.fori_loop(0, count, assimilate, 0)

    for c in range(GROUPS):
        lanes = pl.ds(c * 128, 128)
        out_anom_ref[pl.ds(c, MEMBERS, stride=GROUPS), :] = state[0:MEMBERS, lanes]
        out_mean_ref[pl.ds(c, 1), :] = -state[pl.ds(MEMBERS, 1), lanes]


VMEM = pl.BlockSpec(memory_space=pltpu.VMEM)
SMEM = pl.BlockSpec(memory_space=pltpu.SMEM)
HBM = pl.BlockSpec(memory_space=pl.ANY)
DMA = pltpu.SemaphoreType.DMA


def exchange(listed, planes, collective_id, packet, choice, rows):
    return pl.pallas_call(
        functools.partial(comm_kernel, listed, planes),
        name="exchange",
        out_shape=(
            jax.ShapeDtypeStruct((BANDS, listed // 2, ROWS, 128), F32),
            jax.ShapeDtypeStruct((listed, 2, OBS, OBS), F32),
        ),
        in_specs=[VMEM, VMEM, HBM],
        out_specs=(VMEM, HBM),
        scratch_shapes=[
            pltpu.VMEM((PAIRS, HALF, 128), F32),
            pltpu.VMEM((PAIRS, HALF, 128), F32),
            pltpu.VMEM((RING - 1, HALF, 128), F32),
            pltpu.VMEM((HALF, 128), F32),
            pltpu.VMEM((RING - 1, HALF, 128), F32),
            pltpu.VMEM((PAIRS, HALF, 128), F32),
            DMA, DMA,
            DMA((RING - 1,)), DMA((RING - 1,)),
            DMA((RING - 1,)), DMA((RING - 1,)),
            DMA((RING - 1,)), DMA((RING - 1,)),
            DMA((BANDS - 1,)), DMA((BANDS - 1,)),
            DMA((BANDS,)), DMA((BANDS,)),
            DMA((BANDS - 1,)), DMA((BANDS - 1,)),
            DMA((BANDS - 1,)), DMA((BANDS - 1,)),
        ],
        compiler_params=pltpu.CompilerParams(collective_id=collective_id, has_side_effects=True),
    )(packet, choice, rows)


def solve(listed, owner, table, flat, mean, obs_cell, spread, rows, full):
    return pl.pallas_call(
        solve_kernel,
        name="solve",
        out_shape=(
            jax.ShapeDtypeStruct((MEMBERS * GROUPS, 128), F32),
            jax.ShapeDtypeStruct((GROUPS, 128), F32),
        ),
        in_specs=[SMEM, SMEM, VMEM, VMEM, VMEM, VMEM, HBM, HBM],
        out_specs=(VMEM, VMEM),
        scratch_shapes=[
            pltpu.VMEM((ROWS, CELLS), F32),
            pltpu.VMEM((listed, ROWS, OBS), F32),
            pltpu.VMEM((listed, 2, OBS, OBS), F32),
            pltpu.VMEM((GROUPS * ROWS, OBS), BF16),
            pltpu.VMEM((GROUPS * ROWS, OBS), BF16),
            pltpu.VMEM((GROUPS * ROWS, ROWS), F32),
            DMA((listed, BANDS)),
        ],
    )(owner, table, flat, mean, obs_cell, spread, rows, full)


FEW = 6
NEXT_PLANES = (1, 7)
ALL_PLANES = (4, 3, 5, 2, 6, 1, 7)


def local(anomalies, state_mean, obs_value, obs_cell, owner, order, root_inv, gain_inv):
    flat = anomalies.reshape(MEMBERS * GROUPS, 128)
    mean = state_mean.reshape(GROUPS, 128)
    packet, rows, choice, table = pl.pallas_call(
        prep_kernel,
        name="prep",
        out_shape=(
            jax.ShapeDtypeStruct((PAIRS, ROWS, 128), F32),
            jax.ShapeDtypeStruct((BATCHES, 2, QUARTER, OBS), F32),
            jax.ShapeDtypeStruct((PAIRS, 2 * PAIRS, 128), F32),
            jax.ShapeDtypeStruct((32,), jnp.int32),
        ),
        in_specs=[SMEM, SMEM, VMEM, VMEM, VMEM, VMEM, HBM, HBM],
        out_specs=(VMEM, HBM, VMEM, SMEM),
        scratch_shapes=[
            pltpu.VMEM((ROWS, CELLS), F32),
            pltpu.VMEM((BATCHES, 2, QUARTER, OBS), F32),
            pltpu.VMEM((BATCHES, 128), F32),
            pltpu.SMEM((BATCHES,), jnp.int32),
            DMA((BATCHES, 2)),
            DMA((BATCHES,)),
        ],
    )(order, owner, flat, mean, obs_cell, obs_value, root_inv, gain_inv)

    def finish(listed, planes, collective_id):
        spread, full = exchange(listed, planes, collective_id, packet, choice, rows)
        return solve(listed, owner, table, flat, mean, obs_cell, spread, rows, full)

    out_flat, out_mean = lax.cond(
        table[BATCHES + 1] <= FEW,
        lambda: finish(FEW, NEXT_PLANES, 1),
        lambda: finish(BATCHES, ALL_PLANES, 2),
    )
    return out_flat.reshape(anomalies.shape), out_mean.reshape(state_mean.shape)


def solution(mesh):
    return jax.shard_map(
        local,
        mesh=mesh,
        in_specs=(
            P(None, "gx", "gy", None),
            P("gx", "gy", None),
            P(None, "gy"),
            P(),
            P(),
            P(),
            P(None, "gy", None),
            P(None, "gy", None),
        ),
        out_specs=(P(None, "gx", "gy", None), P("gx", "gy", None)),
        check_vma=False,
    )
```

```python
import functools

import jax
import jax.numpy as jnp
from jax import lax
from jax.experimental import pallas as pl
from jax.experimental.pallas import tpu as pltpu
from jax.sharding import PartitionSpec as P

MEMBERS = 80
OBS = 256
BATCHES = 16
REACH = 3
SLABS = 128
BANDS = 4
NLON = 256
NLAT = 32
QUARTER = 64
CELLS = 2048
GROUPS = 16
ROWS = 96
HALF = 48
PAIRS = 8
RING = 8
FEW = 4
MORE = 6
SOME = 8
GRANT = 24 * 1024 * 1024
NEXT_PLANES = (1, 7)
ALL_PLANES = (4, 3, 5, 2, 6, 1, 7)
MESH = pl.DeviceIdType.MESH
F32 = jnp.float32
BF16 = jnp.bfloat16


def dist(a, b):
    gap = jnp.abs(a - b)
    return jnp.minimum(gap, SLABS - gap)


def split(value):
    high = value.astype(BF16)
    return high, (value - high.astype(F32)).astype(BF16)


def dot(left, right):
    return jnp.dot(left, right, preferred_element_type=F32)


def dot3(left_high, left_low, right_high, right_low):
    return dot(left_high, right_high) + (dot(left_high, right_low) + dot(left_low, right_high))


def prep_kernel(
    order_s, owner_s, anom_ref, mean_ref, cell_ref, value_ref, root_ref, gain_ref,
    packet_ref, lone_ref, rows_ref, choice_ref, direct_ref, state, table_s, branch_s,
    raw, values, rank_s, code_s, raw_sem, in_sem,
):
    column = lax.axis_index("gx")
    band = lax.axis_index("gy")
    load = pltpu.make_async_copy(anom_ref, raw, raw_sem)
    load.start()

    lane = lax.broadcasted_iota(jnp.int32, (8, 128), 1)
    low = 2 * lax.rem(lane, SLABS // 2)
    own_plane = low // (2 * RING)
    batches = [order_s[t] for t in range(BATCHES)]
    slabs = [owner_s[batches[t]] for t in range(BATCHES)]
    needs = [None] * BATCHES
    bits = jnp.zeros((8, 128), jnp.int32)
    total = jnp.zeros((8, 128), jnp.int32)
    far = jnp.zeros((8, 128), jnp.int32)
    for t in reversed(range(BATCHES)):
        near = jnp.minimum(dist(slabs[t], low), dist(slabs[t], low + 1)) <= REACH
        need = jnp.where(near, 1, 0)
        for s in range(t + 1, BATCHES):
            linked = jnp.where(dist(slabs[s], slabs[t]) <= REACH, 1, 0)
            need = need | (needs[s] * linked)
        needs[t] = need
        bits = bits + need * (1 << t)
        total = total + need
        apart = jnp.abs(own_plane - slabs[t] // (2 * RING))
        apart = jnp.minimum(apart, RING - apart)
        far = far | jnp.where(apart > 1, need, 0)
    mine = jnp.max(jnp.where(lane == column // 2, bits, 0))

    deepest = 0
    codes = []
    for t in range(BATCHES):
        rank = 0
        for s in range(t):
            rank = rank + jnp.where(slabs[s] // 2 == slabs[t] // 2, 1, 0)
        rank_s[batches[t]] = rank
        deepest = jnp.maximum(deepest, rank)
        step = lax.rem(slabs[t] // (2 * RING) - column // (2 * RING) + RING, RING)
        step = jnp.where(step == RING - 1, 2, step)
        codes.append((step * RING + lax.rem(slabs[t] // 2, RING)) * 2 + rank)

    for i in range(BATCHES):
        table_s[1 + i] = -1
        code_s[i] = -1
    count = 0
    for t in range(BATCHES):
        flag = lax.rem(mine // (1 << t), 2)

        @pl.when(flag == 1)
        def _(t=t, count=count):
            table_s[1 + count] = batches[t]
            code_s[count] = codes[t]

        count = count + flag
    table_s[0] = count

    def fetch(i, which, source):
        return pltpu.make_async_copy(source, rows_ref.at[i, which], in_sem.at[i, which])

    def start_fetch(i, carry):
        batch = table_s[1 + i]
        fetch(i, 0, root_ref.at[batch]).start()
        fetch(i, 1, gain_ref.at[batch]).start()
        return carry

    lax.fori_loop(0, count, start_fetch, 0)
    longest = jnp.max(total + far * (2 * BATCHES))
    branch_s[0] = jnp.where(
        longest > SOME, 3, jnp.where((deepest > 1) | (longest > MORE), 2, jnp.where(longest > FEW, 1, 0))
    )

    at = lax.broadcasted_iota(jnp.int32, (2 * PAIRS, 128), 0)
    left = lax.broadcasted_iota(jnp.int32, (2 * PAIRS, 128), 1) < QUARTER
    slot = at // 2 + jnp.where(left == (lax.rem(at, 2) == 0), 0, PAIRS)
    for q in range(PAIRS):
        wanted = jnp.where(left, table_s[1 + 2 * q], table_s[2 + 2 * q])
        choice_ref[q] = jnp.where(wanted == slot, 1.0, 0.0)
    at = lax.broadcasted_iota(jnp.int32, (6 * RING, 128), 0)
    left = lax.broadcasted_iota(jnp.int32, (6 * RING, 128), 1) < QUARTER
    slot = at // 2 * 2 + jnp.where(left == (lax.rem(at, 2) == 0), 0, 1)
    for q in range(MORE // 2):
        wanted = jnp.where(left, code_s[2 * q], code_s[1 + 2 * q])
        direct_ref[q] = jnp.where(wanted == slot, 1.0, 0.0)

    values[:, 0:QUARTER] = value_ref[...]
    values[:, QUARTER:128] = value_ref[...]
    packet_ref[...] = jnp.zeros_like(packet_ref)
    lone_ref[...] = jnp.zeros_like(lone_ref)

    tail = lax.broadcasted_iota(jnp.int32, (16, 128), 0)
    for c in range(GROUPS):
        lanes = pl.ds(c * 128, 128)
        state[MEMBERS:ROWS, lanes] = jnp.where(tail == 0, -mean_ref[pl.ds(c, 1), :], 0.0)
    load.wait()
    for c in range(GROUPS):
        state[0:MEMBERS, pl.ds(c * 128, 128)] = raw[pl.ds(c, MEMBERS, stride=GROUPS), :]

    def pick(batch, carry):
        @pl.when(owner_s[batch] == column)
        def _():
            half = batch // PAIRS
            pair = lax.rem(batch, PAIRS)
            cells = jnp.broadcast_to(cell_ref[pl.ds(batch, 1), :], (8, OBS))
            shift = lax.rem(half * QUARTER - band * QUARTER + OBS, OBS)
            mine = pltpu.roll(cells, shift, 1)[0:1, 0:128]
            spot = lax.broadcasted_iota(jnp.int32, (1, 128), 1)
            valid = (spot // QUARTER) == half
            mine = jnp.where(valid, mine, -1)
            picked = jnp.zeros((ROWS, 128), F32)
            step = 512
            for at in range(0, CELLS, step):
                ids = lax.broadcasted_iota(jnp.int32, (step, 128), 0) + at
                hot = jnp.where(ids == mine, 1.0, 0.0).astype(BF16)
                block = state[:, pl.ds(at, step)]
                high = block.astype(BF16)
                rest = block - high.astype(F32)
                mid = rest.astype(BF16)
                last = (rest - mid.astype(F32)).astype(BF16)
                picked = picked + (dot(high, hot) + (dot(mid, hot) + dot(last, hot)))
            row = lax.broadcasted_iota(jnp.int32, (ROWS, 128), 0)
            seen = jnp.where(valid, values[pl.ds(batch, 1), :], 0.0)
            picked = picked + jnp.where(row == MEMBERS, seen, 0.0)
            packet_ref[pair] = packet_ref[pair] + picked
            turn = lax.rem(rank_s[batch] + half, 2) * QUARTER
            lone_ref[...] = lone_ref[...] + pltpu.roll(picked, turn, 1)

        return carry

    lax.fori_loop(0, BATCHES, pick, 0)

    def finish(i, carry):
        fetch(i, 0, root_ref.at[0]).wait()
        fetch(i, 1, gain_ref.at[0]).wait()
        return carry

    lax.fori_loop(0, count, finish, 0)


def comm_kernel(
    listed, planes, packet_ref, choice_ref, rows_ref, spread_ref, full_ref,
    mixed, rx_core, rx_y, plane, rx_z, slots,
    core_s, core_r, y_s, y_r, z_s, z_r, back_s, back_r, x_s, x_r, pair_s, pair_r,
    mat_s, mat_r, far_s, far_r, twin_s, twin_r,
):
    column = lax.axis_index("gx")
    band = lax.axis_index("gy")
    core = lax.rem(column, 2)
    y = lax.rem(column // 2, RING)
    z = column // (2 * RING)
    partner = (z * RING + y) * 2 + 1 - core

    def at_y(step):
        return (z * RING + lax.rem(y + step, RING)) * 2 + core

    def at_z(step):
        return (lax.rem(z + step, RING) * RING + y) * 2 + core

    def at_x(step):
        return lax.rem(band + step, BANDS)

    def copy(src, dst, send, recv, gx, gy):
        return pltpu.make_async_remote_copy(
            src_ref=src, dst_ref=dst, send_sem=send, recv_sem=recv,
            device_id=(gx, gy), device_id_type=MESH,
        )

    barrier = pltpu.get_barrier_semaphore()
    peers = [(partner, band)]
    peers += [(at_y(d), band) for d in range(1, RING)]
    peers += [(at_z(d), band) for d in planes]
    peers += [(column, at_x(d)) for d in range(1, BANDS)]
    for peer in peers:
        pl.semaphore_signal(barrier, inc=1, device_id=peer, device_id_type=MESH)
    pl.semaphore_wait(barrier, len(peers))

    mine = pl.ds(pl.multiple_of(core * HALF, 8), HALF)
    other = pl.ds(pl.multiple_of((1 - core) * HALF, 8), HALF)
    sends = []

    def go(descriptor):
        descriptor.start()
        sends.append(descriptor)

    swap = copy(packet_ref.at[:, other, :], rx_core, core_s, core_r, partner, band)
    go(swap)

    def my_rows(of):
        return pl.ds(pl.multiple_of(of * QUARTER, 8), QUARTER)

    def landed(step, part, core):
        return full_ref.at[pl.ds(part * few, few), core, my_rows(at_x(step)), :]

    few = listed // 2
    for way, part in ((0, 0), (1, 1), (0, 1), (1, 0)):
        source = rows_ref.at[pl.ds(part * few, few), core]
        go(copy(source, landed(0, part, core), mat_s.at[way, part], mat_r.at[way, part], column, at_x(1 if way == 0 else 3)))

    def arrived(way, part, step):
        here = landed(step, part, core)
        copy(here, here, mat_s.at[way, part], mat_r.at[way, part], column, at_x(3 if way == 0 else 1)).wait_recv()
        return here

    def to_twin(here, index):
        go(copy(here, here, twin_s.at[index], twin_r.at[index], partner, band))

    swap.wait_recv()
    mixed[...] = packet_ref[:, mine, :] + rx_core[...]

    for d in (4, 3, 5, 2, 6, 1, 7):
        go(copy(mixed.at[lax.rem(y + d, RING)], rx_y.at[d - 1], y_s.at[d - 1], y_r.at[d - 1], at_y(d), band))
    part = mixed[y]
    for d in (1, 7, 2, 6, 3, 5, 4):
        copy(mixed.at[0], rx_y.at[d - 1], y_s.at[d - 1], y_r.at[d - 1], at_y(RING - d), band).wait_recv()
        part = part + rx_y[d - 1]
    plane[...] = part
    from_left = arrived(0, 0, 3)
    from_right = arrived(1, 1, 1)

    for d in planes:
        go(copy(plane, rx_z.at[d - 1], z_s.at[d - 1], z_r.at[d - 1], at_z(d), band))
    go(copy(from_left, from_left, far_s.at[0], far_r.at[0], column, at_x(1)))
    go(copy(from_right, from_right, far_s.at[1], far_r.at[1], column, at_x(3)))
    to_twin(from_left, 0)
    to_twin(from_right, 1)
    for d in reversed(planes):
        copy(plane, rx_z.at[d - 1], z_s.at[d - 1], z_r.at[d - 1], at_z(RING - d), band).wait_recv()
        part = part + rx_z[d - 1]
    slots[y] = part
    own = slots.at[y]
    for d in (4, 3, 5, 2, 6, 1, 7):
        go(copy(own, own, back_s.at[d - 1], back_r.at[d - 1], at_y(d), band))
    to_twin(arrived(0, 1, 3), 2)
    to_twin(arrived(1, 0, 1), 3)
    for d in (1, 7, 2, 6, 3, 5, 4):
        here = slots.at[lax.rem(y + RING - d, RING)]
        copy(here, here, back_s.at[d - 1], back_r.at[d - 1], at_y(RING - d), band).wait_recv()

    chosen = [jnp.zeros((HALF, 128), F32)] * (listed // 2)
    for p in range(PAIRS):
        straight = slots[p]
        crossed = pltpu.roll(straight, QUARTER, 1)
        for q in range(listed // 2):
            chosen[q] = chosen[q] + (
                straight * choice_ref[q, 2 * p : 2 * p + 1, :]
                + crossed * choice_ref[q, 2 * p + 1 : 2 * p + 2, :]
            )
    for q in range(listed // 2):
        spread_ref[band, q, mine, :] = chosen[q]

    def part_of(x, rows):
        return spread_ref.at[x, :, rows, :]

    here = part_of(band, mine)
    for e in (2, 1, 3):
        go(copy(here, here, x_s.at[e - 1], x_r.at[e - 1], column, at_x(e)))
    go(copy(here, here, pair_s.at[0], pair_r.at[0], partner, band))
    for part in (0, 1):
        there = landed(2, part, core)
        copy(there, there, far_s.at[part], far_r.at[part], column, at_x(3 if part == 0 else 1)).wait_recv()
        to_twin(there, 4 + part)
    for e in (1, 3, 2):
        here = part_of(at_x(BANDS - e), mine)
        copy(here, here, x_s.at[e - 1], x_r.at[e - 1], column, at_x(BANDS - e)).wait_recv()
        go(copy(here, here, pair_s.at[e], pair_r.at[e], partner, band))

    for e in range(BANDS):
        there = part_of(at_x(BANDS - e), other)
        copy(there, there, pair_s.at[e], pair_r.at[e], partner, band).wait_recv()
    for index, step, part in ((0, 3, 0), (1, 1, 1), (2, 3, 1), (3, 1, 0), (4, 2, 0), (5, 2, 1)):
        there = landed(step, part, 1 - core)
        copy(there, there, twin_s.at[index], twin_r.at[index], partner, band).wait_recv()
    for descriptor in sends:
        descriptor.wait_send()


def direct_kernel(
    listed, lone_ref, direct_ref, rows_ref, spread_ref, full_ref,
    slots, rx_core,
    core_s, core_r, y_s, y_r, z_s, z_r, x_s, x_r, pair_s, pair_r,
    mat_s, mat_r, far_s, far_r, twin_s, twin_r,
):
    column = lax.axis_index("gx")
    band = lax.axis_index("gy")
    core = lax.rem(column, 2)
    y = lax.rem(column // 2, RING)
    z = column // (2 * RING)
    partner = (z * RING + y) * 2 + 1 - core

    def at_y(step):
        return (z * RING + lax.rem(y + step, RING)) * 2 + core

    def at_z(step):
        return (lax.rem(z + step, RING) * RING + y) * 2 + core

    def at_x(step):
        return lax.rem(band + step, BANDS)

    def copy(src, dst, send, recv, gx, gy):
        return pltpu.make_async_remote_copy(
            src_ref=src, dst_ref=dst, send_sem=send, recv_sem=recv,
            device_id=(gx, gy), device_id_type=MESH,
        )

    barrier = pltpu.get_barrier_semaphore()
    peers = [(partner, band)]
    peers += [(at_y(d), band) for d in range(1, RING)]
    peers += [(at_z(d), band) for d in (1, RING - 1)]
    peers += [(column, at_x(d)) for d in range(1, BANDS)]
    for peer in peers:
        pl.semaphore_signal(barrier, inc=1, device_id=peer, device_id_type=MESH)
    pl.semaphore_wait(barrier, len(peers))

    mine = pl.ds(pl.multiple_of(core * HALF, 8), HALF)
    other = pl.ds(pl.multiple_of((1 - core) * HALF, 8), HALF)
    sends = []

    def go(descriptor):
        descriptor.start()
        sends.append(descriptor)

    swap = copy(lone_ref.at[other, :], rx_core, core_s, core_r, partner, band)
    go(swap)

    def my_rows(of):
        return pl.ds(pl.multiple_of(of * QUARTER, 8), QUARTER)

    def landed(step, part, core):
        return full_ref.at[pl.ds(part * few, few), core, my_rows(at_x(step)), :]

    few = listed // 2
    for way, part in ((0, 0), (1, 1), (0, 1), (1, 0)):
        source = rows_ref.at[pl.ds(part * few, few), core]
        go(copy(source, landed(0, part, core), mat_s.at[way, part], mat_r.at[way, part], column, at_x(1 if way == 0 else 3)))

    def arrived(way, part, step):
        here = landed(step, part, core)
        copy(here, here, mat_s.at[way, part], mat_r.at[way, part], column, at_x(3 if way == 0 else 1)).wait_recv()
        return here

    def to_twin(here, index):
        go(copy(here, here, twin_s.at[index], twin_r.at[index], partner, band))

    swap.wait_recv()
    slots[0, y] = lone_ref[mine, :] + rx_core[...]

    def to_planes(home, d):
        here = slots.at[0, home]
        go(copy(here, slots.at[2, home], z_s.at[0, d], z_r.at[0, d], at_z(1), band))
        go(copy(here, slots.at[1, home], z_s.at[1, d], z_r.at[1, d], at_z(RING - 1), band))

    own = slots.at[0, y]
    for d in (4, 3, 5, 2, 6, 1, 7):
        go(copy(own, own, y_s.at[d - 1], y_r.at[d - 1], at_y(d), band))
    to_planes(y, 0)
    for d in (1, 7, 2, 6, 3, 5, 4):
        home = lax.rem(y + RING - d, RING)
        here = slots.at[0, home]
        copy(here, here, y_s.at[d - 1], y_r.at[d - 1], at_y(RING - d), band).wait_recv()
        to_planes(home, d)

    from_left = arrived(0, 0, 3)
    from_right = arrived(1, 1, 1)
    to_twin(from_left, 0)
    to_twin(from_right, 1)
    go(copy(from_left, from_left, far_s.at[0], far_r.at[0], column, at_x(1)))
    go(copy(from_right, from_right, far_s.at[1], far_r.at[1], column, at_x(3)))

    chosen = [jnp.zeros((HALF, 128), F32)] * (listed // 2)

    def choose(step, home):
        at = 2 * (step * RING + home)
        straight = slots[step, home]
        crossed = pltpu.roll(straight, QUARTER, 1)
        for q in range(listed // 2):
            chosen[q] = chosen[q] + (
                straight * direct_ref[q, pl.ds(at, 1), :] + crossed * direct_ref[q, pl.ds(at + 1, 1), :]
            )

    for home in range(RING):
        choose(0, home)
    for d in (0, 1, 7, 2, 6, 3, 5, 4):
        home = lax.rem(y + RING - d, RING)
        for step, way in ((2, 0), (1, 1)):
            here = slots.at[step, home]
            copy(here, here, z_s.at[way, d], z_r.at[way, d], at_z(RING - 1 if way == 0 else 1), band).wait_recv()
            choose(step, home)
    for q in range(listed // 2):
        spread_ref[band, q, mine, :] = chosen[q]

    def part_of(x, rows):
        return spread_ref.at[x, :, rows, :]

    here = part_of(band, mine)
    for e in (2, 1, 3):
        go(copy(here, here, x_s.at[e - 1], x_r.at[e - 1], column, at_x(e)))
    go(copy(here, here, pair_s.at[0], pair_r.at[0], partner, band))
    to_twin(arrived(0, 1, 3), 2)
    to_twin(arrived(1, 0, 1), 3)
    for e in (1, 3, 2):
        here = part_of(at_x(BANDS - e), mine)
        copy(here, here, x_s.at[e - 1], x_r.at[e - 1], column, at_x(BANDS - e)).wait_recv()
        go(copy(here, here, pair_s.at[e], pair_r.at[e], partner, band))
    for part in (0, 1):
        there = landed(2, part, core)
        copy(there, there, far_s.at[part], far_r.at[part], column, at_x(3 if part == 0 else 1)).wait_recv()
        to_twin(there, 4 + part)

    for e in range(BANDS):
        there = part_of(at_x(BANDS - e), other)
        copy(there, there, pair_s.at[e], pair_r.at[e], partner, band).wait_recv()
    for index, step, part in ((0, 3, 0), (1, 1, 1), (2, 3, 1), (3, 1, 0), (4, 2, 0), (5, 2, 1)):
        there = landed(step, part, 1 - core)
        copy(there, there, twin_s.at[index], twin_r.at[index], partner, band).wait_recv()
    for descriptor in sends:
        descriptor.wait_send()


def solve_kernel(
    owner_s, table_s, before_ref, cell_ref, spread_ref, rows_ref, full_ref,
    out_anom_ref, out_mean_ref,
    state, prior, mats, left_high, left_low, middle, mat_sem,
):
    column = lax.axis_index("gx")
    band = lax.axis_index("gy")
    count = table_s[0]

    def fetch(i, x, from_own):
        rows = pl.ds(x * QUARTER, QUARTER)
        source = rows_ref.at[i] if from_own else full_ref.at[i, :, rows, :]
        return pltpu.make_async_copy(source, mats.at[i, :, rows, :], mat_sem.at[i, x])

    def start(i, carry):
        for x in range(BANDS):
            @pl.when(band == x)
            def _():
                fetch(i, x, True).start()

            @pl.when(band != x)
            def _():
                fetch(i, x, False).start()

        return carry

    lax.fori_loop(0, count, start, 0)
    state[...] = before_ref[...]

    left = lax.broadcasted_iota(jnp.int32, (ROWS, 128), 1) < QUARTER
    for q in range(spread_ref.shape[1]):
        for x in (0, 2):
            first = spread_ref[x, q]
            second = spread_ref[x + 1, q]
            lanes = pl.ds(x * QUARTER, 128)
            prior[2 * q, :, lanes] = jnp.where(left, first, pltpu.roll(second, QUARTER, 1))
            prior[2 * q + 1, :, lanes] = jnp.where(left, pltpu.roll(first, QUARTER, 1), second)

    spot = lax.broadcasted_iota(jnp.int32, (1, OBS), 1)
    scale = 1.0 / (7.0 * 32.0 * 79.0)

    def places(batch):
        cells = cell_ref[pl.ds(batch, 1), :]
        lon = owner_s[batch] * 2 + cells // 1024
        lat = (spot // QUARTER) * 8 + lax.rem(cells // 128, 8)
        return lon, lat

    def taper(lon_gap, lat_gap):
        lon_gap = jnp.minimum(lon_gap, NLON - lon_gap)
        return (
            jnp.maximum(7 - lon_gap, 0).astype(F32) * (NLAT - lat_gap).astype(F32) * scale
        )

    row = lax.broadcasted_iota(jnp.int32, (ROWS, OBS), 0)

    def assimilate(i, carry):
        batch = table_s[1 + i]
        slab = owner_s[batch]
        for x in range(BANDS):
            fetch(i, x, False).wait()
        z = prior[i]
        z_high, z_low = split(z)
        root_high, root_low = split(mats[i, 0])
        gain_high, gain_low = split(mats[i, 1])
        weighted = dot3(z_high, z_low, root_high, root_low)
        gained = dot3(z_high[MEMBERS:ROWS], z_low[MEMBERS:ROWS], gain_high, gain_low)
        weights = jnp.concatenate([weighted[0:MEMBERS], gained], axis=0)
        turned = jnp.transpose(jnp.where(row < MEMBERS, z, 0.0))
        turned_high, turned_low = split(turned)
        lon, lat = places(batch)
        both = jnp.concatenate(
            [jnp.broadcast_to(lon, (8, OBS)), jnp.broadcast_to(lat, (8, OBS))], axis=0
        ).astype(F32)
        upright = jnp.transpose(both).astype(jnp.int32)
        lon_col = upright[:, 0:1]
        lat_col = upright[:, 8:9]

        weights_high, weights_low = split(weights)

        def later(j, carry):
            other = table_s[1 + j]

            @pl.when(dist(owner_s[other], slab) <= REACH)
            def _():
                held = prior[j]
                held_high, held_low = split(held)
                covariance = dot3(turned_high, turned_low, held_high, held_low)
                lon_j, lat_j = places(other)
                gain = covariance * taper(jnp.abs(lon_col - lon_j), jnp.abs(lat_col - lat_j))
                gain_h, gain_l = split(gain)
                prior[j] = held - dot3(weights_high, weights_low, gain_h, gain_l)

            return carry

        lax.fori_loop(i + 1, count, later, 0)

        @pl.when(dist(slab, column) <= REACH)
        def _():
            for c in range(GROUPS):
                cell_lon = column * 2 + c // 8
                cell_lat = band * 8 + c % 8
                factor = taper(jnp.abs(lon - cell_lon), jnp.abs(lat - cell_lat))
                high, low = split(weights * factor)
                left_high[pl.ds(c * ROWS, ROWS), :] = high
                left_low[pl.ds(c * ROWS, ROWS), :] = low
            middle[...] = dot3(left_high[...], left_low[...], turned_high, turned_low)
            for c in range(GROUPS):
                lanes = pl.ds(c * 128, 128)
                block = state[:, lanes]
                m_high, m_low = split(middle[pl.ds(c * ROWS, ROWS), :])
                b_high, b_low = split(block)
                state[:, lanes] = block - dot3(m_high, m_low, b_high, b_low)

        return carry

    lax.fori_loop(0, count, assimilate, 0)

    for c in range(GROUPS):
        lanes = pl.ds(c * 128, 128)
        out_anom_ref[pl.ds(c, MEMBERS, stride=GROUPS), :] = state[0:MEMBERS, lanes]
        out_mean_ref[pl.ds(c, 1), :] = -state[pl.ds(MEMBERS, 1), lanes]


VMEM = pl.BlockSpec(memory_space=pltpu.VMEM)
SMEM = pl.BlockSpec(memory_space=pltpu.SMEM)
HBM = pl.BlockSpec(memory_space=pl.ANY)
DMA = pltpu.SemaphoreType.DMA


def exchange(listed, planes, collective_id, packet, choice, rows):
    return pl.pallas_call(
        functools.partial(comm_kernel, listed, planes),
        name="exchange",
        out_shape=(
            jax.ShapeDtypeStruct((BANDS, listed // 2, ROWS, 128), F32),
            jax.ShapeDtypeStruct((listed, 2, OBS, OBS), F32),
        ),
        in_specs=[VMEM, VMEM, HBM],
        out_specs=(VMEM, HBM),
        scratch_shapes=[
            pltpu.VMEM((PAIRS, HALF, 128), F32),
            pltpu.VMEM((PAIRS, HALF, 128), F32),
            pltpu.VMEM((RING - 1, HALF, 128), F32),
            pltpu.VMEM((HALF, 128), F32),
            pltpu.VMEM((RING - 1, HALF, 128), F32),
            pltpu.VMEM((PAIRS, HALF, 128), F32),
            DMA, DMA,
            DMA((RING - 1,)), DMA((RING - 1,)),
            DMA((RING - 1,)), DMA((RING - 1,)),
            DMA((RING - 1,)), DMA((RING - 1,)),
            DMA((BANDS - 1,)), DMA((BANDS - 1,)),
            DMA((BANDS,)), DMA((BANDS,)),
            DMA((2, 2)), DMA((2, 2)),
            DMA((2,)), DMA((2,)),
            DMA((6,)), DMA((6,)),
        ],
        compiler_params=pltpu.CompilerParams(collective_id=collective_id, has_side_effects=True, vmem_limit_bytes=GRANT),
    )(packet, choice, rows)


def direct(listed, collective_id, lone, choice, rows):
    return pl.pallas_call(
        functools.partial(direct_kernel, listed),
        name="direct",
        out_shape=(
            jax.ShapeDtypeStruct((BANDS, listed // 2, ROWS, 128), F32),
            jax.ShapeDtypeStruct((listed, 2, OBS, OBS), F32),
        ),
        in_specs=[VMEM, VMEM, HBM],
        out_specs=(VMEM, HBM),
        scratch_shapes=[
            pltpu.VMEM((3, RING, HALF, 128), F32),
            pltpu.VMEM((HALF, 128), F32),
            DMA, DMA,
            DMA((RING - 1,)), DMA((RING - 1,)),
            DMA((2, RING)), DMA((2, RING)),
            DMA((BANDS - 1,)), DMA((BANDS - 1,)),
            DMA((BANDS,)), DMA((BANDS,)),
            DMA((2, 2)), DMA((2, 2)),
            DMA((2,)), DMA((2,)),
            DMA((6,)), DMA((6,)),
        ],
        compiler_params=pltpu.CompilerParams(collective_id=collective_id, has_side_effects=True, vmem_limit_bytes=GRANT),
    )(lone, choice, rows)


def solve(listed, owner, table, state, obs_cell, spread, rows, full):
    return pl.pallas_call(
        solve_kernel,
        name="solve",
        out_shape=(
            jax.ShapeDtypeStruct((MEMBERS * GROUPS, 128), F32),
            jax.ShapeDtypeStruct((GROUPS, 128), F32),
        ),
        in_specs=[SMEM, SMEM, VMEM, VMEM, VMEM, HBM, HBM],
        out_specs=(VMEM, VMEM),
        scratch_shapes=[
            pltpu.VMEM((ROWS, CELLS), F32),
            pltpu.VMEM((listed, ROWS, OBS), F32),
            pltpu.VMEM((listed, 2, OBS, OBS), F32),
            pltpu.VMEM((GROUPS * ROWS, OBS), BF16),
            pltpu.VMEM((GROUPS * ROWS, OBS), BF16),
            pltpu.VMEM((GROUPS * ROWS, ROWS), F32),
            DMA((listed, BANDS)),
        ],
        compiler_params=pltpu.CompilerParams(vmem_limit_bytes=GRANT),
    )(owner, table, state, obs_cell, spread, rows, full)


def local(anomalies, state_mean, obs_value, obs_cell, owner, order, root_inv, gain_inv):
    flat = anomalies.reshape(MEMBERS * GROUPS, 128)
    mean = state_mean.reshape(GROUPS, 128)
    packet, lone, rows, choice, near_choice, state, table, branch = pl.pallas_call(
        prep_kernel,
        name="prep",
        out_shape=(
            jax.ShapeDtypeStruct((PAIRS, ROWS, 128), F32),
            jax.ShapeDtypeStruct((ROWS, 128), F32),
            jax.ShapeDtypeStruct((BATCHES, 2, QUARTER, OBS), F32),
            jax.ShapeDtypeStruct((PAIRS, 2 * PAIRS, 128), F32),
            jax.ShapeDtypeStruct((MORE // 2, 6 * RING, 128), F32),
            jax.ShapeDtypeStruct((ROWS, CELLS), F32),
            jax.ShapeDtypeStruct((32,), jnp.int32),
            jax.ShapeDtypeStruct((1,), jnp.int32),
        ),
        in_specs=[SMEM, SMEM, HBM, VMEM, VMEM, VMEM, HBM, HBM],
        out_specs=(VMEM, VMEM, HBM, VMEM, VMEM, VMEM, SMEM, SMEM),
        scratch_shapes=[
            pltpu.VMEM((MEMBERS * GROUPS, 128), F32),
            pltpu.VMEM((BATCHES, 128), F32),
            pltpu.SMEM((BATCHES,), jnp.int32),
            pltpu.SMEM((BATCHES,), jnp.int32),
            DMA,
            DMA((BATCHES, 2)),
        ],
    )(order, owner, flat, mean, obs_cell, obs_value, root_inv, gain_inv)

    def near(listed, collective_id):
        spread, full = direct(listed, collective_id, lone, near_choice, rows)
        return solve(listed, owner, table, state, obs_cell, spread, rows, full)

    def wide(listed, planes, collective_id):
        spread, full = exchange(listed, planes, collective_id, packet, choice, rows)
        return solve(listed, owner, table, state, obs_cell, spread, rows, full)

    out_flat, out_mean = lax.switch(
        branch[0],
        (
            lambda: near(FEW, 1),
            lambda: near(MORE, 2),
            lambda: wide(SOME, NEXT_PLANES, 3),
            lambda: wide(BATCHES, ALL_PLANES, 4),
        ),
    )
    return out_flat.reshape(anomalies.shape), out_mean.reshape(state_mean.shape)


def solution(mesh):
    return jax.shard_map(
        local,
        mesh=mesh,
        in_specs=(
            P(None, "gx", "gy", None),
            P("gx", "gy", None),
            P(None, "gy"),
            P(),
            P(),
            P(),
            P(None, "gy", None),
            P(None, "gy", None),
        ),
        out_specs=(P(None, "gx", "gy", None), P("gx", "gy", None)),
        check_vma=False,
    )
```

```python
import functools

import jax
import jax.numpy as jnp
from jax import lax
from jax.experimental import pallas as pl
from jax.experimental.pallas import tpu as pltpu
from jax.sharding import PartitionSpec as P

MEMBERS = 80
OBS = 256
BATCHES = 16
REACH = 3
SLABS = 128
BANDS = 4
NLON = 256
NLAT = 32
QUARTER = 64
CELLS = 2048
GROUPS = 16
ROWS = 96
HALF = 48
PAIRS = 8
RING = 8
FEW = 4
MORE = 6
SOME = 8
WINDOW = 5
BUNDLE = 4
GRANT = 24 * 1024 * 1024
NEXT_PLANES = (1, 7)
ALL_PLANES = (4, 3, 5, 2, 6, 1, 7)
MESH = pl.DeviceIdType.MESH
F32 = jnp.float32
BF16 = jnp.bfloat16


def dist(a, b):
    gap = jnp.abs(a - b)
    return jnp.minimum(gap, SLABS - gap)


def split(value):
    high = value.astype(BF16)
    return high, (value - high.astype(F32)).astype(BF16)


def dot(left, right):
    return jnp.dot(left, right, preferred_element_type=F32)


def dot3(left_high, left_low, right_high, right_low):
    return dot(left_high, right_high) + (dot(left_high, right_low) + dot(left_low, right_high))


def prep_kernel(
    order_s, owner_s, anom_ref, mean_ref, cell_ref, value_ref, root_ref, gain_ref,
    packet_ref, lone_ref, rows_ref, choice_ref, direct_ref, state, table_s, branch_s,
    raw, values, rank_s, code_s, raw_sem, in_sem,
):
    column = lax.axis_index("gx")
    band = lax.axis_index("gy")
    load = pltpu.make_async_copy(anom_ref, raw, raw_sem)
    load.start()

    lane = lax.broadcasted_iota(jnp.int32, (8, 128), 1)
    low = 2 * lax.rem(lane, SLABS // 2)
    own_plane = low // (2 * RING)
    batches = [order_s[t] for t in range(BATCHES)]
    slabs = [owner_s[batches[t]] for t in range(BATCHES)]
    needs = [None] * BATCHES
    bits = jnp.zeros((8, 128), jnp.int32)
    total = jnp.zeros((8, 128), jnp.int32)
    far = jnp.zeros((8, 128), jnp.int32)
    beyond = jnp.zeros((8, 128), jnp.int32)
    for t in reversed(range(BATCHES)):
        near = jnp.minimum(dist(slabs[t], low), dist(slabs[t], low + 1)) <= REACH
        need = jnp.where(near, 1, 0)
        for s in range(t + 1, BATCHES):
            linked = jnp.where(dist(slabs[s], slabs[t]) <= REACH, 1, 0)
            need = need | (needs[s] * linked)
        needs[t] = need
        bits = bits + need * (1 << t)
        total = total + need
        apart = jnp.abs(own_plane - slabs[t] // (2 * RING))
        apart = jnp.minimum(apart, RING - apart)
        far = far | jnp.where(apart > 1, need, 0)
        chips = jnp.abs(low // 2 - slabs[t] // 2)
        chips = jnp.minimum(chips, SLABS // 2 - chips)
        beyond = beyond | jnp.where(chips > WINDOW, need, 0)
    mine = jnp.max(jnp.where(lane == column // 2, bits, 0))

    deepest = 0
    codes = []
    for t in range(BATCHES):
        rank = 0
        for s in range(t):
            rank = rank + jnp.where(slabs[s] // 2 == slabs[t] // 2, 1, 0)
        rank_s[batches[t]] = rank
        deepest = jnp.maximum(deepest, rank)
        step = lax.rem(slabs[t] // (2 * RING) - column // (2 * RING) + RING, RING)
        step = jnp.where(step == RING - 1, 2, step)
        codes.append((step * RING + lax.rem(slabs[t] // 2, RING)) * 2 + rank)

    for i in range(BATCHES):
        table_s[1 + i] = -1
        code_s[i] = -1
    count = 0
    for t in range(BATCHES):
        flag = lax.rem(mine // (1 << t), 2)

        @pl.when(flag == 1)
        def _(t=t, count=count):
            table_s[1 + count] = batches[t]
            code_s[count] = codes[t]

        count = count + flag
    table_s[0] = count

    def fetch(i, which, source):
        return pltpu.make_async_copy(source, rows_ref.at[i, which], in_sem.at[i, which])

    def start_fetch(i, carry):
        batch = table_s[1 + i]
        fetch(i, 0, root_ref.at[batch]).start()
        fetch(i, 1, gain_ref.at[batch]).start()
        return carry

    lax.fori_loop(0, count, start_fetch, 0)
    longest = jnp.max(total + far * (2 * BATCHES))
    branch_s[0] = jnp.where(
        longest > SOME,
        3,
        jnp.where((deepest > 1) | (jnp.max(beyond) > 0) | (longest > MORE), 2, jnp.where(longest > FEW, 1, 0))
    )

    at = lax.broadcasted_iota(jnp.int32, (2 * PAIRS, 128), 0)
    left = lax.broadcasted_iota(jnp.int32, (2 * PAIRS, 128), 1) < QUARTER
    slot = at // 2 + jnp.where(left == (lax.rem(at, 2) == 0), 0, PAIRS)
    for q in range(PAIRS):
        wanted = jnp.where(left, table_s[1 + 2 * q], table_s[2 + 2 * q])
        choice_ref[q] = jnp.where(wanted == slot, 1.0, 0.0)
    at = lax.broadcasted_iota(jnp.int32, (6 * RING, 128), 0)
    left = lax.broadcasted_iota(jnp.int32, (6 * RING, 128), 1) < QUARTER
    slot = at // 2 * 2 + jnp.where(left == (lax.rem(at, 2) == 0), 0, 1)
    for q in range(MORE // 2):
        wanted = jnp.where(left, code_s[2 * q], code_s[1 + 2 * q])
        direct_ref[q] = jnp.where(wanted == slot, 1.0, 0.0)

    values[:, 0:QUARTER] = value_ref[...]
    values[:, QUARTER:128] = value_ref[...]
    packet_ref[...] = jnp.zeros_like(packet_ref)
    lone_ref[...] = jnp.zeros_like(lone_ref)

    tail = lax.broadcasted_iota(jnp.int32, (16, 128), 0)
    for c in range(GROUPS):
        lanes = pl.ds(c * 128, 128)
        state[MEMBERS:ROWS, lanes] = jnp.where(tail == 0, -mean_ref[pl.ds(c, 1), :], 0.0)
    load.wait()
    for c in range(GROUPS):
        state[0:MEMBERS, pl.ds(c * 128, 128)] = raw[pl.ds(c, MEMBERS, stride=GROUPS), :]

    def pick(batch, carry):
        @pl.when(owner_s[batch] == column)
        def _():
            half = batch // PAIRS
            pair = lax.rem(batch, PAIRS)
            cells = jnp.broadcast_to(cell_ref[pl.ds(batch, 1), :], (8, OBS))
            shift = lax.rem(half * QUARTER - band * QUARTER + OBS, OBS)
            mine = pltpu.roll(cells, shift, 1)[0:1, 0:128]
            spot = lax.broadcasted_iota(jnp.int32, (1, 128), 1)
            valid = (spot // QUARTER) == half
            mine = jnp.where(valid, mine, -1)
            picked = jnp.zeros((ROWS, 128), F32)
            step = 512
            for at in range(0, CELLS, step):
                ids = lax.broadcasted_iota(jnp.int32, (step, 128), 0) + at
                hot = jnp.where(ids == mine, 1.0, 0.0).astype(BF16)
                block = state[:, pl.ds(at, step)]
                high = block.astype(BF16)
                rest = block - high.astype(F32)
                mid = rest.astype(BF16)
                last = (rest - mid.astype(F32)).astype(BF16)
                picked = picked + (dot(high, hot) + (dot(mid, hot) + dot(last, hot)))
            row = lax.broadcasted_iota(jnp.int32, (ROWS, 128), 0)
            seen = jnp.where(valid, values[pl.ds(batch, 1), :], 0.0)
            picked = picked + jnp.where(row == MEMBERS, seen, 0.0)
            packet_ref[pair] = packet_ref[pair] + picked
            turn = lax.rem(rank_s[batch] + half, 2) * QUARTER
            lone_ref[...] = lone_ref[...] + pltpu.roll(picked, turn, 1)

        return carry

    lax.fori_loop(0, BATCHES, pick, 0)

    def finish(i, carry):
        fetch(i, 0, root_ref.at[0]).wait()
        fetch(i, 1, gain_ref.at[0]).wait()
        return carry

    lax.fori_loop(0, count, finish, 0)


def comm_kernel(
    listed, planes, packet_ref, choice_ref, rows_ref, spread_ref, full_ref,
    mixed, rx_core, rx_y, plane, rx_z, slots,
    core_s, core_r, y_s, y_r, z_s, z_r, back_s, back_r, x_s, x_r, pair_s, pair_r,
    mat_s, mat_r, far_s, far_r, twin_s, twin_r,
):
    column = lax.axis_index("gx")
    band = lax.axis_index("gy")
    core = lax.rem(column, 2)
    y = lax.rem(column // 2, RING)
    z = column // (2 * RING)
    partner = (z * RING + y) * 2 + 1 - core

    def at_y(step):
        return (z * RING + lax.rem(y + step, RING)) * 2 + core

    def at_z(step):
        return (lax.rem(z + step, RING) * RING + y) * 2 + core

    def at_x(step):
        return lax.rem(band + step, BANDS)

    def copy(src, dst, send, recv, gx, gy):
        return pltpu.make_async_remote_copy(
            src_ref=src, dst_ref=dst, send_sem=send, recv_sem=recv,
            device_id=(gx, gy), device_id_type=MESH,
        )

    barrier = pltpu.get_barrier_semaphore()
    peers = [(partner, band)]
    peers += [(at_y(d), band) for d in range(1, RING)]
    peers += [(at_z(d), band) for d in planes]
    peers += [(column, at_x(d)) for d in range(1, BANDS)]
    for peer in peers:
        pl.semaphore_signal(barrier, inc=1, device_id=peer, device_id_type=MESH)
    pl.semaphore_wait(barrier, len(peers))

    mine = pl.ds(pl.multiple_of(core * HALF, 8), HALF)
    other = pl.ds(pl.multiple_of((1 - core) * HALF, 8), HALF)
    sends = []

    def go(descriptor):
        descriptor.start()
        sends.append(descriptor)

    swap = copy(packet_ref.at[:, other, :], rx_core, core_s, core_r, partner, band)
    go(swap)

    def my_rows(of):
        return pl.ds(pl.multiple_of(of * QUARTER, 8), QUARTER)

    def landed(step, part, core):
        return full_ref.at[pl.ds(part * few, few), core, my_rows(at_x(step)), :]

    few = listed // 2
    for way, part in ((0, 0), (1, 1), (0, 1), (1, 0)):
        source = rows_ref.at[pl.ds(part * few, few), core]
        go(copy(source, landed(0, part, core), mat_s.at[way, part], mat_r.at[way, part], column, at_x(1 if way == 0 else 3)))

    def arrived(way, part, step):
        here = landed(step, part, core)
        copy(here, here, mat_s.at[way, part], mat_r.at[way, part], column, at_x(3 if way == 0 else 1)).wait_recv()
        return here

    def to_twin(here, index):
        go(copy(here, here, twin_s.at[index], twin_r.at[index], partner, band))

    swap.wait_recv()
    mixed[...] = packet_ref[:, mine, :] + rx_core[...]

    for d in (4, 3, 5, 2, 6, 1, 7):
        go(copy(mixed.at[lax.rem(y + d, RING)], rx_y.at[d - 1], y_s.at[d - 1], y_r.at[d - 1], at_y(d), band))
    part = mixed[y]
    for d in (1, 7, 2, 6, 3, 5, 4):
        copy(mixed.at[0], rx_y.at[d - 1], y_s.at[d - 1], y_r.at[d - 1], at_y(RING - d), band).wait_recv()
        part = part + rx_y[d - 1]
    plane[...] = part
    from_left = arrived(0, 0, 3)
    from_right = arrived(1, 1, 1)

    for d in planes:
        go(copy(plane, rx_z.at[d - 1], z_s.at[d - 1], z_r.at[d - 1], at_z(d), band))
    go(copy(from_left, from_left, far_s.at[0], far_r.at[0], column, at_x(1)))
    go(copy(from_right, from_right, far_s.at[1], far_r.at[1], column, at_x(3)))
    to_twin(from_left, 0)
    to_twin(from_right, 1)
    for d in reversed(planes):
        copy(plane, rx_z.at[d - 1], z_s.at[d - 1], z_r.at[d - 1], at_z(RING - d), band).wait_recv()
        part = part + rx_z[d - 1]
    slots[y] = part
    own = slots.at[y]
    for d in (4, 3, 5, 2, 6, 1, 7):
        go(copy(own, own, back_s.at[d - 1], back_r.at[d - 1], at_y(d), band))
    to_twin(arrived(0, 1, 3), 2)
    to_twin(arrived(1, 0, 1), 3)
    for d in (1, 7, 2, 6, 3, 5, 4):
        here = slots.at[lax.rem(y + RING - d, RING)]
        copy(here, here, back_s.at[d - 1], back_r.at[d - 1], at_y(RING - d), band).wait_recv()

    chosen = [jnp.zeros((HALF, 128), F32)] * (listed // 2)
    for p in range(PAIRS):
        straight = slots[p]
        crossed = pltpu.roll(straight, QUARTER, 1)
        for q in range(listed // 2):
            chosen[q] = chosen[q] + (
                straight * choice_ref[q, 2 * p : 2 * p + 1, :]
                + crossed * choice_ref[q, 2 * p + 1 : 2 * p + 2, :]
            )
    for q in range(listed // 2):
        spread_ref[band, q, mine, :] = chosen[q]

    def part_of(x, rows):
        return spread_ref.at[x, :, rows, :]

    here = part_of(band, mine)
    for e in (2, 1, 3):
        go(copy(here, here, x_s.at[e - 1], x_r.at[e - 1], column, at_x(e)))
    go(copy(here, here, pair_s.at[0], pair_r.at[0], partner, band))
    for part in (0, 1):
        there = landed(2, part, core)
        copy(there, there, far_s.at[part], far_r.at[part], column, at_x(3 if part == 0 else 1)).wait_recv()
        to_twin(there, 4 + part)
    for e in (1, 3, 2):
        here = part_of(at_x(BANDS - e), mine)
        copy(here, here, x_s.at[e - 1], x_r.at[e - 1], column, at_x(BANDS - e)).wait_recv()
        go(copy(here, here, pair_s.at[e], pair_r.at[e], partner, band))

    for e in range(BANDS):
        there = part_of(at_x(BANDS - e), other)
        copy(there, there, pair_s.at[e], pair_r.at[e], partner, band).wait_recv()
    for index, step, part in ((0, 3, 0), (1, 1, 1), (2, 3, 1), (3, 1, 0), (4, 2, 0), (5, 2, 1)):
        there = landed(step, part, 1 - core)
        copy(there, there, twin_s.at[index], twin_r.at[index], partner, band).wait_recv()
    for descriptor in sends:
        descriptor.wait_send()


def direct_kernel(
    listed, lone_ref, direct_ref, rows_ref, spread_ref, full_ref,
    slots, rx_core,
    core_s, core_r, y_s, y_r, z_s, z_r, x_s, x_r, pair_s, pair_r,
    mat_s, mat_r, far_s, far_r, twin_s, twin_r,
):
    column = lax.axis_index("gx")
    band = lax.axis_index("gy")
    core = lax.rem(column, 2)
    y = lax.rem(column // 2, RING)
    z = column // (2 * RING)
    partner = (z * RING + y) * 2 + 1 - core

    def at_y(step):
        return (z * RING + lax.rem(y + step, RING)) * 2 + core

    def at_z(step):
        return (lax.rem(z + step, RING) * RING + y) * 2 + core

    def at_x(step):
        return lax.rem(band + step, BANDS)

    def copy(src, dst, send, recv, gx, gy):
        return pltpu.make_async_remote_copy(
            src_ref=src, dst_ref=dst, send_sem=send, recv_sem=recv,
            device_id=(gx, gy), device_id_type=MESH,
        )

    slots[1:3] = jnp.zeros((2, RING, HALF, 128), F32)

    barrier = pltpu.get_barrier_semaphore()
    peers = [(partner, band)]
    peers += [(at_y(d), band) for d in range(1, RING)]
    peers += [(at_z(d), band) for d in (1, RING - 1)]
    peers += [(column, at_x(d)) for d in range(1, BANDS)]
    for peer in peers:
        pl.semaphore_signal(barrier, inc=1, device_id=peer, device_id_type=MESH)
    pl.semaphore_wait(barrier, len(peers))

    mine = pl.ds(pl.multiple_of(core * HALF, 8), HALF)
    other = pl.ds(pl.multiple_of((1 - core) * HALF, 8), HALF)
    sends = []

    def go(descriptor):
        descriptor.start()
        sends.append(descriptor)

    swap = copy(lone_ref.at[other, :], rx_core, core_s, core_r, partner, band)
    go(swap)

    def my_rows(of):
        return pl.ds(pl.multiple_of(of * QUARTER, 8), QUARTER)

    def landed(step, part, core):
        return full_ref.at[pl.ds(part * few, few), core, my_rows(at_x(step)), :]

    few = listed // 2
    for way, part in ((0, 0), (1, 1), (0, 1), (1, 0)):
        source = rows_ref.at[pl.ds(part * few, few), core]
        go(copy(source, landed(0, part, core), mat_s.at[way, part], mat_r.at[way, part], column, at_x(1 if way == 0 else 3)))

    def arrived(way, part, step):
        here = landed(step, part, core)
        copy(here, here, mat_s.at[way, part], mat_r.at[way, part], column, at_x(3 if way == 0 else 1)).wait_recv()
        return here

    def to_twin(here, index):
        go(copy(here, here, twin_s.at[index], twin_r.at[index], partner, band))

    swap.wait_recv()
    slots[0, y] = lone_ref[mine, :] + rx_core[...]

    def next_plane(d):
        home = lax.rem(y + RING - d, RING)
        moves = []
        if d <= WINDOW:
            moves.append((y < d, 0, home, 2, 1))
        if d >= RING - WINDOW:
            moves.append((y >= d, 1, home, 1, RING - 1))
        return moves

    def over_z(d, act, back):
        for here, way, home, slot, step in next_plane(d):
            @pl.when(here)
            def _(way=way, home=home, slot=slot, step=RING - step if back else step):
                act(copy(
                    slots.at[0, home], slots.at[slot, home], z_s.at[way, d], z_r.at[way, d], at_z(step), band
                ))

    own = slots.at[0, y]
    for d in (4, 3, 5, 2, 6, 1, 7):
        go(copy(own, own, y_s.at[d - 1], y_r.at[d - 1], at_y(d), band))
    for d in (1, 7, 2, 6, 3, 5, 4):
        home = lax.rem(y + RING - d, RING)
        here = slots.at[0, home]
        copy(here, here, y_s.at[d - 1], y_r.at[d - 1], at_y(RING - d), band).wait_recv()
        over_z(d, lambda c: c.start(), False)

    from_left = arrived(0, 0, 3)
    from_right = arrived(1, 1, 1)
    to_twin(from_left, 0)
    to_twin(from_right, 1)
    go(copy(from_left, from_left, far_s.at[0], far_r.at[0], column, at_x(1)))
    go(copy(from_right, from_right, far_s.at[1], far_r.at[1], column, at_x(3)))

    chosen = [jnp.zeros((HALF, 128), F32)] * (listed // 2)

    def choose(step, home):
        at = 2 * (step * RING + home)
        straight = slots[step, home]
        crossed = pltpu.roll(straight, QUARTER, 1)
        for q in range(listed // 2):
            chosen[q] = chosen[q] + (
                straight * direct_ref[q, pl.ds(at, 1), :] + crossed * direct_ref[q, pl.ds(at + 1, 1), :]
            )

    for home in range(RING):
        choose(0, home)
    for d in (1, 7, 2, 6, 3, 5, 4):
        over_z(d, lambda c: c.wait_recv(), True)
        choose(jnp.where(y < d, 2, 1), lax.rem(y + RING - d, RING))
    for q in range(listed // 2):
        spread_ref[band, q, mine, :] = chosen[q]

    def part_of(x, rows):
        return spread_ref.at[x, :, rows, :]

    here = part_of(band, mine)
    for e in (2, 1, 3):
        go(copy(here, here, x_s.at[e - 1], x_r.at[e - 1], column, at_x(e)))
    go(copy(here, here, pair_s.at[0], pair_r.at[0], partner, band))
    to_twin(arrived(0, 1, 3), 2)
    to_twin(arrived(1, 0, 1), 3)
    for e in (1, 3, 2):
        here = part_of(at_x(BANDS - e), mine)
        copy(here, here, x_s.at[e - 1], x_r.at[e - 1], column, at_x(BANDS - e)).wait_recv()
        go(copy(here, here, pair_s.at[e], pair_r.at[e], partner, band))
    for part in (0, 1):
        there = landed(2, part, core)
        copy(there, there, far_s.at[part], far_r.at[part], column, at_x(3 if part == 0 else 1)).wait_recv()
        to_twin(there, 4 + part)

    for e in range(BANDS):
        there = part_of(at_x(BANDS - e), other)
        copy(there, there, pair_s.at[e], pair_r.at[e], partner, band).wait_recv()
    for index, step, part in ((0, 3, 0), (1, 1, 1), (2, 3, 1), (3, 1, 0), (4, 2, 0), (5, 2, 1)):
        there = landed(step, part, 1 - core)
        copy(there, there, twin_s.at[index], twin_r.at[index], partner, band).wait_recv()
    for d in range(1, RING):
        over_z(d, lambda c: c.wait_send(), False)
    for descriptor in sends:
        descriptor.wait_send()


def solve_kernel(
    owner_s, table_s, before_ref, cell_ref, spread_ref, rows_ref, full_ref,
    out_anom_ref, out_mean_ref,
    state, prior, mats, mat_sem,
):
    column = lax.axis_index("gx")
    band = lax.axis_index("gy")
    count = table_s[0]

    def fetch(i, x, from_own):
        rows = pl.ds(x * QUARTER, QUARTER)
        source = rows_ref.at[i] if from_own else full_ref.at[i, :, rows, :]
        return pltpu.make_async_copy(source, mats.at[i, :, rows, :], mat_sem.at[i, x])

    def start(i, carry):
        for x in range(BANDS):
            @pl.when(band == x)
            def _():
                fetch(i, x, True).start()

            @pl.when(band != x)
            def _():
                fetch(i, x, False).start()

        return carry

    lax.fori_loop(0, count, start, 0)
    state[...] = before_ref[...]

    left = lax.broadcasted_iota(jnp.int32, (ROWS, 128), 1) < QUARTER
    for q in range(spread_ref.shape[1]):
        for x in (0, 2):
            first = spread_ref[x, q]
            second = spread_ref[x + 1, q]
            lanes = pl.ds(x * QUARTER, 128)
            prior[2 * q, :, lanes] = jnp.where(left, first, pltpu.roll(second, QUARTER, 1))
            prior[2 * q + 1, :, lanes] = jnp.where(left, pltpu.roll(first, QUARTER, 1), second)

    spot = lax.broadcasted_iota(jnp.int32, (1, OBS), 1)
    scale = 1.0 / (7.0 * 32.0 * 79.0)

    def places(batch):
        cells = cell_ref[pl.ds(batch, 1), :]
        lon = owner_s[batch] * 2 + cells // 1024
        lat = (spot // QUARTER) * 8 + lax.rem(cells // 128, 8)
        return lon, lat

    def taper(lon_gap, lat_gap):
        lon_gap = jnp.minimum(lon_gap, NLON - lon_gap)
        return (
            jnp.maximum(7 - lon_gap, 0).astype(F32) * (NLAT - lat_gap).astype(F32) * scale
        )

    row = lax.broadcasted_iota(jnp.int32, (ROWS, OBS), 0)

    def assimilate(i, carry):
        batch = table_s[1 + i]
        slab = owner_s[batch]
        for x in range(BANDS):
            fetch(i, x, False).wait()
        z = prior[i]
        turned = jnp.transpose(jnp.concatenate([z, jnp.zeros((128 - ROWS, OBS), F32)], axis=0))
        gained = jnp.sum(mats[i, 1] * turned[:, MEMBERS : MEMBERS + 1], axis=0, keepdims=True)
        z_high, z_low = split(z)
        root_high, root_low = split(mats[i, 0])
        weighted = dot(jnp.concatenate([z_high, z_low], axis=0), root_high)
        weighted = weighted[0:ROWS] + (weighted[ROWS : 2 * ROWS] + dot(z_high, root_low))
        weights = jnp.where(row < MEMBERS, weighted, jnp.where(row == MEMBERS, gained, 0.0))
        column_id = lax.broadcasted_iota(jnp.int32, (OBS, 128), 1)
        turned_high, turned_low = split(jnp.where(column_id < MEMBERS, turned, 0.0))
        turned_both = jnp.concatenate([turned_high, turned_low], axis=1)
        short_high, short_low = turned_high[:, 0:ROWS], turned_low[:, 0:ROWS]
        lon, lat = places(batch)
        both = jnp.concatenate(
            [jnp.broadcast_to(lon, (8, OBS)), jnp.broadcast_to(lat, (8, OBS))], axis=0
        ).astype(F32)
        upright = jnp.transpose(both).astype(jnp.int32)
        lon_col = upright[:, 0:1]
        lat_col = upright[:, 8:9]

        weights_high, weights_low = split(weights)

        def later(j, carry):
            other = table_s[1 + j]

            @pl.when(dist(owner_s[other], slab) <= REACH)
            def _():
                held = prior[j]
                held_high, held_low = split(held)
                covariance = dot3(short_high, short_low, held_high, held_low)
                lon_j, lat_j = places(other)
                gain = covariance * taper(jnp.abs(lon_col - lon_j), jnp.abs(lat_col - lat_j))
                gain_h, gain_l = split(gain)
                prior[j] = held - dot3(weights_high, weights_low, gain_h, gain_l)

            return carry

        lax.fori_loop(i + 1, count, later, 0)

        @pl.when(dist(slab, column) <= REACH)
        def _():
            for at in range(0, GROUPS, BUNDLE):
                highs, lows = [], []
                for c in range(at, at + BUNDLE):
                    cell_lon = column * 2 + c // 8
                    cell_lat = band * 8 + c % 8
                    factor = taper(jnp.abs(lon - cell_lon), jnp.abs(lat - cell_lat))
                    high, low = split(weights * factor)
                    highs.append(high)
                    lows.append(low)
                wide = dot(jnp.concatenate(highs, axis=0), turned_both)
                middle = wide[:, 0:128] + (wide[:, 128:256] + dot(jnp.concatenate(lows, axis=0), turned_high))
                middle = middle[:, 0:ROWS]
                for c in range(at, at + BUNDLE):
                    lanes = pl.ds(c * 128, 128)
                    block = state[:, lanes]
                    m_high, m_low = split(middle[(c - at) * ROWS : (c - at + 1) * ROWS])
                    b_high, b_low = split(block)
                    moved = dot(m_high, jnp.concatenate([b_high, b_low], axis=1))
                    state[:, lanes] = block - (moved[:, 0:128] + (moved[:, 128:256] + dot(m_low, b_high)))

        return carry

    lax.fori_loop(0, count, assimilate, 0)

    for c in range(GROUPS):
        lanes = pl.ds(c * 128, 128)
        out_anom_ref[pl.ds(c, MEMBERS, stride=GROUPS), :] = state[0:MEMBERS, lanes]
        out_mean_ref[pl.ds(c, 1), :] = -state[pl.ds(MEMBERS, 1), lanes]


VMEM = pl.BlockSpec(memory_space=pltpu.VMEM)
SMEM = pl.BlockSpec(memory_space=pltpu.SMEM)
HBM = pl.BlockSpec(memory_space=pl.ANY)
DMA = pltpu.SemaphoreType.DMA


def exchange(listed, planes, collective_id, packet, choice, rows):
    return pl.pallas_call(
        functools.partial(comm_kernel, listed, planes),
        name="exchange",
        out_shape=(
            jax.ShapeDtypeStruct((BANDS, listed // 2, ROWS, 128), F32),
            jax.ShapeDtypeStruct((listed, 2, OBS, OBS), F32),
        ),
        in_specs=[VMEM, VMEM, HBM],
        out_specs=(VMEM, HBM),
        scratch_shapes=[
            pltpu.VMEM((PAIRS, HALF, 128), F32),
            pltpu.VMEM((PAIRS, HALF, 128), F32),
            pltpu.VMEM((RING - 1, HALF, 128), F32),
            pltpu.VMEM((HALF, 128), F32),
            pltpu.VMEM((RING - 1, HALF, 128), F32),
            pltpu.VMEM((PAIRS, HALF, 128), F32),
            DMA, DMA,
            DMA((RING - 1,)), DMA((RING - 1,)),
            DMA((RING - 1,)), DMA((RING - 1,)),
            DMA((RING - 1,)), DMA((RING - 1,)),
            DMA((BANDS - 1,)), DMA((BANDS - 1,)),
            DMA((BANDS,)), DMA((BANDS,)),
            DMA((2, 2)), DMA((2, 2)),
            DMA((2,)), DMA((2,)),
            DMA((6,)), DMA((6,)),
        ],
        compiler_params=pltpu.CompilerParams(collective_id=collective_id, has_side_effects=True, vmem_limit_bytes=GRANT),
    )(packet, choice, rows)


def direct(listed, collective_id, lone, choice, rows):
    return pl.pallas_call(
        functools.partial(direct_kernel, listed),
        name="direct",
        out_shape=(
            jax.ShapeDtypeStruct((BANDS, listed // 2, ROWS, 128), F32),
            jax.ShapeDtypeStruct((listed, 2, OBS, OBS), F32),
        ),
        in_specs=[VMEM, VMEM, HBM],
        out_specs=(VMEM, HBM),
        scratch_shapes=[
            pltpu.VMEM((3, RING, HALF, 128), F32),
            pltpu.VMEM((HALF, 128), F32),
            DMA, DMA,
            DMA((RING - 1,)), DMA((RING - 1,)),
            DMA((2, RING)), DMA((2, RING)),
            DMA((BANDS - 1,)), DMA((BANDS - 1,)),
            DMA((BANDS,)), DMA((BANDS,)),
            DMA((2, 2)), DMA((2, 2)),
            DMA((2,)), DMA((2,)),
            DMA((6,)), DMA((6,)),
        ],
        compiler_params=pltpu.CompilerParams(collective_id=collective_id, has_side_effects=True, vmem_limit_bytes=GRANT),
    )(lone, choice, rows)


def solve(listed, owner, table, state, obs_cell, spread, rows, full):
    return pl.pallas_call(
        solve_kernel,
        name="solve",
        out_shape=(
            jax.ShapeDtypeStruct((MEMBERS * GROUPS, 128), F32),
            jax.ShapeDtypeStruct((GROUPS, 128), F32),
        ),
        in_specs=[SMEM, SMEM, VMEM, VMEM, VMEM, HBM, HBM],
        out_specs=(VMEM, VMEM),
        scratch_shapes=[
            pltpu.VMEM((ROWS, CELLS), F32),
            pltpu.VMEM((listed, ROWS, OBS), F32),
            pltpu.VMEM((listed, 2, OBS, OBS), F32),
            DMA((listed, BANDS)),
        ],
        compiler_params=pltpu.CompilerParams(vmem_limit_bytes=GRANT),
    )(owner, table, state, obs_cell, spread, rows, full)


def local(anomalies, state_mean, obs_value, obs_cell, owner, order, root_inv, gain_inv):
    flat = anomalies.reshape(MEMBERS * GROUPS, 128)
    mean = state_mean.reshape(GROUPS, 128)
    packet, lone, rows, choice, near_choice, state, table, branch = pl.pallas_call(
        prep_kernel,
        name="prep",
        out_shape=(
            jax.ShapeDtypeStruct((PAIRS, ROWS, 128), F32),
            jax.ShapeDtypeStruct((ROWS, 128), F32),
            jax.ShapeDtypeStruct((BATCHES, 2, QUARTER, OBS), F32),
            jax.ShapeDtypeStruct((PAIRS, 2 * PAIRS, 128), F32),
            jax.ShapeDtypeStruct((MORE // 2, 6 * RING, 128), F32),
            jax.ShapeDtypeStruct((ROWS, CELLS), F32),
            jax.ShapeDtypeStruct((32,), jnp.int32),
            jax.ShapeDtypeStruct((1,), jnp.int32),
        ),
        in_specs=[SMEM, SMEM, HBM, VMEM, VMEM, VMEM, HBM, HBM],
        out_specs=(VMEM, VMEM, HBM, VMEM, VMEM, VMEM, SMEM, SMEM),
        scratch_shapes=[
            pltpu.VMEM((MEMBERS * GROUPS, 128), F32),
            pltpu.VMEM((BATCHES, 128), F32),
            pltpu.SMEM((BATCHES,), jnp.int32),
            pltpu.SMEM((BATCHES,), jnp.int32),
            DMA,
            DMA((BATCHES, 2)),
        ],
    )(order, owner, flat, mean, obs_cell, obs_value, root_inv, gain_inv)

    def near(listed, collective_id):
        spread, full = direct(listed, collective_id, lone, near_choice, rows)
        return solve(listed, owner, table, state, obs_cell, spread, rows, full)

    def wide(listed, planes, collective_id):
        spread, full = exchange(listed, planes, collective_id, packet, choice, rows)
        return solve(listed, owner, table, state, obs_cell, spread, rows, full)

    out_flat, out_mean = lax.switch(
        branch[0],
        (
            lambda: near(FEW, 1),
            lambda: near(MORE, 2),
            lambda: wide(SOME, NEXT_PLANES, 3),
            lambda: wide(BATCHES, ALL_PLANES, 4),
        ),
    )
    return out_flat.reshape(anomalies.shape), out_mean.reshape(state_mean.shape)


def solution(mesh):
    return jax.shard_map(
        local,
        mesh=mesh,
        in_specs=(
            P(None, "gx", "gy", None),
            P("gx", "gy", None),
            P(None, "gy"),
            P(),
            P(),
            P(),
            P(None, "gy", None),
            P(None, "gy", None),
        ),
        out_specs=(P(None, "gx", "gy", None), P("gx", "gy", None)),
        check_vma=False,
    )
```

```python
import functools

import jax
import jax.numpy as jnp
from jax import lax
from jax.experimental import pallas as pl
from jax.experimental.pallas import tpu as pltpu
from jax.sharding import PartitionSpec as P

MEMBERS = 80
OBS = 256
BATCHES = 16
REACH = 3
SLABS = 128
BANDS = 4
NLON = 256
NLAT = 32
QUARTER = 64
CELLS = 2048
GROUPS = 16
ROWS = 96
HALF = 48
PAIRS = 8
RING = 8
FEW = 4
MORE = 6
SOME = 8
WINDOW = 5
BUNDLE = 16
GRANT = 24 * 1024 * 1024
NEXT_PLANES = (1, 7)
ALL_PLANES = (4, 3, 5, 2, 6, 1, 7)
MESH = pl.DeviceIdType.MESH
F32 = jnp.float32
BF16 = jnp.bfloat16


def dist(a, b):
    gap = jnp.abs(a - b)
    return jnp.minimum(gap, SLABS - gap)


def split(value):
    high = value.astype(BF16)
    return high, (value - high.astype(F32)).astype(BF16)


def dot(left, right):
    return jnp.dot(left, right, preferred_element_type=F32)


def dot3(left_high, left_low, right_high, right_low):
    return dot(left_high, right_high) + (dot(left_high, right_low) + dot(left_low, right_high))


def prep_kernel(
    order_s, owner_s, anom_ref, mean_ref, cell_ref, value_ref, root_ref, gain_ref,
    packet_ref, lone_ref, rows_ref, choice_ref, direct_ref, state, table_s, branch_s,
    raw, values, rank_s, code_s, raw_sem, in_sem,
):
    column = lax.axis_index("gx")
    band = lax.axis_index("gy")
    load = pltpu.make_async_copy(anom_ref, raw, raw_sem)
    load.start()

    lane = lax.broadcasted_iota(jnp.int32, (8, 128), 1)
    low = 2 * lax.rem(lane, SLABS // 2)
    own_plane = low // (2 * RING)
    batches = [order_s[t] for t in range(BATCHES)]
    slabs = [owner_s[batches[t]] for t in range(BATCHES)]
    needs = [None] * BATCHES
    bits = jnp.zeros((8, 128), jnp.int32)
    total = jnp.zeros((8, 128), jnp.int32)
    far = jnp.zeros((8, 128), jnp.int32)
    beyond = jnp.zeros((8, 128), jnp.int32)
    for t in reversed(range(BATCHES)):
        near = jnp.minimum(dist(slabs[t], low), dist(slabs[t], low + 1)) <= REACH
        need = jnp.where(near, 1, 0)
        for s in range(t + 1, BATCHES):
            linked = jnp.where(dist(slabs[s], slabs[t]) <= REACH, 1, 0)
            need = need | (needs[s] * linked)
        needs[t] = need
        bits = bits + need * (1 << t)
        total = total + need
        apart = jnp.abs(own_plane - slabs[t] // (2 * RING))
        apart = jnp.minimum(apart, RING - apart)
        far = far | jnp.where(apart > 1, need, 0)
        chips = jnp.abs(low // 2 - slabs[t] // 2)
        chips = jnp.minimum(chips, SLABS // 2 - chips)
        beyond = beyond | jnp.where(chips > WINDOW, need, 0)
    mine = jnp.max(jnp.where(lane == column // 2, bits, 0))

    deepest = 0
    codes = []
    for t in range(BATCHES):
        rank = 0
        for s in range(t):
            rank = rank + jnp.where(slabs[s] // 2 == slabs[t] // 2, 1, 0)
        rank_s[batches[t]] = rank
        deepest = jnp.maximum(deepest, rank)
        step = lax.rem(slabs[t] // (2 * RING) - column // (2 * RING) + RING, RING)
        step = jnp.where(step == RING - 1, 2, step)
        codes.append((step * RING + lax.rem(slabs[t] // 2, RING)) * 2 + rank)

    for i in range(BATCHES):
        table_s[1 + i] = -1
        code_s[i] = -1
    count = 0
    for t in range(BATCHES):
        flag = lax.rem(mine // (1 << t), 2)

        @pl.when(flag == 1)
        def _(t=t, count=count):
            table_s[1 + count] = batches[t]
            code_s[count] = codes[t]

        count = count + flag
    table_s[0] = count

    def fetch(i, which, source):
        return pltpu.make_async_copy(source, rows_ref.at[i, which], in_sem.at[i, which])

    def start_fetch(i, carry):
        batch = table_s[1 + i]
        fetch(i, 0, root_ref.at[batch]).start()
        fetch(i, 1, gain_ref.at[batch]).start()
        return carry

    lax.fori_loop(0, count, start_fetch, 0)
    longest = jnp.max(total + far * (2 * BATCHES))
    branch_s[0] = jnp.where(
        longest > SOME,
        3,
        jnp.where((deepest > 1) | (jnp.max(beyond) > 0) | (longest > MORE), 2, jnp.where(longest > FEW, 1, 0))
    )

    at = lax.broadcasted_iota(jnp.int32, (2 * PAIRS, 128), 0)
    left = lax.broadcasted_iota(jnp.int32, (2 * PAIRS, 128), 1) < QUARTER
    slot = at // 2 + jnp.where(left == (lax.rem(at, 2) == 0), 0, PAIRS)
    for q in range(PAIRS):
        wanted = jnp.where(left, table_s[1 + 2 * q], table_s[2 + 2 * q])
        choice_ref[q] = jnp.where(wanted == slot, 1.0, 0.0)
    at = lax.broadcasted_iota(jnp.int32, (6 * RING, 128), 0)
    left = lax.broadcasted_iota(jnp.int32, (6 * RING, 128), 1) < QUARTER
    slot = at // 2 * 2 + jnp.where(left == (lax.rem(at, 2) == 0), 0, 1)
    for q in range(MORE // 2):
        wanted = jnp.where(left, code_s[2 * q], code_s[1 + 2 * q])
        direct_ref[q] = jnp.where(wanted == slot, 1.0, 0.0)

    values[:, 0:QUARTER] = value_ref[...]
    values[:, QUARTER:128] = value_ref[...]
    packet_ref[...] = jnp.zeros_like(packet_ref)
    lone_ref[...] = jnp.zeros_like(lone_ref)

    tail = lax.broadcasted_iota(jnp.int32, (16, 128), 0)
    for c in range(GROUPS):
        lanes = pl.ds(c * 128, 128)
        state[MEMBERS:ROWS, lanes] = jnp.where(tail == 0, -mean_ref[pl.ds(c, 1), :], 0.0)
    load.wait()
    for c in range(GROUPS):
        state[0:MEMBERS, pl.ds(c * 128, 128)] = raw[pl.ds(c, MEMBERS, stride=GROUPS), :]

    def pick(batch, carry):
        @pl.when(owner_s[batch] == column)
        def _():
            half = batch // PAIRS
            pair = lax.rem(batch, PAIRS)
            cells = jnp.broadcast_to(cell_ref[pl.ds(batch, 1), :], (8, OBS))
            shift = lax.rem(half * QUARTER - band * QUARTER + OBS, OBS)
            mine = pltpu.roll(cells, shift, 1)[0:1, 0:128]
            spot = lax.broadcasted_iota(jnp.int32, (1, 128), 1)
            valid = (spot // QUARTER) == half
            mine = jnp.where(valid, mine, -1)
            picked = jnp.zeros((ROWS, 128), F32)
            step = 512
            for at in range(0, CELLS, step):
                ids = lax.broadcasted_iota(jnp.int32, (step, 128), 0) + at
                hot = jnp.where(ids == mine, 1.0, 0.0).astype(BF16)
                block = state[:, pl.ds(at, step)]
                high = block.astype(BF16)
                rest = block - high.astype(F32)
                mid = rest.astype(BF16)
                last = (rest - mid.astype(F32)).astype(BF16)
                picked = picked + (dot(high, hot) + (dot(mid, hot) + dot(last, hot)))
            row = lax.broadcasted_iota(jnp.int32, (ROWS, 128), 0)
            seen = jnp.where(valid, values[pl.ds(batch, 1), :], 0.0)
            picked = picked + jnp.where(row == MEMBERS, seen, 0.0)
            packet_ref[pair] = packet_ref[pair] + picked
            turn = lax.rem(rank_s[batch] + half, 2) * QUARTER
            lone_ref[...] = lone_ref[...] + pltpu.roll(picked, turn, 1)

        return carry

    lax.fori_loop(0, BATCHES, pick, 0)

    def finish(i, carry):
        fetch(i, 0, root_ref.at[0]).wait()
        fetch(i, 1, gain_ref.at[0]).wait()
        return carry

    lax.fori_loop(0, count, finish, 0)


def comm_kernel(
    listed, planes, packet_ref, choice_ref, rows_ref, spread_ref, full_ref,
    mixed, rx_core, rx_y, plane, rx_z, slots,
    core_s, core_r, y_s, y_r, z_s, z_r, back_s, back_r, x_s, x_r, pair_s, pair_r,
    mat_s, mat_r, far_s, far_r, twin_s, twin_r,
):
    column = lax.axis_index("gx")
    band = lax.axis_index("gy")
    core = lax.rem(column, 2)
    y = lax.rem(column // 2, RING)
    z = column // (2 * RING)
    partner = (z * RING + y) * 2 + 1 - core

    def at_y(step):
        return (z * RING + lax.rem(y + step, RING)) * 2 + core

    def at_z(step):
        return (lax.rem(z + step, RING) * RING + y) * 2 + core

    def at_x(step):
        return lax.rem(band + step, BANDS)

    def copy(src, dst, send, recv, gx, gy):
        return pltpu.make_async_remote_copy(
            src_ref=src, dst_ref=dst, send_sem=send, recv_sem=recv,
            device_id=(gx, gy), device_id_type=MESH,
        )

    barrier = pltpu.get_barrier_semaphore()
    peers = [(partner, band)]
    peers += [(at_y(d), band) for d in range(1, RING)]
    peers += [(at_z(d), band) for d in planes]
    peers += [(column, at_x(d)) for d in range(1, BANDS)]
    for peer in peers:
        pl.semaphore_signal(barrier, inc=1, device_id=peer, device_id_type=MESH)
    for which in range(2):
        own_rows = pl.ds(pl.multiple_of(band * QUARTER, 8), QUARTER)
        full_ref[:, which, own_rows, :] = rows_ref[pl.ds(0, listed), which]
    pl.semaphore_wait(barrier, len(peers))

    mine = pl.ds(pl.multiple_of(core * HALF, 8), HALF)
    other = pl.ds(pl.multiple_of((1 - core) * HALF, 8), HALF)
    sends = []

    def go(descriptor):
        descriptor.start()
        sends.append(descriptor)

    swap = copy(packet_ref.at[:, other, :], rx_core, core_s, core_r, partner, band)
    go(swap)

    def my_rows(of):
        return pl.ds(pl.multiple_of(of * QUARTER, 8), QUARTER)

    def landed(step, part, core):
        return full_ref.at[pl.ds(part * few, few), core, my_rows(at_x(step)), :]

    few = listed // 2
    for way, part in ((0, 0), (1, 1), (0, 1), (1, 0)):
        source = rows_ref.at[pl.ds(part * few, few), core]
        go(copy(source, landed(0, part, core), mat_s.at[way, part], mat_r.at[way, part], column, at_x(1 if way == 0 else 3)))

    def arrived(way, part, step):
        here = landed(step, part, core)
        copy(here, here, mat_s.at[way, part], mat_r.at[way, part], column, at_x(3 if way == 0 else 1)).wait_recv()
        return here

    def to_twin(here, index):
        go(copy(here, here, twin_s.at[index], twin_r.at[index], partner, band))

    swap.wait_recv()
    mixed[...] = packet_ref[:, mine, :] + rx_core[...]

    for d in (4, 3, 5, 2, 6, 1, 7):
        go(copy(mixed.at[lax.rem(y + d, RING)], rx_y.at[d - 1], y_s.at[d - 1], y_r.at[d - 1], at_y(d), band))
    part = mixed[y]
    for d in (1, 7, 2, 6, 3, 5, 4):
        copy(mixed.at[0], rx_y.at[d - 1], y_s.at[d - 1], y_r.at[d - 1], at_y(RING - d), band).wait_recv()
        part = part + rx_y[d - 1]
    plane[...] = part
    from_left = arrived(0, 0, 3)
    from_right = arrived(1, 1, 1)

    for d in planes:
        go(copy(plane, rx_z.at[d - 1], z_s.at[d - 1], z_r.at[d - 1], at_z(d), band))
    go(copy(from_left, from_left, far_s.at[0], far_r.at[0], column, at_x(1)))
    go(copy(from_right, from_right, far_s.at[1], far_r.at[1], column, at_x(3)))
    to_twin(from_left, 0)
    to_twin(from_right, 1)
    for d in reversed(planes):
        copy(plane, rx_z.at[d - 1], z_s.at[d - 1], z_r.at[d - 1], at_z(RING - d), band).wait_recv()
        part = part + rx_z[d - 1]
    slots[y] = part
    own = slots.at[y]
    for d in (4, 3, 5, 2, 6, 1, 7):
        go(copy(own, own, back_s.at[d - 1], back_r.at[d - 1], at_y(d), band))
    to_twin(arrived(0, 1, 3), 2)
    to_twin(arrived(1, 0, 1), 3)
    for d in (1, 7, 2, 6, 3, 5, 4):
        here = slots.at[lax.rem(y + RING - d, RING)]
        copy(here, here, back_s.at[d - 1], back_r.at[d - 1], at_y(RING - d), band).wait_recv()

    chosen = [jnp.zeros((HALF, 128), F32)] * (listed // 2)
    for p in range(PAIRS):
        straight = slots[p]
        crossed = pltpu.roll(straight, QUARTER, 1)
        for q in range(listed // 2):
            chosen[q] = chosen[q] + (
                straight * choice_ref[q, 2 * p : 2 * p + 1, :]
                + crossed * choice_ref[q, 2 * p + 1 : 2 * p + 2, :]
            )
    for q in range(listed // 2):
        spread_ref[band, q, mine, :] = chosen[q]

    def part_of(x, rows):
        return spread_ref.at[x, :, rows, :]

    here = part_of(band, mine)
    for e in (2, 1, 3):
        go(copy(here, here, x_s.at[e - 1], x_r.at[e - 1], column, at_x(e)))
    go(copy(here, here, pair_s.at[0], pair_r.at[0], partner, band))
    for part in (0, 1):
        there = landed(2, part, core)
        copy(there, there, far_s.at[part], far_r.at[part], column, at_x(3 if part == 0 else 1)).wait_recv()
        to_twin(there, 4 + part)
    for e in (1, 3, 2):
        here = part_of(at_x(BANDS - e), mine)
        copy(here, here, x_s.at[e - 1], x_r.at[e - 1], column, at_x(BANDS - e)).wait_recv()
        go(copy(here, here, pair_s.at[e], pair_r.at[e], partner, band))

    for e in range(BANDS):
        there = part_of(at_x(BANDS - e), other)
        copy(there, there, pair_s.at[e], pair_r.at[e], partner, band).wait_recv()
    for index, step, part in ((0, 3, 0), (1, 1, 1), (2, 3, 1), (3, 1, 0), (4, 2, 0), (5, 2, 1)):
        there = landed(step, part, 1 - core)
        copy(there, there, twin_s.at[index], twin_r.at[index], partner, band).wait_recv()
    for descriptor in sends:
        descriptor.wait_send()


def direct_kernel(
    listed, lone_ref, direct_ref, rows_ref, spread_ref, full_ref,
    slots, rx_core,
    core_s, core_r, y_s, y_r, z_s, z_r, x_s, x_r, pair_s, pair_r,
    mat_s, mat_r, far_s, far_r, twin_s, twin_r,
):
    column = lax.axis_index("gx")
    band = lax.axis_index("gy")
    core = lax.rem(column, 2)
    y = lax.rem(column // 2, RING)
    z = column // (2 * RING)
    partner = (z * RING + y) * 2 + 1 - core

    def at_y(step):
        return (z * RING + lax.rem(y + step, RING)) * 2 + core

    def at_z(step):
        return (lax.rem(z + step, RING) * RING + y) * 2 + core

    def at_x(step):
        return lax.rem(band + step, BANDS)

    def copy(src, dst, send, recv, gx, gy):
        return pltpu.make_async_remote_copy(
            src_ref=src, dst_ref=dst, send_sem=send, recv_sem=recv,
            device_id=(gx, gy), device_id_type=MESH,
        )

    slots[1:3] = jnp.zeros((2, RING, HALF, 128), F32)

    barrier = pltpu.get_barrier_semaphore()
    peers = [(partner, band)]
    peers += [(at_y(d), band) for d in range(1, RING)]
    peers += [(at_z(d), band) for d in (1, RING - 1)]
    peers += [(column, at_x(d)) for d in range(1, BANDS)]
    for peer in peers:
        pl.semaphore_signal(barrier, inc=1, device_id=peer, device_id_type=MESH)
    for which in range(2):
        own_rows = pl.ds(pl.multiple_of(band * QUARTER, 8), QUARTER)
        full_ref[:, which, own_rows, :] = rows_ref[pl.ds(0, listed), which]
    pl.semaphore_wait(barrier, len(peers))

    mine = pl.ds(pl.multiple_of(core * HALF, 8), HALF)
    other = pl.ds(pl.multiple_of((1 - core) * HALF, 8), HALF)
    sends = []

    def go(descriptor):
        descriptor.start()
        sends.append(descriptor)

    swap = copy(lone_ref.at[other, :], rx_core, core_s, core_r, partner, band)
    go(swap)

    def my_rows(of):
        return pl.ds(pl.multiple_of(of * QUARTER, 8), QUARTER)

    def landed(step, part, core):
        return full_ref.at[pl.ds(part * few, few), core, my_rows(at_x(step)), :]

    few = listed // 2
    for way, part in ((0, 0), (1, 1), (0, 1), (1, 0)):
        source = rows_ref.at[pl.ds(part * few, few), core]
        go(copy(source, landed(0, part, core), mat_s.at[way, part], mat_r.at[way, part], column, at_x(1 if way == 0 else 3)))

    def arrived(way, part, step):
        here = landed(step, part, core)
        copy(here, here, mat_s.at[way, part], mat_r.at[way, part], column, at_x(3 if way == 0 else 1)).wait_recv()
        return here

    def to_twin(here, index):
        go(copy(here, here, twin_s.at[index], twin_r.at[index], partner, band))

    swap.wait_recv()
    slots[0, y] = lone_ref[mine, :] + rx_core[...]

    def next_plane(d):
        home = lax.rem(y + RING - d, RING)
        moves = []
        if d <= WINDOW:
            moves.append((y < d, 0, home, 2, 1))
        if d >= RING - WINDOW:
            moves.append((y >= d, 1, home, 1, RING - 1))
        return moves

    def over_z(d, act, back):
        for here, way, home, slot, step in next_plane(d):
            @pl.when(here)
            def _(way=way, home=home, slot=slot, step=RING - step if back else step):
                act(copy(
                    slots.at[0, home], slots.at[slot, home], z_s.at[way, d], z_r.at[way, d], at_z(step), band
                ))

    own = slots.at[0, y]
    for d in (4, 3, 5, 2, 6, 1, 7):
        go(copy(own, own, y_s.at[d - 1], y_r.at[d - 1], at_y(d), band))
    for d in (1, 7, 2, 6, 3, 5, 4):
        home = lax.rem(y + RING - d, RING)
        here = slots.at[0, home]
        copy(here, here, y_s.at[d - 1], y_r.at[d - 1], at_y(RING - d), band).wait_recv()
        over_z(d, lambda c: c.start(), False)

    from_left = arrived(0, 0, 3)
    from_right = arrived(1, 1, 1)
    to_twin(from_left, 0)
    to_twin(from_right, 1)
    go(copy(from_left, from_left, far_s.at[0], far_r.at[0], column, at_x(1)))
    go(copy(from_right, from_right, far_s.at[1], far_r.at[1], column, at_x(3)))

    chosen = [jnp.zeros((HALF, 128), F32)] * (listed // 2)

    def choose(step, home):
        at = 2 * (step * RING + home)
        straight = slots[step, home]
        crossed = pltpu.roll(straight, QUARTER, 1)
        for q in range(listed // 2):
            chosen[q] = chosen[q] + (
                straight * direct_ref[q, pl.ds(at, 1), :] + crossed * direct_ref[q, pl.ds(at + 1, 1), :]
            )

    for home in range(RING):
        choose(0, home)
    for d in (1, 7, 2, 6, 3, 5, 4):
        over_z(d, lambda c: c.wait_recv(), True)
        choose(jnp.where(y < d, 2, 1), lax.rem(y + RING - d, RING))
    for q in range(listed // 2):
        spread_ref[band, q, mine, :] = chosen[q]

    def part_of(x, rows):
        return spread_ref.at[x, :, rows, :]

    here = part_of(band, mine)
    for e in (2, 1, 3):
        go(copy(here, here, x_s.at[e - 1], x_r.at[e - 1], column, at_x(e)))
    go(copy(here, here, pair_s.at[0], pair_r.at[0], partner, band))
    to_twin(arrived(0, 1, 3), 2)
    to_twin(arrived(1, 0, 1), 3)
    for e in (1, 3, 2):
        here = part_of(at_x(BANDS - e), mine)
        copy(here, here, x_s.at[e - 1], x_r.at[e - 1], column, at_x(BANDS - e)).wait_recv()
        go(copy(here, here, pair_s.at[e], pair_r.at[e], partner, band))
    for part in (0, 1):
        there = landed(2, part, core)
        copy(there, there, far_s.at[part], far_r.at[part], column, at_x(3 if part == 0 else 1)).wait_recv()
        to_twin(there, 4 + part)

    for e in range(BANDS):
        there = part_of(at_x(BANDS - e), other)
        copy(there, there, pair_s.at[e], pair_r.at[e], partner, band).wait_recv()
    for index, step, part in ((0, 3, 0), (1, 1, 1), (2, 3, 1), (3, 1, 0), (4, 2, 0), (5, 2, 1)):
        there = landed(step, part, 1 - core)
        copy(there, there, twin_s.at[index], twin_r.at[index], partner, band).wait_recv()
    for d in range(1, RING):
        over_z(d, lambda c: c.wait_send(), False)
    for descriptor in sends:
        descriptor.wait_send()


def solve_kernel(
    owner_s, table_s, before_ref, cell_ref, spread_ref, full_ref,
    out_anom_ref, out_mean_ref,
    state, prior,
):
    column = lax.axis_index("gx")
    band = lax.axis_index("gy")
    count = table_s[0]

    state[...] = before_ref[...]

    left = lax.broadcasted_iota(jnp.int32, (ROWS, 128), 1) < QUARTER
    for q in range(spread_ref.shape[1]):
        for x in (0, 2):
            first = spread_ref[x, q]
            second = spread_ref[x + 1, q]
            lanes = pl.ds(x * QUARTER, 128)
            prior[2 * q, :, lanes] = jnp.where(left, first, pltpu.roll(second, QUARTER, 1))
            prior[2 * q + 1, :, lanes] = jnp.where(left, pltpu.roll(first, QUARTER, 1), second)

    spot = lax.broadcasted_iota(jnp.int32, (1, OBS), 1)
    scale = 1.0 / (7.0 * 32.0 * 79.0)

    def places(batch):
        cells = cell_ref[pl.ds(batch, 1), :]
        lon = owner_s[batch] * 2 + cells // 1024
        lat = (spot // QUARTER) * 8 + lax.rem(cells // 128, 8)
        return lon, lat

    def taper(lon_gap, lat_gap):
        lon_gap = jnp.minimum(lon_gap, NLON - lon_gap)
        return (
            jnp.maximum(7 - lon_gap, 0).astype(F32) * (NLAT - lat_gap).astype(F32) * scale
        )

    row = lax.broadcasted_iota(jnp.int32, (ROWS, OBS), 0)

    def assimilate(i, carry):
        batch = table_s[1 + i]
        slab = owner_s[batch]
        z = prior[i]
        turned = jnp.transpose(jnp.concatenate([z, jnp.zeros((128 - ROWS, OBS), F32)], axis=0))
        gained = jnp.sum(full_ref[i, 1] * turned[:, MEMBERS : MEMBERS + 1], axis=0, keepdims=True)
        z_high, z_low = split(z)
        root_high, root_low = split(full_ref[i, 0])
        weighted = dot(jnp.concatenate([z_high, z_low], axis=0), root_high)
        weighted = weighted[0:ROWS] + (weighted[ROWS : 2 * ROWS] + dot(z_high, root_low))
        weights = jnp.where(row < MEMBERS, weighted, jnp.where(row == MEMBERS, gained, 0.0))
        column_id = lax.broadcasted_iota(jnp.int32, (OBS, 128), 1)
        turned_high, turned_low = split(jnp.where(column_id < MEMBERS, turned, 0.0))
        turned_both = jnp.concatenate([turned_high, turned_low], axis=1)
        short_high, short_low = turned_high[:, 0:ROWS], turned_low[:, 0:ROWS]
        lon, lat = places(batch)
        both = jnp.concatenate(
            [jnp.broadcast_to(lon, (8, OBS)), jnp.broadcast_to(lat, (8, OBS))], axis=0
        ).astype(F32)
        upright = jnp.transpose(both).astype(jnp.int32)
        lon_col = upright[:, 0:1]
        lat_col = upright[:, 8:9]

        weights_high, weights_low = split(weights)

        def later(j, carry):
            other = table_s[1 + j]

            @pl.when(dist(owner_s[other], slab) <= REACH)
            def _():
                held = prior[j]
                held_high, held_low = split(held)
                covariance = dot3(short_high, short_low, held_high, held_low)
                lon_j, lat_j = places(other)
                gain = covariance * taper(jnp.abs(lon_col - lon_j), jnp.abs(lat_col - lat_j))
                gain_h, gain_l = split(gain)
                prior[j] = held - dot3(weights_high, weights_low, gain_h, gain_l)

            return carry

        lax.fori_loop(i + 1, count, later, 0)

        @pl.when(dist(slab, column) <= REACH)
        def _():
            for at in range(0, GROUPS, BUNDLE):
                highs, lows = [], []
                for c in range(at, at + BUNDLE):
                    cell_lon = column * 2 + c // 8
                    cell_lat = band * 8 + c % 8
                    factor = taper(jnp.abs(lon - cell_lon), jnp.abs(lat - cell_lat))
                    high, low = split(weights * factor)
                    highs.append(high)
                    lows.append(low)
                wide = dot(jnp.concatenate(highs, axis=0), turned_both)
                middle = wide[:, 0:128] + (wide[:, 128:256] + dot(jnp.concatenate(lows, axis=0), turned_high))
                middle = middle[:, 0:ROWS]
                for c in range(at, at + BUNDLE):
                    lanes = pl.ds(c * 128, 128)
                    block = state[:, lanes]
                    m_high, m_low = split(middle[(c - at) * ROWS : (c - at + 1) * ROWS])
                    b_high, b_low = split(block)
                    moved = dot(m_high, jnp.concatenate([b_high, b_low], axis=1))
                    state[:, lanes] = block - (moved[:, 0:128] + (moved[:, 128:256] + dot(m_low, b_high)))

        return carry

    lax.fori_loop(0, count, assimilate, 0)

    for c in range(GROUPS):
        lanes = pl.ds(c * 128, 128)
        out_anom_ref[pl.ds(c, MEMBERS, stride=GROUPS), :] = state[0:MEMBERS, lanes]
        out_mean_ref[pl.ds(c, 1), :] = -state[pl.ds(MEMBERS, 1), lanes]


VMEM = pl.BlockSpec(memory_space=pltpu.VMEM)
SMEM = pl.BlockSpec(memory_space=pltpu.SMEM)
HBM = pl.BlockSpec(memory_space=pl.ANY)
DMA = pltpu.SemaphoreType.DMA


def exchange(listed, planes, collective_id, packet, choice, rows):
    return pl.pallas_call(
        functools.partial(comm_kernel, listed, planes),
        name="exchange",
        out_shape=(
            jax.ShapeDtypeStruct((BANDS, listed // 2, ROWS, 128), F32),
            jax.ShapeDtypeStruct((listed, 2, OBS, OBS), F32),
        ),
        in_specs=[VMEM, VMEM, VMEM],
        out_specs=(VMEM, VMEM),
        scratch_shapes=[
            pltpu.VMEM((PAIRS, HALF, 128), F32),
            pltpu.VMEM((PAIRS, HALF, 128), F32),
            pltpu.VMEM((RING - 1, HALF, 128), F32),
            pltpu.VMEM((HALF, 128), F32),
            pltpu.VMEM((RING - 1, HALF, 128), F32),
            pltpu.VMEM((PAIRS, HALF, 128), F32),
            DMA, DMA,
            DMA((RING - 1,)), DMA((RING - 1,)),
            DMA((RING - 1,)), DMA((RING - 1,)),
            DMA((RING - 1,)), DMA((RING - 1,)),
            DMA((BANDS - 1,)), DMA((BANDS - 1,)),
            DMA((BANDS,)), DMA((BANDS,)),
            DMA((2, 2)), DMA((2, 2)),
            DMA((2,)), DMA((2,)),
            DMA((6,)), DMA((6,)),
        ],
        compiler_params=pltpu.CompilerParams(collective_id=collective_id, has_side_effects=True, vmem_limit_bytes=GRANT),
    )(packet, choice, rows)


def direct(listed, collective_id, lone, choice, rows):
    return pl.pallas_call(
        functools.partial(direct_kernel, listed),
        name="direct",
        out_shape=(
            jax.ShapeDtypeStruct((BANDS, listed // 2, ROWS, 128), F32),
            jax.ShapeDtypeStruct((listed, 2, OBS, OBS), F32),
        ),
        in_specs=[VMEM, VMEM, VMEM],
        out_specs=(VMEM, VMEM),
        scratch_shapes=[
            pltpu.VMEM((3, RING, HALF, 128), F32),
            pltpu.VMEM((HALF, 128), F32),
            DMA, DMA,
            DMA((RING - 1,)), DMA((RING - 1,)),
            DMA((2, RING)), DMA((2, RING)),
            DMA((BANDS - 1,)), DMA((BANDS - 1,)),
            DMA((BANDS,)), DMA((BANDS,)),
            DMA((2, 2)), DMA((2, 2)),
            DMA((2,)), DMA((2,)),
            DMA((6,)), DMA((6,)),
        ],
        compiler_params=pltpu.CompilerParams(collective_id=collective_id, has_side_effects=True, vmem_limit_bytes=GRANT),
    )(lone, choice, rows)


def solve(listed, owner, table, state, obs_cell, spread, full):
    return pl.pallas_call(
        solve_kernel,
        name="solve",
        out_shape=(
            jax.ShapeDtypeStruct((MEMBERS * GROUPS, 128), F32),
            jax.ShapeDtypeStruct((GROUPS, 128), F32),
        ),
        in_specs=[SMEM, SMEM, VMEM, VMEM, VMEM, VMEM],
        out_specs=(VMEM, VMEM),
        scratch_shapes=[
            pltpu.VMEM((ROWS, CELLS), F32),
            pltpu.VMEM((listed, ROWS, OBS), F32),
        ],
        compiler_params=pltpu.CompilerParams(vmem_limit_bytes=GRANT),
    )(owner, table, state, obs_cell, spread, full)


def local(anomalies, state_mean, obs_value, obs_cell, owner, order, root_inv, gain_inv):
    flat = anomalies.reshape(MEMBERS * GROUPS, 128)
    mean = state_mean.reshape(GROUPS, 128)
    packet, lone, rows, choice, near_choice, state, table, branch = pl.pallas_call(
        prep_kernel,
        name="prep",
        out_shape=(
            jax.ShapeDtypeStruct((PAIRS, ROWS, 128), F32),
            jax.ShapeDtypeStruct((ROWS, 128), F32),
            jax.ShapeDtypeStruct((BATCHES, 2, QUARTER, OBS), F32),
            jax.ShapeDtypeStruct((PAIRS, 2 * PAIRS, 128), F32),
            jax.ShapeDtypeStruct((MORE // 2, 6 * RING, 128), F32),
            jax.ShapeDtypeStruct((ROWS, CELLS), F32),
            jax.ShapeDtypeStruct((32,), jnp.int32),
            jax.ShapeDtypeStruct((1,), jnp.int32),
        ),
        in_specs=[SMEM, SMEM, HBM, VMEM, VMEM, VMEM, HBM, HBM],
        out_specs=(VMEM, VMEM, HBM, VMEM, VMEM, VMEM, SMEM, SMEM),
        scratch_shapes=[
            pltpu.VMEM((MEMBERS * GROUPS, 128), F32),
            pltpu.VMEM((BATCHES, 128), F32),
            pltpu.SMEM((BATCHES,), jnp.int32),
            pltpu.SMEM((BATCHES,), jnp.int32),
            DMA,
            DMA((BATCHES, 2)),
        ],
    )(order, owner, flat, mean, obs_cell, obs_value, root_inv, gain_inv)

    def near(listed, collective_id):
        spread, full = direct(listed, collective_id, lone, near_choice, rows)
        return solve(listed, owner, table, state, obs_cell, spread, full)

    def wide(listed, planes, collective_id):
        spread, full = exchange(listed, planes, collective_id, packet, choice, rows)
        return solve(listed, owner, table, state, obs_cell, spread, full)

    out_flat, out_mean = lax.switch(
        branch[0],
        (
            lambda: near(FEW, 1),
            lambda: near(MORE, 2),
            lambda: wide(SOME, NEXT_PLANES, 3),
            lambda: wide(BATCHES, ALL_PLANES, 4),
        ),
    )
    return out_flat.reshape(anomalies.shape), out_mean.reshape(state_mean.shape)


def solution(mesh):
    return jax.shard_map(
        local,
        mesh=mesh,
        in_specs=(
            P(None, "gx", "gy", None),
            P("gx", "gy", None),
            P(None, "gy"),
            P(),
            P(),
            P(),
            P(None, "gy", None),
            P(None, "gy", None),
        ),
        out_specs=(P(None, "gx", "gy", None), P("gx", "gy", None)),
        check_vma=False,
    )
```

```python
import functools

import jax
import jax.numpy as jnp
from jax import lax
from jax.experimental import pallas as pl
from jax.experimental.pallas import tpu as pltpu
from jax.sharding import PartitionSpec as P

MEMBERS = 80
OBS = 256
BATCHES = 16
REACH = 3
SLABS = 128
CHIPS = 64
BANDS = 4
NLON = 256
NLAT = 32
QUARTER = 64
CELLS = 2048
GROUPS = 16
ROWS = 96
HALF = 48
PAIRS = 8
RING = 8
FEW = 4
MORE = 6
SOME = 8
WINDOW = 5
BUNDLE = 16
GRANT = 24 * 1024 * 1024
NEXT_PLANES = (1, 7)
ALL_PLANES = (4, 3, 5, 2, 6, 1, 7)
MESH = pl.DeviceIdType.MESH
F32 = jnp.float32
BF16 = jnp.bfloat16


def dist(a, b):
    gap = jnp.abs(a - b)
    return jnp.minimum(gap, SLABS - gap)


def split(value):
    high = value.astype(BF16)
    return high, (value - high.astype(F32)).astype(BF16)


def dot(left, right):
    return jnp.dot(left, right, preferred_element_type=F32)


def dot3(left_high, left_low, right_high, right_low):
    return dot(left_high, right_high) + (dot(left_high, right_low) + dot(left_low, right_high))


def prep_kernel(
    order_s, owner_s, anom_ref, mean_ref, cell_ref, value_ref, root_ref, gain_ref,
    packet_ref, lone_ref, rows_ref, choice_ref, direct_ref, state, table_s, branch_s,
    raw, values, rank_s, code_s, own_s, raw_sem, in_sem,
):
    column = lax.axis_index("gx")
    band = lax.axis_index("gy")
    load = pltpu.make_async_copy(anom_ref, raw, raw_sem)
    load.start()

    @pl.when(column >= 0)
    def _():
        lane = lax.broadcasted_iota(jnp.int32, (8, 128), 1)
        chip = lane & (CHIPS - 1)
        own_plane = chip // RING
        slabs = [owner_s[order_s[t]] for t in range(BATCHES)]
        needs = [None] * BATCHES
        bits = jnp.zeros((8, 128), jnp.int32)
        total = jnp.zeros((8, 128), jnp.int32)
        far = jnp.zeros((8, 128), jnp.int32)
        beyond = jnp.zeros((8, 128), jnp.int32)
        deepest = 0
        for t in reversed(range(BATCHES)):
            near = ((slabs[t] + REACH - 2 * chip) & (SLABS - 1)) <= 2 * REACH + 1
            need = jnp.where(near, -1, 0)
            for s in range(t + 1, BATCHES):
                linked = ((slabs[s] + REACH - slabs[t]) & (SLABS - 1)) <= 2 * REACH
                need = need | (needs[s] & jnp.where(linked, -1, 0))
            needs[t] = need
            bits = bits | (need & (1 << t))
            total = total - need
            far = far | jnp.where(((slabs[t] // (2 * RING) + 1 - own_plane) & (RING - 1)) > 2, need, 0)
            beyond = beyond | jnp.where(((slabs[t] // 2 + WINDOW - chip) & (CHIPS - 1)) > 2 * WINDOW, need, 0)
            rank = 0
            for s in range(t):
                rank = rank + jnp.where(slabs[s] // 2 == slabs[t] // 2, 1, 0)
            rank_s[order_s[t]] = rank
            deepest = jnp.maximum(deepest, rank)
        own_s[0] = jnp.max(jnp.where(lane == column // 2, bits, 0))
        longest = jnp.max(total + (far & (2 * BATCHES)))
        beyond_any = jnp.max(beyond & 1)
        branch_s[0] = jnp.where(
            longest > SOME,
            3,
            jnp.where((deepest > 1) | (beyond_any > 0) | (longest > MORE), 2, jnp.where(longest > FEW, 1, 0)),
        )

    mine = own_s[0]
    for i in range(BATCHES):
        table_s[1 + i] = -1
        code_s[i] = -1
    count = 0
    for t in range(BATCHES):
        flag = (mine >> t) & 1

        @pl.when(flag == 1)
        def _(t=t, count=count):
            batch = order_s[t]
            slab = owner_s[batch]
            step = (slab // (2 * RING) - column // (2 * RING)) & (RING - 1)
            step = jnp.where(step == RING - 1, 2, step)
            table_s[1 + count] = batch
            code_s[count] = (step * RING + ((slab // 2) & (RING - 1))) * 2 + rank_s[batch]

        count = count + flag
    table_s[0] = count

    def fetch(i, which, source):
        return pltpu.make_async_copy(source, rows_ref.at[i, which], in_sem.at[i, which])

    def start_fetch(i, carry):
        batch = table_s[1 + i]
        fetch(i, 0, root_ref.at[batch]).start()
        fetch(i, 1, gain_ref.at[batch]).start()
        return carry

    lax.fori_loop(0, count, start_fetch, 0)

    at = lax.broadcasted_iota(jnp.int32, (2 * PAIRS, 128), 0)
    left = lax.broadcasted_iota(jnp.int32, (2 * PAIRS, 128), 1) < QUARTER
    slot = at // 2 + jnp.where(left == (lax.rem(at, 2) == 0), 0, PAIRS)
    for q in range(PAIRS):
        wanted = jnp.where(left, table_s[1 + 2 * q], table_s[2 + 2 * q])
        choice_ref[q] = jnp.where(wanted == slot, 1.0, 0.0)
    at = lax.broadcasted_iota(jnp.int32, (6 * RING, 128), 0)
    left = lax.broadcasted_iota(jnp.int32, (6 * RING, 128), 1) < QUARTER
    slot = at // 2 * 2 + jnp.where(left == (lax.rem(at, 2) == 0), 0, 1)
    for q in range(MORE // 2):
        wanted = jnp.where(left, code_s[2 * q], code_s[1 + 2 * q])
        direct_ref[q] = jnp.where(wanted == slot, 1.0, 0.0)

    values[:, 0:QUARTER] = value_ref[...]
    values[:, QUARTER:128] = value_ref[...]
    packet_ref[...] = jnp.zeros_like(packet_ref)
    lone_ref[...] = jnp.zeros_like(lone_ref)

    tail = lax.broadcasted_iota(jnp.int32, (16, 128), 0)
    for c in range(GROUPS):
        lanes = pl.ds(c * 128, 128)
        state[MEMBERS:ROWS, lanes] = jnp.where(tail == 0, -mean_ref[pl.ds(c, 1), :], 0.0)
    load.wait()
    for c in range(GROUPS):
        state[0:MEMBERS, pl.ds(c * 128, 128)] = raw[pl.ds(c, MEMBERS, stride=GROUPS), :]

    def pick(batch, carry):
        @pl.when(owner_s[batch] == column)
        def _():
            half = batch // PAIRS
            pair = lax.rem(batch, PAIRS)
            cells = jnp.broadcast_to(cell_ref[pl.ds(batch, 1), :], (8, OBS))
            shift = lax.rem(half * QUARTER - band * QUARTER + OBS, OBS)
            mine = pltpu.roll(cells, shift, 1)[0:1, 0:128]
            spot = lax.broadcasted_iota(jnp.int32, (1, 128), 1)
            valid = (spot // QUARTER) == half
            mine = jnp.where(valid, mine, -1)
            picked = jnp.zeros((ROWS, 128), F32)
            step = 512
            for at in range(0, CELLS, step):
                ids = lax.broadcasted_iota(jnp.int32, (step, 128), 0) + at
                hot = jnp.where(ids == mine, 1.0, 0.0).astype(BF16)
                block = state[:, pl.ds(at, step)]
                high = block.astype(BF16)
                rest = block - high.astype(F32)
                mid = rest.astype(BF16)
                last = (rest - mid.astype(F32)).astype(BF16)
                picked = picked + (dot(high, hot) + (dot(mid, hot) + dot(last, hot)))
            row = lax.broadcasted_iota(jnp.int32, (ROWS, 128), 0)
            seen = jnp.where(valid, values[pl.ds(batch, 1), :], 0.0)
            picked = picked + jnp.where(row == MEMBERS, seen, 0.0)
            packet_ref[pair] = packet_ref[pair] + picked
            turn = lax.rem(rank_s[batch] + half, 2) * QUARTER
            lone_ref[...] = lone_ref[...] + pltpu.roll(picked, turn, 1)

        return carry

    lax.fori_loop(0, BATCHES, pick, 0)

    def finish(i, carry):
        fetch(i, 0, root_ref.at[0]).wait()
        fetch(i, 1, gain_ref.at[0]).wait()
        return carry

    lax.fori_loop(0, count, finish, 0)


def comm_kernel(
    listed, planes, packet_ref, choice_ref, rows_ref, spread_ref, full_ref,
    mixed, rx_core, rx_y, plane, rx_z, slots,
    core_s, core_r, y_s, y_r, z_s, z_r, back_s, back_r, x_s, x_r, pair_s, pair_r,
    mat_s, mat_r, far_s, far_r, twin_s, twin_r,
):
    column = lax.axis_index("gx")
    band = lax.axis_index("gy")
    core = lax.rem(column, 2)
    y = lax.rem(column // 2, RING)
    z = column // (2 * RING)
    partner = (z * RING + y) * 2 + 1 - core

    def at_y(step):
        return (z * RING + lax.rem(y + step, RING)) * 2 + core

    def at_z(step):
        return (lax.rem(z + step, RING) * RING + y) * 2 + core

    def at_x(step):
        return lax.rem(band + step, BANDS)

    def copy(src, dst, send, recv, gx, gy):
        return pltpu.make_async_remote_copy(
            src_ref=src, dst_ref=dst, send_sem=send, recv_sem=recv,
            device_id=(gx, gy), device_id_type=MESH,
        )

    barrier = pltpu.get_barrier_semaphore()
    peers = [(partner, band)]
    peers += [(at_y(d), band) for d in range(1, RING)]
    peers += [(at_z(d), band) for d in planes]
    peers += [(column, at_x(d)) for d in range(1, BANDS)]
    for peer in peers:
        pl.semaphore_signal(barrier, inc=1, device_id=peer, device_id_type=MESH)
    for which in range(2):
        own_rows = pl.ds(pl.multiple_of(band * QUARTER, 8), QUARTER)
        full_ref[:, which, own_rows, :] = rows_ref[pl.ds(0, listed), which]
    pl.semaphore_wait(barrier, len(peers))

    mine = pl.ds(pl.multiple_of(core * HALF, 8), HALF)
    other = pl.ds(pl.multiple_of((1 - core) * HALF, 8), HALF)
    sends = []

    def go(descriptor):
        descriptor.start()
        sends.append(descriptor)

    swap = copy(packet_ref.at[:, other, :], rx_core, core_s, core_r, partner, band)
    go(swap)

    def my_rows(of):
        return pl.ds(pl.multiple_of(of * QUARTER, 8), QUARTER)

    def landed(step, part, core):
        return full_ref.at[pl.ds(part * few, few), core, my_rows(at_x(step)), :]

    few = listed // 2
    for way, part in ((0, 0), (1, 1), (0, 1), (1, 0)):
        source = rows_ref.at[pl.ds(part * few, few), core]
        go(copy(source, landed(0, part, core), mat_s.at[way, part], mat_r.at[way, part], column, at_x(1 if way == 0 else 3)))

    def arrived(way, part, step):
        here = landed(step, part, core)
        copy(here, here, mat_s.at[way, part], mat_r.at[way, part], column, at_x(3 if way == 0 else 1)).wait_recv()
        return here

    def to_twin(here, index):
        go(copy(here, here, twin_s.at[index], twin_r.at[index], partner, band))

    swap.wait_recv()
    mixed[...] = packet_ref[:, mine, :] + rx_core[...]

    for d in (4, 3, 5, 2, 6, 1, 7):
        go(copy(mixed.at[lax.rem(y + d, RING)], rx_y.at[d - 1], y_s.at[d - 1], y_r.at[d - 1], at_y(d), band))
    part = mixed[y]
    for d in (1, 7, 2, 6, 3, 5, 4):
        copy(mixed.at[0], rx_y.at[d - 1], y_s.at[d - 1], y_r.at[d - 1], at_y(RING - d), band).wait_recv()
        part = part + rx_y[d - 1]
    plane[...] = part
    from_left = arrived(0, 0, 3)
    from_right = arrived(1, 1, 1)

    for d in planes:
        go(copy(plane, rx_z.at[d - 1], z_s.at[d - 1], z_r.at[d - 1], at_z(d), band))
    go(copy(from_left, from_left, far_s.at[0], far_r.at[0], column, at_x(1)))
    go(copy(from_right, from_right, far_s.at[1], far_r.at[1], column, at_x(3)))
    to_twin(from_left, 0)
    to_twin(from_right, 1)
    for d in reversed(planes):
        copy(plane, rx_z.at[d - 1], z_s.at[d - 1], z_r.at[d - 1], at_z(RING - d), band).wait_recv()
        part = part + rx_z[d - 1]
    slots[y] = part
    own = slots.at[y]
    for d in (4, 3, 5, 2, 6, 1, 7):
        go(copy(own, own, back_s.at[d - 1], back_r.at[d - 1], at_y(d), band))
    to_twin(arrived(0, 1, 3), 2)
    to_twin(arrived(1, 0, 1), 3)
    for d in (1, 7, 2, 6, 3, 5, 4):
        here = slots.at[lax.rem(y + RING - d, RING)]
        copy(here, here, back_s.at[d - 1], back_r.at[d - 1], at_y(RING - d), band).wait_recv()

    chosen = [jnp.zeros((HALF, 128), F32)] * (listed // 2)
    for p in range(PAIRS):
        straight = slots[p]
        crossed = pltpu.roll(straight, QUARTER, 1)
        for q in range(listed // 2):
            chosen[q] = chosen[q] + (
                straight * choice_ref[q, 2 * p : 2 * p + 1, :]
                + crossed * choice_ref[q, 2 * p + 1 : 2 * p + 2, :]
            )
    for q in range(listed // 2):
        spread_ref[band, q, mine, :] = chosen[q]

    def part_of(x, rows):
        return spread_ref.at[x, :, rows, :]

    here = part_of(band, mine)
    for e in (2, 1, 3):
        go(copy(here, here, x_s.at[e - 1], x_r.at[e - 1], column, at_x(e)))
    go(copy(here, here, pair_s.at[0], pair_r.at[0], partner, band))
    for part in (0, 1):
        there = landed(2, part, core)
        copy(there, there, far_s.at[part], far_r.at[part], column, at_x(3 if part == 0 else 1)).wait_recv()
        to_twin(there, 4 + part)
    for e in (1, 3, 2):
        here = part_of(at_x(BANDS - e), mine)
        copy(here, here, x_s.at[e - 1], x_r.at[e - 1], column, at_x(BANDS - e)).wait_recv()
        go(copy(here, here, pair_s.at[e], pair_r.at[e], partner, band))

    for e in range(BANDS):
        there = part_of(at_x(BANDS - e), other)
        copy(there, there, pair_s.at[e], pair_r.at[e], partner, band).wait_recv()
    for index, step, part in ((0, 3, 0), (1, 1, 1), (2, 3, 1), (3, 1, 0), (4, 2, 0), (5, 2, 1)):
        there = landed(step, part, 1 - core)
        copy(there, there, twin_s.at[index], twin_r.at[index], partner, band).wait_recv()
    for descriptor in sends:
        descriptor.wait_send()


def direct_kernel(
    listed, lone_ref, direct_ref, rows_ref, spread_ref, full_ref,
    slots, rx_core,
    core_s, core_r, y_s, y_r, z_s, z_r, x_s, x_r, pair_s, pair_r,
    mat_s, mat_r, far_s, far_r, twin_s, twin_r,
):
    column = lax.axis_index("gx")
    band = lax.axis_index("gy")
    core = lax.rem(column, 2)
    y = lax.rem(column // 2, RING)
    z = column // (2 * RING)
    partner = (z * RING + y) * 2 + 1 - core

    def at_y(step):
        return (z * RING + lax.rem(y + step, RING)) * 2 + core

    def at_z(step):
        return (lax.rem(z + step, RING) * RING + y) * 2 + core

    def at_x(step):
        return lax.rem(band + step, BANDS)

    def copy(src, dst, send, recv, gx, gy):
        return pltpu.make_async_remote_copy(
            src_ref=src, dst_ref=dst, send_sem=send, recv_sem=recv,
            device_id=(gx, gy), device_id_type=MESH,
        )

    slots[1:3] = jnp.zeros((2, RING, HALF, 128), F32)

    barrier = pltpu.get_barrier_semaphore()
    peers = [(partner, band)]
    peers += [(at_y(d), band) for d in range(1, RING)]
    peers += [(at_z(d), band) for d in (1, RING - 1)]
    peers += [(column, at_x(d)) for d in range(1, BANDS)]
    for peer in peers:
        pl.semaphore_signal(barrier, inc=1, device_id=peer, device_id_type=MESH)
    for which in range(2):
        own_rows = pl.ds(pl.multiple_of(band * QUARTER, 8), QUARTER)
        full_ref[:, which, own_rows, :] = rows_ref[pl.ds(0, listed), which]
    pl.semaphore_wait(barrier, len(peers))

    mine = pl.ds(pl.multiple_of(core * HALF, 8), HALF)
    other = pl.ds(pl.multiple_of((1 - core) * HALF, 8), HALF)
    sends = []

    def go(descriptor):
        descriptor.start()
        sends.append(descriptor)

    swap = copy(lone_ref.at[other, :], rx_core, core_s, core_r, partner, band)
    go(swap)

    def my_rows(of):
        return pl.ds(pl.multiple_of(of * QUARTER, 8), QUARTER)

    def landed(step, part, core):
        return full_ref.at[pl.ds(part * few, few), core, my_rows(at_x(step)), :]

    few = listed // 2
    for way, part in ((0, 0), (1, 1), (0, 1), (1, 0)):
        source = rows_ref.at[pl.ds(part * few, few), core]
        go(copy(source, landed(0, part, core), mat_s.at[way, part], mat_r.at[way, part], column, at_x(1 if way == 0 else 3)))

    def arrived(way, part, step):
        here = landed(step, part, core)
        copy(here, here, mat_s.at[way, part], mat_r.at[way, part], column, at_x(3 if way == 0 else 1)).wait_recv()
        return here

    def to_twin(here, index):
        go(copy(here, here, twin_s.at[index], twin_r.at[index], partner, band))

    swap.wait_recv()
    slots[0, y] = lone_ref[mine, :] + rx_core[...]

    def next_plane(d):
        home = lax.rem(y + RING - d, RING)
        moves = []
        if d <= WINDOW:
            moves.append((y < d, 0, home, 2, 1))
        if d >= RING - WINDOW:
            moves.append((y >= d, 1, home, 1, RING - 1))
        return moves

    def over_z(d, act, back):
        for here, way, home, slot, step in next_plane(d):
            @pl.when(here)
            def _(way=way, home=home, slot=slot, step=RING - step if back else step):
                act(copy(
                    slots.at[0, home], slots.at[slot, home], z_s.at[way, d], z_r.at[way, d], at_z(step), band
                ))

    own = slots.at[0, y]
    for d in (4, 3, 5, 2, 6, 1, 7):
        go(copy(own, own, y_s.at[d - 1], y_r.at[d - 1], at_y(d), band))
    for d in (1, 7, 2, 6, 3, 5, 4):
        home = lax.rem(y + RING - d, RING)
        here = slots.at[0, home]
        copy(here, here, y_s.at[d - 1], y_r.at[d - 1], at_y(RING - d), band).wait_recv()
        over_z(d, lambda c: c.start(), False)

    from_left = arrived(0, 0, 3)
    from_right = arrived(1, 1, 1)
    to_twin(from_left, 0)
    to_twin(from_right, 1)
    go(copy(from_left, from_left, far_s.at[0], far_r.at[0], column, at_x(1)))
    go(copy(from_right, from_right, far_s.at[1], far_r.at[1], column, at_x(3)))

    chosen = [jnp.zeros((HALF, 128), F32)] * (listed // 2)

    def choose(step, home):
        at = 2 * (step * RING + home)
        straight = slots[step, home]
        crossed = pltpu.roll(straight, QUARTER, 1)
        for q in range(listed // 2):
            chosen[q] = chosen[q] + (
                straight * direct_ref[q, pl.ds(at, 1), :] + crossed * direct_ref[q, pl.ds(at + 1, 1), :]
            )

    for home in range(RING):
        choose(0, home)
    for d in (1, 7, 2, 6, 3, 5, 4):
        over_z(d, lambda c: c.wait_recv(), True)
        choose(jnp.where(y < d, 2, 1), lax.rem(y + RING - d, RING))
    for q in range(listed // 2):
        spread_ref[band, q, mine, :] = chosen[q]

    def part_of(x, rows):
        return spread_ref.at[x, :, rows, :]

    here = part_of(band, mine)
    for e in (2, 1, 3):
        go(copy(here, here, x_s.at[e - 1], x_r.at[e - 1], column, at_x(e)))
    go(copy(here, here, pair_s.at[0], pair_r.at[0], partner, band))
    to_twin(arrived(0, 1, 3), 2)
    to_twin(arrived(1, 0, 1), 3)
    for e in (1, 3, 2):
        here = part_of(at_x(BANDS - e), mine)
        copy(here, here, x_s.at[e - 1], x_r.at[e - 1], column, at_x(BANDS - e)).wait_recv()
        go(copy(here, here, pair_s.at[e], pair_r.at[e], partner, band))
    for part in (0, 1):
        there = landed(2, part, core)
        copy(there, there, far_s.at[part], far_r.at[part], column, at_x(3 if part == 0 else 1)).wait_recv()
        to_twin(there, 4 + part)

    for e in range(BANDS):
        there = part_of(at_x(BANDS - e), other)
        copy(there, there, pair_s.at[e], pair_r.at[e], partner, band).wait_recv()
    for index, step, part in ((0, 3, 0), (1, 1, 1), (2, 3, 1), (3, 1, 0), (4, 2, 0), (5, 2, 1)):
        there = landed(step, part, 1 - core)
        copy(there, there, twin_s.at[index], twin_r.at[index], partner, band).wait_recv()
    for d in range(1, RING):
        over_z(d, lambda c: c.wait_send(), False)
    for descriptor in sends:
        descriptor.wait_send()


def solve_kernel(
    owner_s, table_s, before_ref, cell_ref, spread_ref, full_ref,
    out_anom_ref, out_mean_ref,
    state, prior,
):
    column = lax.axis_index("gx")
    band = lax.axis_index("gy")
    count = table_s[0]

    state[...] = before_ref[...]

    left = lax.broadcasted_iota(jnp.int32, (ROWS, 128), 1) < QUARTER
    for q in range(spread_ref.shape[1]):
        for x in (0, 2):
            first = spread_ref[x, q]
            second = spread_ref[x + 1, q]
            lanes = pl.ds(x * QUARTER, 128)
            prior[2 * q, :, lanes] = jnp.where(left, first, pltpu.roll(second, QUARTER, 1))
            prior[2 * q + 1, :, lanes] = jnp.where(left, pltpu.roll(first, QUARTER, 1), second)

    spot = lax.broadcasted_iota(jnp.int32, (1, OBS), 1)
    scale = 1.0 / (7.0 * 32.0 * 79.0)

    def places(batch):
        cells = cell_ref[pl.ds(batch, 1), :]
        lon = owner_s[batch] * 2 + cells // 1024
        lat = (spot // QUARTER) * 8 + lax.rem(cells // 128, 8)
        return lon, lat

    def taper(lon_gap, lat_gap):
        lon_gap = jnp.minimum(lon_gap, NLON - lon_gap)
        return (
            jnp.maximum(7 - lon_gap, 0).astype(F32) * (NLAT - lat_gap).astype(F32) * scale
        )

    row = lax.broadcasted_iota(jnp.int32, (ROWS, OBS), 0)

    def assimilate(i, carry):
        batch = table_s[1 + i]
        slab = owner_s[batch]
        z = prior[i]
        turned = jnp.transpose(jnp.concatenate([z, jnp.zeros((128 - ROWS, OBS), F32)], axis=0))
        gained = jnp.sum(full_ref[i, 1] * turned[:, MEMBERS : MEMBERS + 1], axis=0, keepdims=True)
        z_high, z_low = split(z)
        root_high, root_low = split(full_ref[i, 0])
        weighted = dot(jnp.concatenate([z_high, z_low], axis=0), root_high)
        weighted = weighted[0:ROWS] + (weighted[ROWS : 2 * ROWS] + dot(z_high, root_low))
        weights = jnp.where(row < MEMBERS, weighted, jnp.where(row == MEMBERS, gained, 0.0))
        column_id = lax.broadcasted_iota(jnp.int32, (OBS, 128), 1)
        turned_high, turned_low = split(jnp.where(column_id < MEMBERS, turned, 0.0))
        turned_both = jnp.concatenate([turned_high, turned_low], axis=1)
        short_high, short_low = turned_high[:, 0:ROWS], turned_low[:, 0:ROWS]
        lon, lat = places(batch)
        both = jnp.concatenate(
            [jnp.broadcast_to(lon, (8, OBS)), jnp.broadcast_to(lat, (8, OBS))], axis=0
        ).astype(F32)
        upright = jnp.transpose(both).astype(jnp.int32)
        lon_col = upright[:, 0:1]
        lat_col = upright[:, 8:9]

        weights_high, weights_low = split(weights)

        def later(j, carry):
            other = table_s[1 + j]

            @pl.when(dist(owner_s[other], slab) <= REACH)
            def _():
                held = prior[j]
                held_high, held_low = split(held)
                covariance = dot3(short_high, short_low, held_high, held_low)
                lon_j, lat_j = places(other)
                gain = covariance * taper(jnp.abs(lon_col - lon_j), jnp.abs(lat_col - lat_j))
                gain_h, gain_l = split(gain)
                prior[j] = held - dot3(weights_high, weights_low, gain_h, gain_l)

            return carry

        lax.fori_loop(i + 1, count, later, 0)

        @pl.when(dist(slab, column) <= REACH)
        def _():
            for at in range(0, GROUPS, BUNDLE):
                highs, lows = [], []
                for c in range(at, at + BUNDLE):
                    cell_lon = column * 2 + c // 8
                    cell_lat = band * 8 + c % 8
                    factor = taper(jnp.abs(lon - cell_lon), jnp.abs(lat - cell_lat))
                    high, low = split(weights * factor)
                    highs.append(high)
                    lows.append(low)
                wide = dot(jnp.concatenate(highs, axis=0), turned_both)
                middle = wide[:, 0:128] + (wide[:, 128:256] + dot(jnp.concatenate(lows, axis=0), turned_high))
                middle = middle[:, 0:ROWS]
                for c in range(at, at + BUNDLE):
                    lanes = pl.ds(c * 128, 128)
                    block = state[:, lanes]
                    m_high, m_low = split(middle[(c - at) * ROWS : (c - at + 1) * ROWS])
                    b_high, b_low = split(block)
                    moved = dot(m_high, jnp.concatenate([b_high, b_low], axis=1))
                    state[:, lanes] = block - (moved[:, 0:128] + (moved[:, 128:256] + dot(m_low, b_high)))

        return carry

    lax.fori_loop(0, count, assimilate, 0)

    for c in range(GROUPS):
        lanes = pl.ds(c * 128, 128)
        out_anom_ref[pl.ds(c, MEMBERS, stride=GROUPS), :] = state[0:MEMBERS, lanes]
        out_mean_ref[pl.ds(c, 1), :] = -state[pl.ds(MEMBERS, 1), lanes]


VMEM = pl.BlockSpec(memory_space=pltpu.VMEM)
SMEM = pl.BlockSpec(memory_space=pltpu.SMEM)
HBM = pl.BlockSpec(memory_space=pl.ANY)
DMA = pltpu.SemaphoreType.DMA


def exchange(listed, planes, collective_id, packet, choice, rows):
    return pl.pallas_call(
        functools.partial(comm_kernel, listed, planes),
        name="exchange",
        out_shape=(
            jax.ShapeDtypeStruct((BANDS, listed // 2, ROWS, 128), F32),
            jax.ShapeDtypeStruct((listed, 2, OBS, OBS), F32),
        ),
        in_specs=[VMEM, VMEM, VMEM],
        out_specs=(VMEM, VMEM),
        scratch_shapes=[
            pltpu.VMEM((PAIRS, HALF, 128), F32),
            pltpu.VMEM((PAIRS, HALF, 128), F32),
            pltpu.VMEM((RING - 1, HALF, 128), F32),
            pltpu.VMEM((HALF, 128), F32),
            pltpu.VMEM((RING - 1, HALF, 128), F32),
            pltpu.VMEM((PAIRS, HALF, 128), F32),
            DMA, DMA,
            DMA((RING - 1,)), DMA((RING - 1,)),
            DMA((RING - 1,)), DMA((RING - 1,)),
            DMA((RING - 1,)), DMA((RING - 1,)),
            DMA((BANDS - 1,)), DMA((BANDS - 1,)),
            DMA((BANDS,)), DMA((BANDS,)),
            DMA((2, 2)), DMA((2, 2)),
            DMA((2,)), DMA((2,)),
            DMA((6,)), DMA((6,)),
        ],
        compiler_params=pltpu.CompilerParams(collective_id=collective_id, has_side_effects=True, vmem_limit_bytes=GRANT),
    )(packet, choice, rows)


def direct(listed, collective_id, lone, choice, rows):
    return pl.pallas_call(
        functools.partial(direct_kernel, listed),
        name="direct",
        out_shape=(
            jax.ShapeDtypeStruct((BANDS, listed // 2, ROWS, 128), F32),
            jax.ShapeDtypeStruct((listed, 2, OBS, OBS), F32),
        ),
        in_specs=[VMEM, VMEM, VMEM],
        out_specs=(VMEM, VMEM),
        scratch_shapes=[
            pltpu.VMEM((3, RING, HALF, 128), F32),
            pltpu.VMEM((HALF, 128), F32),
            DMA, DMA,
            DMA((RING - 1,)), DMA((RING - 1,)),
            DMA((2, RING)), DMA((2, RING)),
            DMA((BANDS - 1,)), DMA((BANDS - 1,)),
            DMA((BANDS,)), DMA((BANDS,)),
            DMA((2, 2)), DMA((2, 2)),
            DMA((2,)), DMA((2,)),
            DMA((6,)), DMA((6,)),
        ],
        compiler_params=pltpu.CompilerParams(collective_id=collective_id, has_side_effects=True, vmem_limit_bytes=GRANT),
    )(lone, choice, rows)


def solve(listed, owner, table, state, obs_cell, spread, full):
    return pl.pallas_call(
        solve_kernel,
        name="solve",
        out_shape=(
            jax.ShapeDtypeStruct((MEMBERS * GROUPS, 128), F32),
            jax.ShapeDtypeStruct((GROUPS, 128), F32),
        ),
        in_specs=[SMEM, SMEM, VMEM, VMEM, VMEM, VMEM],
        out_specs=(VMEM, VMEM),
        scratch_shapes=[
            pltpu.VMEM((ROWS, CELLS), F32),
            pltpu.VMEM((listed, ROWS, OBS), F32),
        ],
        compiler_params=pltpu.CompilerParams(vmem_limit_bytes=GRANT),
    )(owner, table, state, obs_cell, spread, full)


def local(anomalies, state_mean, obs_value, obs_cell, owner, order, root_inv, gain_inv):
    flat = anomalies.reshape(MEMBERS * GROUPS, 128)
    mean = state_mean.reshape(GROUPS, 128)
    packet, lone, rows, choice, near_choice, state, table, branch = pl.pallas_call(
        prep_kernel,
        name="prep",
        out_shape=(
            jax.ShapeDtypeStruct((PAIRS, ROWS, 128), F32),
            jax.ShapeDtypeStruct((ROWS, 128), F32),
            jax.ShapeDtypeStruct((BATCHES, 2, QUARTER, OBS), F32),
            jax.ShapeDtypeStruct((PAIRS, 2 * PAIRS, 128), F32),
            jax.ShapeDtypeStruct((MORE // 2, 6 * RING, 128), F32),
            jax.ShapeDtypeStruct((ROWS, CELLS), F32),
            jax.ShapeDtypeStruct((32,), jnp.int32),
            jax.ShapeDtypeStruct((1,), jnp.int32),
        ),
        in_specs=[SMEM, SMEM, HBM, VMEM, VMEM, VMEM, HBM, HBM],
        out_specs=(VMEM, VMEM, HBM, VMEM, VMEM, VMEM, SMEM, SMEM),
        scratch_shapes=[
            pltpu.VMEM((MEMBERS * GROUPS, 128), F32),
            pltpu.VMEM((BATCHES, 128), F32),
            pltpu.SMEM((BATCHES,), jnp.int32),
            pltpu.SMEM((BATCHES,), jnp.int32),
            pltpu.SMEM((1,), jnp.int32),
            DMA,
            DMA((BATCHES, 2)),
        ],
    )(order, owner, flat, mean, obs_cell, obs_value, root_inv, gain_inv)

    def near(listed, collective_id):
        spread, full = direct(listed, collective_id, lone, near_choice, rows)
        return solve(listed, owner, table, state, obs_cell, spread, full)

    def wide(listed, planes, collective_id):
        spread, full = exchange(listed, planes, collective_id, packet, choice, rows)
        return solve(listed, owner, table, state, obs_cell, spread, full)

    out_flat, out_mean = lax.switch(
        branch[0],
        (
            lambda: near(FEW, 1),
            lambda: near(MORE, 2),
            lambda: wide(SOME, NEXT_PLANES, 3),
            lambda: wide(BATCHES, ALL_PLANES, 4),
        ),
    )
    return out_flat.reshape(anomalies.shape), out_mean.reshape(state_mean.shape)


def solution(mesh):
    return jax.shard_map(
        local,
        mesh=mesh,
        in_specs=(
            P(None, "gx", "gy", None),
            P("gx", "gy", None),
            P(None, "gy"),
            P(),
            P(),
            P(),
            P(None, "gy", None),
            P(None, "gy", None),
        ),
        out_specs=(P(None, "gx", "gy", None), P("gx", "gy", None)),
        check_vma=False,
    )
```

```python
import functools

import jax
import jax.numpy as jnp
from jax import lax
from jax.experimental import pallas as pl
from jax.experimental.pallas import tpu as pltpu
from jax.sharding import PartitionSpec as P

MEMBERS = 80
OBS = 256
BATCHES = 16
REACH = 3
SLABS = 128
CHIPS = 64
BANDS = 4
NLON = 256
NLAT = 32
QUARTER = 64
CELLS = 2048
GROUPS = 16
ROWS = 96
HALF = 48
PAIRS = 8
RING = 8
FEW = 4
MORE = 6
SOME = 8
WINDOW = 5
BUNDLE = 16
GRANT = 24 * 1024 * 1024
NEXT_PLANES = (1, 7)
ALL_PLANES = (4, 3, 5, 2, 6, 1, 7)
MESH = pl.DeviceIdType.MESH
F32 = jnp.float32
BF16 = jnp.bfloat16


def dist(a, b):
    gap = jnp.abs(a - b)
    return jnp.minimum(gap, SLABS - gap)


def split(value):
    high = value.astype(BF16)
    return high, (value - high.astype(F32)).astype(BF16)


def dot(left, right):
    return jnp.dot(left, right, preferred_element_type=F32)


def dot3(left_high, left_low, right_high, right_low):
    return dot(left_high, right_high) + (dot(left_high, right_low) + dot(left_low, right_high))


def prep_kernel(
    order_s, owner_s, anom_ref, mean_ref, cell_ref, value_ref, root_ref, gain_ref,
    packet_ref, lone_ref, rows_ref, choice_ref, direct_ref, state, table_s, branch_s,
    raw, values, rank_s, code_s, own_s, raw_sem, in_sem,
):
    column = lax.axis_index("gx")
    band = lax.axis_index("gy")
    load = pltpu.make_async_copy(anom_ref, raw, raw_sem)
    load.start()

    @pl.when(column >= 0)
    def _():
        lane = lax.broadcasted_iota(jnp.int32, (8, 128), 1)
        chip = lane & (CHIPS - 1)
        own_plane = chip // RING
        slabs = [owner_s[order_s[t]] for t in range(BATCHES)]
        needs = [None] * BATCHES
        bits = jnp.zeros((8, 128), jnp.int32)
        total = jnp.zeros((8, 128), jnp.int32)
        far = jnp.zeros((8, 128), jnp.int32)
        beyond = jnp.zeros((8, 128), jnp.int32)
        deepest = 0
        for t in reversed(range(BATCHES)):
            near = ((slabs[t] + REACH - 2 * chip) & (SLABS - 1)) <= 2 * REACH + 1
            need = jnp.where(near, -1, 0)
            for s in range(t + 1, BATCHES):
                linked = ((slabs[s] + REACH - slabs[t]) & (SLABS - 1)) <= 2 * REACH
                need = need | (needs[s] & jnp.where(linked, -1, 0))
            needs[t] = need
            bits = bits | (need & (1 << t))
            total = total - need
            far = far | jnp.where(((slabs[t] // (2 * RING) + 1 - own_plane) & (RING - 1)) > 2, need, 0)
            beyond = beyond | jnp.where(((slabs[t] // 2 + WINDOW - chip) & (CHIPS - 1)) > 2 * WINDOW, need, 0)
            rank = 0
            for s in range(t):
                rank = rank + jnp.where(slabs[s] // 2 == slabs[t] // 2, 1, 0)
            rank_s[order_s[t]] = rank
            deepest = jnp.maximum(deepest, rank)
        own_s[0] = jnp.max(jnp.where(lane == column // 2, bits, 0))
        longest = jnp.max(total + (far & (2 * BATCHES)))
        beyond_any = jnp.max(beyond & 1)
        branch_s[0] = jnp.where(
            longest > SOME,
            3,
            jnp.where((deepest > 1) | (beyond_any > 0) | (longest > MORE), 2, jnp.where(longest > FEW, 1, 0)),
        )

    mine = own_s[0]
    for i in range(BATCHES):
        table_s[1 + i] = -1
        code_s[i] = -1
    count = 0
    for t in range(BATCHES):
        flag = (mine >> t) & 1

        @pl.when(flag == 1)
        def _(t=t, count=count):
            batch = order_s[t]
            slab = owner_s[batch]
            step = (slab // (2 * RING) - column // (2 * RING)) & (RING - 1)
            step = jnp.where(step == RING - 1, 2, step)
            table_s[1 + count] = batch
            code_s[count] = (step * RING + ((slab // 2) & (RING - 1))) * 2 + rank_s[batch]

        count = count + flag
    table_s[0] = count

    def fetch(i, which, source):
        return pltpu.make_async_copy(source, rows_ref.at[i, which], in_sem.at[i, which])

    def start_fetch(i, carry):
        batch = table_s[1 + i]
        fetch(i, 0, root_ref.at[batch]).start()
        fetch(i, 1, gain_ref.at[batch]).start()
        return carry

    lax.fori_loop(0, count, start_fetch, 0)

    at = lax.broadcasted_iota(jnp.int32, (2 * PAIRS, 128), 0)
    left = lax.broadcasted_iota(jnp.int32, (2 * PAIRS, 128), 1) < QUARTER
    slot = at // 2 + jnp.where(left == (lax.rem(at, 2) == 0), 0, PAIRS)
    for q in range(PAIRS):
        wanted = jnp.where(left, table_s[1 + 2 * q], table_s[2 + 2 * q])
        choice_ref[q] = jnp.where(wanted == slot, 1.0, 0.0)
    at = lax.broadcasted_iota(jnp.int32, (6 * RING, 128), 0)
    left = lax.broadcasted_iota(jnp.int32, (6 * RING, 128), 1) < QUARTER
    slot = at // 2 * 2 + jnp.where(left == (lax.rem(at, 2) == 0), 0, 1)
    for q in range(MORE // 2):
        wanted = jnp.where(left, code_s[2 * q], code_s[1 + 2 * q])
        direct_ref[q] = jnp.where(wanted == slot, 1.0, 0.0)

    values[:, 0:QUARTER] = value_ref[...]
    values[:, QUARTER:128] = value_ref[...]
    packet_ref[...] = jnp.zeros_like(packet_ref)
    lone_ref[...] = jnp.zeros_like(lone_ref)

    tail = lax.broadcasted_iota(jnp.int32, (16, 128), 0)
    for c in range(GROUPS):
        lanes = pl.ds(c * 128, 128)
        state[MEMBERS:ROWS, lanes] = jnp.where(tail == 0, -mean_ref[pl.ds(c, 1), :], 0.0)
    load.wait()
    for c in range(GROUPS):
        state[0:MEMBERS, pl.ds(c * 128, 128)] = raw[pl.ds(c, MEMBERS, stride=GROUPS), :]

    def pick(batch, carry):
        @pl.when(owner_s[batch] == column)
        def _():
            half = batch // PAIRS
            pair = lax.rem(batch, PAIRS)
            cells = jnp.broadcast_to(cell_ref[pl.ds(batch, 1), :], (8, OBS))
            shift = lax.rem(half * QUARTER - band * QUARTER + OBS, OBS)
            mine = pltpu.roll(cells, shift, 1)[0:1, 0:128]
            spot = lax.broadcasted_iota(jnp.int32, (1, 128), 1)
            valid = (spot // QUARTER) == half
            mine = jnp.where(valid, mine, -1)
            picked = jnp.zeros((ROWS, 128), F32)
            step = 512
            for at in range(0, CELLS, step):
                ids = lax.broadcasted_iota(jnp.int32, (step, 128), 0) + at
                hot = jnp.where(ids == mine, 1.0, 0.0).astype(BF16)
                block = state[:, pl.ds(at, step)]
                high = block.astype(BF16)
                rest = block - high.astype(F32)
                mid = rest.astype(BF16)
                last = (rest - mid.astype(F32)).astype(BF16)
                both = dot(jnp.concatenate([high, mid, last], axis=0), hot)
                picked = picked + (both[0:ROWS] + (both[ROWS : 2 * ROWS] + both[2 * ROWS : 3 * ROWS]))
            row = lax.broadcasted_iota(jnp.int32, (ROWS, 128), 0)
            seen = jnp.where(valid, values[pl.ds(batch, 1), :], 0.0)
            picked = picked + jnp.where(row == MEMBERS, seen, 0.0)
            packet_ref[pair] = packet_ref[pair] + picked
            turn = lax.rem(rank_s[batch] + half, 2) * QUARTER
            lone_ref[...] = lone_ref[...] + pltpu.roll(picked, turn, 1)

        return carry

    lax.fori_loop(0, BATCHES, pick, 0)

    def finish(i, carry):
        fetch(i, 0, root_ref.at[0]).wait()
        fetch(i, 1, gain_ref.at[0]).wait()
        return carry

    lax.fori_loop(0, count, finish, 0)


def comm_kernel(
    listed, planes, packet_ref, choice_ref, rows_ref, spread_ref, full_ref,
    mixed, rx_core, rx_y, plane, rx_z, slots,
    core_s, core_r, y_s, y_r, z_s, z_r, back_s, back_r, x_s, x_r, pair_s, pair_r,
    mat_s, mat_r, far_s, far_r, twin_s, twin_r,
):
    column = lax.axis_index("gx")
    band = lax.axis_index("gy")
    core = lax.rem(column, 2)
    y = lax.rem(column // 2, RING)
    z = column // (2 * RING)
    partner = (z * RING + y) * 2 + 1 - core

    def at_y(step):
        return (z * RING + lax.rem(y + step, RING)) * 2 + core

    def at_z(step):
        return (lax.rem(z + step, RING) * RING + y) * 2 + core

    def at_x(step):
        return lax.rem(band + step, BANDS)

    def copy(src, dst, send, recv, gx, gy):
        return pltpu.make_async_remote_copy(
            src_ref=src, dst_ref=dst, send_sem=send, recv_sem=recv,
            device_id=(gx, gy), device_id_type=MESH,
        )

    barrier = pltpu.get_barrier_semaphore()
    peers = [(partner, band)]
    peers += [(at_y(d), band) for d in range(1, RING)]
    peers += [(at_z(d), band) for d in planes]
    peers += [(column, at_x(d)) for d in range(1, BANDS)]
    for peer in peers:
        pl.semaphore_signal(barrier, inc=1, device_id=peer, device_id_type=MESH)
    for which in range(2):
        own_rows = pl.ds(pl.multiple_of(band * QUARTER, 8), QUARTER)
        full_ref[:, which, own_rows, :] = rows_ref[pl.ds(0, listed), which]
    pl.semaphore_wait(barrier, len(peers))

    mine = pl.ds(pl.multiple_of(core * HALF, 8), HALF)
    other = pl.ds(pl.multiple_of((1 - core) * HALF, 8), HALF)
    sends = []

    def go(descriptor):
        descriptor.start()
        sends.append(descriptor)

    swap = copy(packet_ref.at[:, other, :], rx_core, core_s, core_r, partner, band)
    go(swap)

    def my_rows(of):
        return pl.ds(pl.multiple_of(of * QUARTER, 8), QUARTER)

    def landed(step, part, core):
        return full_ref.at[pl.ds(part * few, few), core, my_rows(at_x(step)), :]

    few = listed // 2
    for way, part in ((0, 0), (1, 1), (0, 1), (1, 0)):
        source = rows_ref.at[pl.ds(part * few, few), core]
        go(copy(source, landed(0, part, core), mat_s.at[way, part], mat_r.at[way, part], column, at_x(1 if way == 0 else 3)))

    def arrived(way, part, step):
        here = landed(step, part, core)
        copy(here, here, mat_s.at[way, part], mat_r.at[way, part], column, at_x(3 if way == 0 else 1)).wait_recv()
        return here

    def to_twin(here, index):
        go(copy(here, here, twin_s.at[index], twin_r.at[index], partner, band))

    swap.wait_recv()
    mixed[...] = packet_ref[:, mine, :] + rx_core[...]

    for d in (4, 3, 5, 2, 6, 1, 7):
        go(copy(mixed.at[lax.rem(y + d, RING)], rx_y.at[d - 1], y_s.at[d - 1], y_r.at[d - 1], at_y(d), band))
    part = mixed[y]
    for d in (1, 7, 2, 6, 3, 5, 4):
        copy(mixed.at[0], rx_y.at[d - 1], y_s.at[d - 1], y_r.at[d - 1], at_y(RING - d), band).wait_recv()
        part = part + rx_y[d - 1]
    plane[...] = part
    from_left = arrived(0, 0, 3)
    from_right = arrived(1, 1, 1)

    for d in planes:
        go(copy(plane, rx_z.at[d - 1], z_s.at[d - 1], z_r.at[d - 1], at_z(d), band))
    go(copy(from_left, from_left, far_s.at[0], far_r.at[0], column, at_x(1)))
    go(copy(from_right, from_right, far_s.at[1], far_r.at[1], column, at_x(3)))
    to_twin(from_left, 0)
    to_twin(from_right, 1)
    for d in reversed(planes):
        copy(plane, rx_z.at[d - 1], z_s.at[d - 1], z_r.at[d - 1], at_z(RING - d), band).wait_recv()
        part = part + rx_z[d - 1]
    slots[y] = part
    own = slots.at[y]
    for d in (4, 3, 5, 2, 6, 1, 7):
        go(copy(own, own, back_s.at[d - 1], back_r.at[d - 1], at_y(d), band))
    to_twin(arrived(0, 1, 3), 2)
    to_twin(arrived(1, 0, 1), 3)
    for d in (1, 7, 2, 6, 3, 5, 4):
        here = slots.at[lax.rem(y + RING - d, RING)]
        copy(here, here, back_s.at[d - 1], back_r.at[d - 1], at_y(RING - d), band).wait_recv()

    chosen = [jnp.zeros((HALF, 128), F32)] * (listed // 2)
    for p in range(PAIRS):
        straight = slots[p]
        crossed = pltpu.roll(straight, QUARTER, 1)
        for q in range(listed // 2):
            chosen[q] = chosen[q] + (
                straight * choice_ref[q, 2 * p : 2 * p + 1, :]
                + crossed * choice_ref[q, 2 * p + 1 : 2 * p + 2, :]
            )
    for q in range(listed // 2):
        spread_ref[band, q, mine, :] = chosen[q]

    def part_of(x, rows):
        return spread_ref.at[x, :, rows, :]

    here = part_of(band, mine)
    for e in (2, 1, 3):
        go(copy(here, here, x_s.at[e - 1], x_r.at[e - 1], column, at_x(e)))
    go(copy(here, here, pair_s.at[0], pair_r.at[0], partner, band))
    for part in (0, 1):
        there = landed(2, part, core)
        copy(there, there, far_s.at[part], far_r.at[part], column, at_x(3 if part == 0 else 1)).wait_recv()
        to_twin(there, 4 + part)
    for e in (1, 3, 2):
        here = part_of(at_x(BANDS - e), mine)
        copy(here, here, x_s.at[e - 1], x_r.at[e - 1], column, at_x(BANDS - e)).wait_recv()
        go(copy(here, here, pair_s.at[e], pair_r.at[e], partner, band))

    for e in range(BANDS):
        there = part_of(at_x(BANDS - e), other)
        copy(there, there, pair_s.at[e], pair_r.at[e], partner, band).wait_recv()
    for index, step, part in ((0, 3, 0), (1, 1, 1), (2, 3, 1), (3, 1, 0), (4, 2, 0), (5, 2, 1)):
        there = landed(step, part, 1 - core)
        copy(there, there, twin_s.at[index], twin_r.at[index], partner, band).wait_recv()
    for descriptor in sends:
        descriptor.wait_send()


def direct_kernel(
    listed, lone_ref, direct_ref, rows_ref, spread_ref, full_ref,
    slots, rx_core,
    core_s, core_r, y_s, y_r, z_s, z_r, x_s, x_r, pair_s, pair_r,
    mat_s, mat_r, far_s, far_r, twin_s, twin_r,
):
    column = lax.axis_index("gx")
    band = lax.axis_index("gy")
    core = lax.rem(column, 2)
    y = lax.rem(column // 2, RING)
    z = column // (2 * RING)
    partner = (z * RING + y) * 2 + 1 - core

    def at_y(step):
        return (z * RING + lax.rem(y + step, RING)) * 2 + core

    def at_z(step):
        return (lax.rem(z + step, RING) * RING + y) * 2 + core

    def at_x(step):
        return lax.rem(band + step, BANDS)

    def copy(src, dst, send, recv, gx, gy):
        return pltpu.make_async_remote_copy(
            src_ref=src, dst_ref=dst, send_sem=send, recv_sem=recv,
            device_id=(gx, gy), device_id_type=MESH,
        )

    slots[1:3] = jnp.zeros((2, RING, HALF, 128), F32)

    barrier = pltpu.get_barrier_semaphore()
    peers = [(partner, band)]
    peers += [(at_y(d), band) for d in range(1, RING)]
    peers += [(at_z(d), band) for d in (1, RING - 1)]
    peers += [(column, at_x(d)) for d in range(1, BANDS)]
    for peer in peers:
        pl.semaphore_signal(barrier, inc=1, device_id=peer, device_id_type=MESH)
    for which in range(2):
        own_rows = pl.ds(pl.multiple_of(band * QUARTER, 8), QUARTER)
        full_ref[:, which, own_rows, :] = rows_ref[pl.ds(0, listed), which]
    pl.semaphore_wait(barrier, len(peers))

    mine = pl.ds(pl.multiple_of(core * HALF, 8), HALF)
    other = pl.ds(pl.multiple_of((1 - core) * HALF, 8), HALF)
    sends = []

    def go(descriptor):
        descriptor.start()
        sends.append(descriptor)

    swap = copy(lone_ref.at[other, :], rx_core, core_s, core_r, partner, band)
    go(swap)

    def my_rows(of):
        return pl.ds(pl.multiple_of(of * QUARTER, 8), QUARTER)

    def landed(step, part, core):
        return full_ref.at[pl.ds(part * few, few), core, my_rows(at_x(step)), :]

    few = listed // 2
    for way, part in ((0, 0), (1, 1), (0, 1), (1, 0)):
        source = rows_ref.at[pl.ds(part * few, few), core]
        go(copy(source, landed(0, part, core), mat_s.at[way, part], mat_r.at[way, part], column, at_x(1 if way == 0 else 3)))

    def arrived(way, part, step):
        here = landed(step, part, core)
        copy(here, here, mat_s.at[way, part], mat_r.at[way, part], column, at_x(3 if way == 0 else 1)).wait_recv()
        return here

    def to_twin(here, index):
        go(copy(here, here, twin_s.at[index], twin_r.at[index], partner, band))

    swap.wait_recv()
    slots[0, y] = lone_ref[mine, :] + rx_core[...]

    def next_plane(d):
        home = lax.rem(y + RING - d, RING)
        moves = []
        if d <= WINDOW:
            moves.append((y < d, 0, home, 2, 1))
        if d >= RING - WINDOW:
            moves.append((y >= d, 1, home, 1, RING - 1))
        return moves

    def over_z(d, act, back):
        for here, way, home, slot, step in next_plane(d):
            @pl.when(here)
            def _(way=way, home=home, slot=slot, step=RING - step if back else step):
                act(copy(
                    slots.at[0, home], slots.at[slot, home], z_s.at[way, d], z_r.at[way, d], at_z(step), band
                ))

    own = slots.at[0, y]
    for d in (1, 7, 2, 6, 3, 5, 4):
        go(copy(own, own, y_s.at[d - 1], y_r.at[d - 1], at_y(d), band))
    for d in (1, 7, 2, 6, 3, 5, 4):
        home = lax.rem(y + RING - d, RING)
        here = slots.at[0, home]
        copy(here, here, y_s.at[d - 1], y_r.at[d - 1], at_y(RING - d), band).wait_recv()
        over_z(d, lambda c: c.start(), False)

    from_left = arrived(0, 0, 3)
    from_right = arrived(1, 1, 1)
    to_twin(from_left, 0)
    to_twin(from_right, 1)
    go(copy(from_left, from_left, far_s.at[0], far_r.at[0], column, at_x(1)))
    go(copy(from_right, from_right, far_s.at[1], far_r.at[1], column, at_x(3)))

    chosen = [jnp.zeros((HALF, 128), F32)] * (listed // 2)

    def choose(step, home):
        at = 2 * (step * RING + home)
        straight = slots[step, home]
        crossed = pltpu.roll(straight, QUARTER, 1)
        for q in range(listed // 2):
            chosen[q] = chosen[q] + (
                straight * direct_ref[q, pl.ds(at, 1), :] + crossed * direct_ref[q, pl.ds(at + 1, 1), :]
            )

    for home in range(RING):
        choose(0, home)
    for d in (1, 7, 2, 6, 3, 5, 4):
        over_z(d, lambda c: c.wait_recv(), True)
        choose(jnp.where(y < d, 2, 1), lax.rem(y + RING - d, RING))
    for q in range(listed // 2):
        spread_ref[band, q, mine, :] = chosen[q]

    def part_of(x, rows):
        return spread_ref.at[x, :, rows, :]

    here = part_of(band, mine)
    for e in (2, 1, 3):
        go(copy(here, here, x_s.at[e - 1], x_r.at[e - 1], column, at_x(e)))
    go(copy(here, here, pair_s.at[0], pair_r.at[0], partner, band))
    to_twin(arrived(0, 1, 3), 2)
    to_twin(arrived(1, 0, 1), 3)
    for e in (1, 3, 2):
        here = part_of(at_x(BANDS - e), mine)
        copy(here, here, x_s.at[e - 1], x_r.at[e - 1], column, at_x(BANDS - e)).wait_recv()
        go(copy(here, here, pair_s.at[e], pair_r.at[e], partner, band))
    for part in (0, 1):
        there = landed(2, part, core)
        copy(there, there, far_s.at[part], far_r.at[part], column, at_x(3 if part == 0 else 1)).wait_recv()
        to_twin(there, 4 + part)

    for e in range(BANDS):
        there = part_of(at_x(BANDS - e), other)
        copy(there, there, pair_s.at[e], pair_r.at[e], partner, band).wait_recv()
    for index, step, part in ((0, 3, 0), (1, 1, 1), (2, 3, 1), (3, 1, 0), (4, 2, 0), (5, 2, 1)):
        there = landed(step, part, 1 - core)
        copy(there, there, twin_s.at[index], twin_r.at[index], partner, band).wait_recv()
    for d in range(1, RING):
        over_z(d, lambda c: c.wait_send(), False)
    for descriptor in sends:
        descriptor.wait_send()


def solve_kernel(
    owner_s, table_s, before_ref, cell_ref, spread_ref, full_ref,
    out_anom_ref, out_mean_ref,
    state, prior,
):
    column = lax.axis_index("gx")
    band = lax.axis_index("gy")
    count = table_s[0]

    state[...] = before_ref[...]

    left = lax.broadcasted_iota(jnp.int32, (ROWS, 128), 1) < QUARTER
    for q in range(spread_ref.shape[1]):
        for x in (0, 2):
            first = spread_ref[x, q]
            second = spread_ref[x + 1, q]
            lanes = pl.ds(x * QUARTER, 128)
            prior[2 * q, :, lanes] = jnp.where(left, first, pltpu.roll(second, QUARTER, 1))
            prior[2 * q + 1, :, lanes] = jnp.where(left, pltpu.roll(first, QUARTER, 1), second)

    spot = lax.broadcasted_iota(jnp.int32, (1, OBS), 1)
    scale = 1.0 / (7.0 * 32.0 * 79.0)

    def places(batch):
        cells = cell_ref[pl.ds(batch, 1), :]
        lon = owner_s[batch] * 2 + cells // 1024
        lat = (spot // QUARTER) * 8 + lax.rem(cells // 128, 8)
        return lon, lat

    def taper(lon_gap, lat_gap):
        lon_gap = jnp.minimum(lon_gap, NLON - lon_gap)
        return (
            jnp.maximum(7 - lon_gap, 0).astype(F32) * (NLAT - lat_gap).astype(F32) * scale
        )

    row = lax.broadcasted_iota(jnp.int32, (ROWS, OBS), 0)

    def assimilate(i, carry):
        batch = table_s[1 + i]
        slab = owner_s[batch]
        z = prior[i]
        turned = jnp.transpose(jnp.concatenate([z, jnp.zeros((128 - ROWS, OBS), F32)], axis=0))
        gained = jnp.sum(full_ref[i, 1] * turned[:, MEMBERS : MEMBERS + 1], axis=0, keepdims=True)
        z_high, z_low = split(z)
        root_high, root_low = split(full_ref[i, 0])
        weighted = dot(jnp.concatenate([z_high, z_low], axis=0), root_high)
        weighted = weighted[0:ROWS] + (weighted[ROWS : 2 * ROWS] + dot(z_high, root_low))
        weights = jnp.where(row < MEMBERS, weighted, jnp.where(row == MEMBERS, gained, 0.0))
        column_id = lax.broadcasted_iota(jnp.int32, (OBS, 128), 1)
        turned_high, turned_low = split(jnp.where(column_id < MEMBERS, turned, 0.0))
        turned_both = jnp.concatenate([turned_high, turned_low], axis=1)
        short_high, short_low = turned_high[:, 0:ROWS], turned_low[:, 0:ROWS]
        lon, lat = places(batch)
        both = jnp.concatenate(
            [jnp.broadcast_to(lon, (8, OBS)), jnp.broadcast_to(lat, (8, OBS))], axis=0
        ).astype(F32)
        upright = jnp.transpose(both).astype(jnp.int32)
        lon_col = upright[:, 0:1]
        lat_col = upright[:, 8:9]

        weights_high, weights_low = split(weights)

        def later(j, carry):
            other = table_s[1 + j]

            @pl.when(dist(owner_s[other], slab) <= REACH)
            def _():
                held = prior[j]
                held_high, held_low = split(held)
                covariance = dot3(short_high, short_low, held_high, held_low)
                lon_j, lat_j = places(other)
                gain = covariance * taper(jnp.abs(lon_col - lon_j), jnp.abs(lat_col - lat_j))
                gain_h, gain_l = split(gain)
                prior[j] = held - dot3(weights_high, weights_low, gain_h, gain_l)

            return carry

        lax.fori_loop(i + 1, count, later, 0)

        @pl.when(dist(slab, column) <= REACH)
        def _():
            for at in range(0, GROUPS, BUNDLE):
                highs, lows = [], []
                for c in range(at, at + BUNDLE):
                    cell_lon = column * 2 + c // 8
                    cell_lat = band * 8 + c % 8
                    factor = taper(jnp.abs(lon - cell_lon), jnp.abs(lat - cell_lat))
                    high, low = split(weights * factor)
                    highs.append(high)
                    lows.append(low)
                wide = dot(jnp.concatenate(highs, axis=0), turned_both)
                middle = wide[:, 0:128] + (wide[:, 128:256] + dot(jnp.concatenate(lows, axis=0), turned_high))
                middle = middle[:, 0:ROWS]
                for c in range(at, at + BUNDLE):
                    lanes = pl.ds(c * 128, 128)
                    block = state[:, lanes]
                    m_high, m_low = split(middle[(c - at) * ROWS : (c - at + 1) * ROWS])
                    b_high, b_low = split(block)
                    moved = dot(m_high, jnp.concatenate([b_high, b_low], axis=1))
                    state[:, lanes] = block - (moved[:, 0:128] + (moved[:, 128:256] + dot(m_low, b_high)))

        return carry

    lax.fori_loop(0, count, assimilate, 0)

    for c in range(GROUPS):
        lanes = pl.ds(c * 128, 128)
        out_anom_ref[pl.ds(c, MEMBERS, stride=GROUPS), :] = state[0:MEMBERS, lanes]
        out_mean_ref[pl.ds(c, 1), :] = -state[pl.ds(MEMBERS, 1), lanes]


VMEM = pl.BlockSpec(memory_space=pltpu.VMEM)
SMEM = pl.BlockSpec(memory_space=pltpu.SMEM)
HBM = pl.BlockSpec(memory_space=pl.ANY)
DMA = pltpu.SemaphoreType.DMA


def exchange(listed, planes, collective_id, packet, choice, rows):
    return pl.pallas_call(
        functools.partial(comm_kernel, listed, planes),
        name="exchange",
        out_shape=(
            jax.ShapeDtypeStruct((BANDS, listed // 2, ROWS, 128), F32),
            jax.ShapeDtypeStruct((listed, 2, OBS, OBS), F32),
        ),
        in_specs=[VMEM, VMEM, VMEM],
        out_specs=(VMEM, VMEM),
        scratch_shapes=[
            pltpu.VMEM((PAIRS, HALF, 128), F32),
            pltpu.VMEM((PAIRS, HALF, 128), F32),
            pltpu.VMEM((RING - 1, HALF, 128), F32),
            pltpu.VMEM((HALF, 128), F32),
            pltpu.VMEM((RING - 1, HALF, 128), F32),
            pltpu.VMEM((PAIRS, HALF, 128), F32),
            DMA, DMA,
            DMA((RING - 1,)), DMA((RING - 1,)),
            DMA((RING - 1,)), DMA((RING - 1,)),
            DMA((RING - 1,)), DMA((RING - 1,)),
            DMA((BANDS - 1,)), DMA((BANDS - 1,)),
            DMA((BANDS,)), DMA((BANDS,)),
            DMA((2, 2)), DMA((2, 2)),
            DMA((2,)), DMA((2,)),
            DMA((6,)), DMA((6,)),
        ],
        compiler_params=pltpu.CompilerParams(collective_id=collective_id, has_side_effects=True, vmem_limit_bytes=GRANT),
    )(packet, choice, rows)


def direct(listed, collective_id, lone, choice, rows):
    return pl.pallas_call(
        functools.partial(direct_kernel, listed),
        name="direct",
        out_shape=(
            jax.ShapeDtypeStruct((BANDS, listed // 2, ROWS, 128), F32),
            jax.ShapeDtypeStruct((listed, 2, OBS, OBS), F32),
        ),
        in_specs=[VMEM, VMEM, VMEM],
        out_specs=(VMEM, VMEM),
        scratch_shapes=[
            pltpu.VMEM((3, RING, HALF, 128), F32),
            pltpu.VMEM((HALF, 128), F32),
            DMA, DMA,
            DMA((RING - 1,)), DMA((RING - 1,)),
            DMA((2, RING)), DMA((2, RING)),
            DMA((BANDS - 1,)), DMA((BANDS - 1,)),
            DMA((BANDS,)), DMA((BANDS,)),
            DMA((2, 2)), DMA((2, 2)),
            DMA((2,)), DMA((2,)),
            DMA((6,)), DMA((6,)),
        ],
        compiler_params=pltpu.CompilerParams(collective_id=collective_id, has_side_effects=True, vmem_limit_bytes=GRANT),
    )(lone, choice, rows)


def solve(listed, owner, table, state, obs_cell, spread, full):
    return pl.pallas_call(
        solve_kernel,
        name="solve",
        out_shape=(
            jax.ShapeDtypeStruct((MEMBERS * GROUPS, 128), F32),
            jax.ShapeDtypeStruct((GROUPS, 128), F32),
        ),
        in_specs=[SMEM, SMEM, VMEM, VMEM, VMEM, VMEM],
        out_specs=(VMEM, VMEM),
        scratch_shapes=[
            pltpu.VMEM((ROWS, CELLS), F32),
            pltpu.VMEM((listed, ROWS, OBS), F32),
        ],
        compiler_params=pltpu.CompilerParams(vmem_limit_bytes=GRANT),
    )(owner, table, state, obs_cell, spread, full)


def local(anomalies, state_mean, obs_value, obs_cell, owner, order, root_inv, gain_inv):
    flat = anomalies.reshape(MEMBERS * GROUPS, 128)
    mean = state_mean.reshape(GROUPS, 128)
    packet, lone, rows, choice, near_choice, state, table, branch = pl.pallas_call(
        prep_kernel,
        name="prep",
        out_shape=(
            jax.ShapeDtypeStruct((PAIRS, ROWS, 128), F32),
            jax.ShapeDtypeStruct((ROWS, 128), F32),
            jax.ShapeDtypeStruct((BATCHES, 2, QUARTER, OBS), F32),
            jax.ShapeDtypeStruct((PAIRS, 2 * PAIRS, 128), F32),
            jax.ShapeDtypeStruct((MORE // 2, 6 * RING, 128), F32),
            jax.ShapeDtypeStruct((ROWS, CELLS), F32),
            jax.ShapeDtypeStruct((32,), jnp.int32),
            jax.ShapeDtypeStruct((1,), jnp.int32),
        ),
        in_specs=[SMEM, SMEM, HBM, VMEM, VMEM, VMEM, HBM, HBM],
        out_specs=(VMEM, VMEM, HBM, VMEM, VMEM, VMEM, SMEM, SMEM),
        scratch_shapes=[
            pltpu.VMEM((MEMBERS * GROUPS, 128), F32),
            pltpu.VMEM((BATCHES, 128), F32),
            pltpu.SMEM((BATCHES,), jnp.int32),
            pltpu.SMEM((BATCHES,), jnp.int32),
            pltpu.SMEM((1,), jnp.int32),
            DMA,
            DMA((BATCHES, 2)),
        ],
    )(order, owner, flat, mean, obs_cell, obs_value, root_inv, gain_inv)

    def near(listed, collective_id):
        spread, full = direct(listed, collective_id, lone, near_choice, rows)
        return solve(listed, owner, table, state, obs_cell, spread, full)

    def wide(listed, planes, collective_id):
        spread, full = exchange(listed, planes, collective_id, packet, choice, rows)
        return solve(listed, owner, table, state, obs_cell, spread, full)

    out_flat, out_mean = lax.switch(
        branch[0],
        (
            lambda: near(FEW, 1),
            lambda: near(MORE, 2),
            lambda: wide(SOME, NEXT_PLANES, 3),
            lambda: wide(BATCHES, ALL_PLANES, 4),
        ),
    )
    return out_flat.reshape(anomalies.shape), out_mean.reshape(state_mean.shape)


def solution(mesh):
    return jax.shard_map(
        local,
        mesh=mesh,
        in_specs=(
            P(None, "gx", "gy", None),
            P("gx", "gy", None),
            P(None, "gy"),
            P(),
            P(),
            P(),
            P(None, "gy", None),
            P(None, "gy", None),
        ),
        out_specs=(P(None, "gx", "gy", None), P("gx", "gy", None)),
        check_vma=False,
    )
```
